32 devices in a mesh: seq: 8 (over z, x), head: 4 (over y, core).
Axes of the slice: x: 2, y: 2, z: 4, core: 2. Of those that a mesh axis runs over, the one named last changes fastest.
Arguments:
- tokens: bfloat16 [8192, 1024], P(('seq', 'head')), may hold values from -6 to 6
- seq_lengths: int32 [8, 1], P('seq'), may hold values from 1024 to 1024, as said below
- w_qkvu: bfloat16 [4, 1024, 1024], replicated, may hold values from -0.1875 to 0.1875
- w_out: bfloat16 [1024, 1024], replicated, may hold values from -0.1875 to 0.1875
- w_glu: bfloat16 [2, 1024, 2816], replicated, may hold values from -0.1875 to 0.1875
- w_down: bfloat16 [2816, 1024], replicated, may hold values from -0.109375 to 0.109375
- cotangent: bfloat16 [8192, 1024], P(('seq', 'head')), may hold values from -6 to 6
Outputs:
- layer_out: bfloat16 [8192, 1024], P(('seq', 'head'))
- grad_tokens: float32 [8192, 1024], P(('seq', 'head'))
- grad_qkvu: float32 [4, 1024, 1024], P(None, None, 'head')
- grad_out: float32 [1024, 1024], P('head')
- grad_glu: float32 [2, 1024, 2816], P(None, None, 'head')
- grad_down: float32 [2816, 1024], P('head')
The draws below stay inside these ranges and needn't reach their ends.
Inputs may be any that keep to these rules, and one draw needn't show every extreme that they name: `seq_lengths`: row g lists the lengths in tokens of group g's sequences in order, each a multiple of 1024, summing to 1024, with zeros after the last. In every draw one group holds a single sequence and another holds 1 sequence of 1024 tokens.
All inputs are finite; a program needn't handle non-finite values.
Results may differ from the reference program's by a relative error of at most 0.013.
Values may be sent and summed in bfloat16 or wider, within the bound.
A program may use at most 192 MiB of HBM per device.

```python
import jax
import jax.numpy as jnp
from jax import lax

D = 1024
HEADS = 8
HEAD_DIM = 128
FF = 2816
BLK = 512
SEQ_MIN = 1024
GROUPS = 8
GROUP_TOK = 1024
UNITS = 1
TOKENS = 8192


def draw_seq_lengths(key, part):
    draw_key = jax.random.fold_in(key, 17)
    bit_key, pick_key, other_key = jax.random.split(draw_key, 3)
    breaks = jax.random.randint(bit_key, (GROUPS, UNITS), 0, 2).astype(jnp.int32)
    single_row = jax.random.randint(pick_key, (), 0, GROUPS)
    split_row = (single_row + 1 + jax.random.randint(other_key, (), 0, GROUPS - 1)) % GROUPS
    row_ids = jnp.arange(GROUPS, dtype=jnp.int32)[:, None]
    col_ids = jnp.arange(UNITS, dtype=jnp.int32)[None, :]
    breaks = jnp.where(row_ids == single_row, 0, breaks)
    breaks = jnp.where(row_ids == split_row, 1, breaks)
    breaks = jnp.where(col_ids == 0, 1, breaks).astype(jnp.int32)
    seq_ids = (jnp.cumsum(breaks, axis=1) - 1).astype(jnp.int32)
    slot_ids = jnp.arange(UNITS, dtype=jnp.int32)
    members = (seq_ids[:, :, None] == slot_ids[None, None, :]).astype(jnp.int32)
    return (jnp.sum(members, axis=1) * SEQ_MIN).astype(jnp.int32)


def levels(own_key, shape, shards, low, high):
    factor_of, own = 1.0, jax.random.fold_in(own_key, 6)
    for axis_at, shards_of in shards:
        steps = jnp.exp(jax.random.uniform(jax.random.fold_in(own, axis_at), (shards_of,), jnp.float32, low / len(shards), high / len(shards)))
        factor_of = factor_of * jnp.repeat(steps, shape[axis_at] // shards_of).reshape([-1 if axis == axis_at else 1 for axis in range(len(shape))])
    return factor_of


def noise(key, shape, scale, bound, shards=(), held_as=jnp.bfloat16):
    array = jax.random.normal(key, shape, jnp.float32) * scale
    if len(shards) > 0:
        array = levels(key, shape, shards, -0.22, 0.18) * array
    return jnp.clip(array, min=-bound, max=bound).astype(held_as)


def setup_inputs(seed: int = 0) -> dict:
    key_of = jax.random.split(jax.random.key(seed), 8)
    tokens = noise(key_of[0], (TOKENS, D), 1.0, 6.0, ((0, 32),))
    seq_lengths = draw_seq_lengths(jax.random.fold_in(key_of[7], 71), 0)
    w_qkvu = noise(key_of[2], (4, D, D), D ** -0.5, 0.1875)
    w_out = noise(key_of[3], (D, D), D ** -0.5, 0.1875)
    w_glu = noise(key_of[4], (2, D, FF), D ** -0.5, 0.1875)
    w_down = noise(key_of[5], (FF, D), FF ** -0.5, 0.109375)
    cotangent = noise(key_of[6], (TOKENS, D), 1.0, 6.0, ((0, 32),))
    return dict(tokens=tokens, seq_lengths=seq_lengths, w_qkvu=w_qkvu, w_out=w_out, w_glu=w_glu, w_down=w_down, cotangent=cotangent)


EPSILON = 1e-06
EXACT = lax.Precision.HIGHEST

@jax.custom_vjp
def low(v):
    return lax.optimization_barrier(v.astype(jnp.bfloat16)).astype(jnp.float32)

@jax.custom_vjp
def low_back(v):
    return v

def low_keep(v):
    return (low(v), None)

def low_pass(kept, grad):
    return (grad,)

def back_keep(v):
    return (v, None)

def back_low(kept, grad):
    return (low(grad),)
low.defvjp(low_keep, low_pass)
low_back.defvjp(back_keep, back_low)

def swish(values):
    return values * jax.nn.sigmoid(values)

def normalize(values):
    return values * lax.rsqrt(lax.optimization_barrier(jnp.mean(values * values, axis=-1, keepdims=True)) + EPSILON)

def layout(lengths, length_all):
    lengths = lengths.reshape(-1).astype(jnp.int32)
    offsets = (jnp.cumsum(lengths) - lengths).astype(jnp.int32)
    active_seq = lengths > 0
    token_ids = jnp.arange(length_all, dtype=jnp.int32)
    has_begun = active_seq[None, :] & (offsets[None, :] <= token_ids[:, None])
    starts = lax.optimization_barrier(jnp.max(jnp.where(has_begun, offsets[None, :], 0), axis=1)).astype(jnp.int32)
    places = (token_ids - starts).astype(jnp.float32)
    block_first = jnp.arange(length_all // BLK, dtype=jnp.int32) * BLK
    restarts = jnp.any(active_seq[None, :] & (offsets[None, :] == block_first[:, None]), axis=1)
    return (places, restarts)

def rotary(places):
    frequency = 10000.0 ** (-jnp.arange(HEAD_DIM, dtype=jnp.float32) / HEAD_DIM)
    angles = places[:, None] * frequency[None, :]
    return (jnp.cos(angles), jnp.sin(angles))

def decay_tables(slopes):
    positions = jnp.arange(BLK, dtype=jnp.float32)
    distance = positions[:, None] - positions[None, :]
    exponent = jnp.where(distance[None] >= 0, -slopes[:, None, None] * distance[None], -jnp.inf)
    decay_mask = jnp.exp(exponent)
    out_weight = jnp.exp(-slopes[:, None] * positions[None, :])
    in_weight = jnp.exp(-slopes[:, None] * (BLK - positions[None, :]))
    carry_weight = jnp.exp(-slopes * BLK)
    return (decay_mask, out_weight, in_weight, carry_weight)

def decay_pass(left_rows, right_rows, carried_rows, slopes, restarts):
    head_count, length_all, inner_width = left_rows.shape
    out_width = carried_rows.shape[2]
    block_count = length_all // BLK

    def blocks(values):
        return values.reshape(head_count, block_count, BLK, values.shape[2]).transpose(1, 0, 2, 3)
    decay_mask, out_weight, in_weight, carry_weight = decay_tables(slopes)

    @jax.checkpoint
    def advance(memory, pieces):
        part_a, part_b, part_c, restart = pieces
        memory = jnp.where(restart, jnp.zeros_like(memory), memory)
        scores = low(decay_mask * low_back(jnp.einsum('hnp,hmp->hnm', part_a, part_b, precision=EXACT)))
        inside = jnp.einsum('hnm,hmr->hnr', scores, part_c, precision=EXACT)
        carried = jnp.einsum('hnp,hpr->hnr', part_a, memory, precision=EXACT) * out_weight[:, :, None]
        update = jnp.einsum('hmp,hmr->hpr', part_b * in_weight[:, :, None], part_c, precision=EXACT)
        return (memory * carry_weight[:, None, None] + update, inside + carried)
    start_memory = jnp.zeros((head_count, inner_width, out_width), jnp.float32)
    _, results = lax.scan(advance, start_memory, (blocks(left_rows), blocks(right_rows), blocks(carried_rows), restarts))
    return results.transpose(1, 0, 2, 3).reshape(head_count, length_all, out_width)

def group_layer(inputs, w_qkvu, w_out, w_glu, w_down, places, restarts):
    length_all = inputs.shape[0]
    head_ids = jnp.arange(HEADS, dtype=jnp.float32)
    slopes = 2.0 ** (-8.0 * (head_ids + 1.0) / HEADS)
    normed_one = low(normalize(inputs))
    projected = jnp.einsum('td,kde->tke', normed_one, w_qkvu, precision=EXACT)
    moved = low(low_back(projected[:, :3]))
    gate_raw = low_back(projected[:, 3])
    per_head = moved.reshape(length_all, 3, HEADS, HEAD_DIM).transpose(1, 2, 0, 3)
    cosine, sine = rotary(places)
    query_act = swish(per_head[0])
    key_act = swish(per_head[1])
    query_pos = low(jnp.concatenate([query_act * cosine, query_act * sine], -1))
    key_pos = low(jnp.concatenate([key_act * cosine, key_act * sine], -1))
    attended = decay_pass(query_pos, key_pos, per_head[2], slopes, restarts)
    attended = low(low_back(attended)).transpose(1, 0, 2).reshape(length_all, D)
    mixed = low(normalize(attended) * swish(gate_raw))
    hidden_sum = inputs + low_back(jnp.dot(mixed, w_out, precision=EXACT))
    normed_two = low(normalize(hidden_sum))
    glu_pair = low_back(jnp.einsum('td,kdf->tkf', normed_two, w_glu, precision=EXACT))
    product = low(glu_pair[:, 0] * glu_pair[:, 1])
    return hidden_sum + jnp.dot(product, w_down, precision=EXACT)

def reference(tokens, seq_lengths, w_qkvu, w_out, w_glu, w_down, cotangent):
    weights = (w_qkvu.astype(jnp.float32), w_out.astype(jnp.float32), w_glu.astype(jnp.float32), w_down.astype(jnp.float32))
    token_groups = tokens.reshape(GROUPS, GROUP_TOK, D)
    grad_groups = cotangent.reshape(GROUPS, GROUP_TOK, D)

    def one_group(totals, pieces):
        inputs, upstream, lengths = pieces
        places, restarts = layout(lengths, GROUP_TOK)

        def forward(inputs_f, wq, wo, wg, wd):
            return group_layer(inputs_f, wq, wo, wg, wd, places, restarts)
        outputs, pullback = jax.vjp(forward, inputs.astype(jnp.float32), *weights)
        grads = pullback(upstream.astype(jnp.float32))
        new_totals = tuple((total + grad for total, grad in zip(totals, grads[1:])))
        return (new_totals, (outputs.astype(jnp.bfloat16), grads[0]))
    zero_grads = tuple((jnp.zeros_like(weight) for weight in weights))
    sums, (outputs, input_grads) = lax.scan(one_group, zero_grads, (token_groups, grad_groups, seq_lengths))
    return (outputs.reshape(TOKENS, D), input_grads.reshape(TOKENS, D), sums[0], sums[1], sums[2], sums[3])
```

```python
import functools

import jax
import jax.numpy as jnp
from jax import lax
from jax.experimental import pallas as pl
from jax.experimental.pallas import tpu as pltpu
from jax.sharding import PartitionSpec as P

D = 1024
HEADS = 8
HEAD_DIM = 128
EPSILON = 1e-06
PARTS = 4
LOCAL = D // PARTS
BF = jnp.bfloat16
F32 = jnp.float32
MESH = pl.DeviceIdType.MESH


def dot(a, b):
    return lax.dot_general(a, b, (((1,), (0,)), ((), ())), preferred_element_type=F32)


def dot_nt(a, b):
    return lax.dot_general(a, b, (((1,), (1,)), ((), ())), preferred_element_type=F32)


def dot_tn(a, b):
    return lax.dot_general(a, b, (((0,), (0,)), ((), ())), preferred_element_type=F32)


def sigmoid(v):
    return 1.0 / (1.0 + jnp.exp(-v))


def rms_scale(v):
    return lax.rsqrt(jnp.mean(v * v, axis=-1, keepdims=True) + EPSILON)


def norm_back(v, scale, grad):
    normed = v * scale
    return scale * (grad - normed * jnp.mean(grad * normed, axis=-1, keepdims=True))


def round_up(n, m):
    return -(-n // m) * m


def rows(start, size, align):
    return pl.ds(pl.multiple_of(start, align), size)


class Sizes:
    def __init__(self, seq, block, ff):
        self.seq = seq
        self.tb = block
        self.t = block * PARTS
        self.fs = ff // PARTS
        self.fp = round_up(self.fs, 256)
        self.full_tiles = self.fs // 128
        self.glu_tiles = 2 * self.full_tiles + (1 if self.fs % 128 else 0)
        counts = (
            (D // 128) * self.fs,
            self.glu_tiles * D,
            (D // 128) * LOCAL + 4 * (LOCAL // 128) * D,
        )
        self.chunk = tuple(round_up(-(-n // (2 * seq)), 16) for n in counts)
        self.base = (0, 2 * seq * self.chunk[0], 2 * seq * (self.chunk[0] + self.chunk[1]))
        self.total = self.base[2] + 2 * seq * self.chunk[2]


class Gather:
    def __init__(self, ctx, count, own, place, first):
        self.ctx, self.count, self.own, self.place, self.first = ctx, count, own, place, first

    def copy(self, src, dst, index, target):
        c = self.ctx
        return pltpu.make_async_remote_copy(
            src_ref=src,
            dst_ref=dst,
            send_sem=c.gsend.at[index],
            recv_sem=c.grecv.at[index],
            device_id=(c.s, target),
            device_id_type=MESH,
        )

    def across(self, k):
        c = self.ctx
        return self.copy(self.own(k), self.place(c.h, k), self.first + 3 * k, c.yp)

    def beside(self, k):
        c = self.ctx
        return self.copy(self.own(k), self.place(c.h, k), self.first + 3 * k + 1, c.sib)

    def relay(self, k):
        c = self.ctx
        spot = self.place(c.yp, k)
        return self.copy(spot, spot, self.first + 3 * k + 2, c.sib)

    def start(self, k):
        self.across(k).start()
        self.beside(k).start()

    def pass_on(self, k):
        self.across(k).wait_recv()
        self.relay(k).start()

    def wait_beside(self, k):
        self.beside(k).wait_recv()

    def wait_relay(self, k):
        self.relay(k).wait_recv()

    def drain(self):
        for k in range(self.count):
            self.across(k).wait_send()
            self.beside(k).wait_send()
            self.relay(k).wait_send()


class Scatter:
    def __init__(self, ctx, part, near, cross, first):
        self.ctx, self.part, self.near, self.cross, self.first = ctx, part, near, cross, first
        self.tb = ctx.sz.tb

    def block(self, index):
        return self.part.at[rows(index * self.tb, self.tb, self.tb), :]

    def copy(self, src, dst, index, target):
        c = self.ctx
        return pltpu.make_async_remote_copy(
            src_ref=src,
            dst_ref=dst,
            send_sem=c.gsend.at[index],
            recv_sem=c.grecv.at[index],
            device_id=(c.s, target),
            device_id_type=MESH,
        )

    def beside(self, k):
        c = self.ctx
        return self.copy(self.block(2 * k + 1 - c.c), self.near.at[k], self.first + k, c.sib)

    def across(self):
        c = self.ctx
        return self.copy(self.block(c.yp), self.cross, self.first + 2, c.yp)

    def start(self):
        self.beside(0).start()
        self.beside(1).start()

    def middle(self):
        c = self.ctx
        self.beside(0).wait_recv()
        self.beside(1).wait_recv()
        there = self.block(c.yp)
        there[...] = (there[...].astype(F32) + self.near[1 - c.y].astype(F32)).astype(BF)
        self.across().start()

    def result(self, lo, size):
        c = self.ctx
        here = self.part[rows(c.h * self.tb + lo, size, size), :].astype(F32)
        at = pl.ds(lo, size)
        return here + self.near[c.y, at, :].astype(F32) + self.cross[at, :].astype(F32)

    def wait(self):
        self.across().wait_recv()

    def drain(self):
        self.beside(0).wait_send()
        self.beside(1).wait_send()
        self.across().wait_send()


class Ring:
    def __init__(self, ctx, index, slots):
        self.ctx, self.index, self.slots = ctx, index, slots
        self.base, self.chunk = ctx.sz.base[index], ctx.sz.chunk[index]
        self.n = ctx.sz.seq

    def mine(self, d, k):
        k = lax.rem(k, self.n)
        return rows(self.base + (2 * k + d) * self.chunk, self.chunk, 16)

    def copy(self, d, src, dst, step):
        c = self.ctx
        return pltpu.make_async_remote_copy(
            src_ref=src,
            dst_ref=dst,
            send_sem=c.rsend.at[self.index, d, step],
            recv_sem=c.rrecv.at[self.index, d, step],
            device_id=(c.right if d == 0 else c.left, c.h),
            device_id_type=MESH,
        )

    def toward(self, d, t):
        return self.ctx.p + (self.n - t if d == 0 else t)

    def reduce_copy(self, d, t, first=False):
        f = self.ctx.f
        src = f.at[self.mine(d, self.toward(d, t)), :] if first else self.slots.at[d, t - 1]
        return self.copy(d, src, self.slots.at[d, t], t)

    def reduce_send(self, t, first=False):
        for d in range(2):
            self.reduce_copy(d, t, first).start()

    def reduce_take(self, t, last=False):
        f = self.ctx.f
        pieces = 4 if self.chunk % 64 == 0 else (2 if self.chunk % 32 == 0 else 1)
        size = self.chunk // pieces
        for d in range(2):
            self.reduce_copy(d, t, first=True).wait_recv()
            k = lax.rem(self.toward(d, t) + (self.n - 1 if d == 0 else 1), self.n)
            start = self.base + (2 * k + d) * self.chunk
            for i in range(pieces):
                at = rows(start + i * size, size, 16)
                inside = pl.ds(i * size, size)
                total = f[at, :].astype(F32) + self.slots[d, t, inside, :].astype(F32)
                if last:
                    f[at, :] = total.astype(BF)
                else:
                    self.slots[d, t, inside, :] = total.astype(BF)

    def spread_copy(self, d, t):
        spot = self.ctx.f.at[self.mine(d, self.toward(d, t) + (1 if d == 0 else self.n - 1)), :]
        return self.copy(d, spot, spot, self.n - 1 + t)

    def spread_send(self, t):
        for d in range(2):
            self.spread_copy(d, t).start()

    def spread_take(self, t):
        for d in range(2):
            self.spread_copy(d, t).wait_recv()

    def leave(self):
        for d in range(2):
            self.reduce_copy(d, 0, first=True).wait_send()

    def step(self, t):
        last = self.n - 2
        if t <= last:
            self.reduce_take(t, last=t == last)
            if t == 0:
                self.leave()
            if t < last:
                self.reduce_send(t + 1)
            else:
                self.spread_send(0)
        else:
            t -= self.n - 1
            self.spread_take(t)
            if t < last:
                self.spread_send(t + 1)

    def all_steps(self):
        last = self.n - 2

        def turn(t, carry):
            self.reduce_take(t)
            self.reduce_send(t + 1)
            return carry

        self.leave()
        lax.fori_loop(0, last, turn, 0)
        self.reduce_take(last, last=True)
        self.spread_send(0)

        def pass_on(t, carry):
            self.spread_take(t)
            self.spread_send(t + 1)
            return carry

        lax.fori_loop(0, last, pass_on, 0)
        self.spread_take(last)

    def drain(self):
        if self.n > 16:

            def one(t, carry):
                for d in range(2):
                    self.reduce_copy(d, t + 1, first=True).wait_send()
                    self.spread_copy(d, t).wait_send()
                return carry

            lax.fori_loop(0, self.n - 2, one, 0)
        else:
            for t in range(1, self.n - 1):
                for d in range(2):
                    self.reduce_copy(d, t, first=True).wait_send()
                    self.spread_copy(d, t - 1).wait_send()
        for d in range(2):
            self.spread_copy(d, self.n - 2).wait_send()


class Ctx:
    pass


def layer_kernel(sz, names, *refs):
    r = dict(zip(names, refs))
    ctx = Ctx()
    ctx.sz = sz
    seq, tb, t_all, fs, fp = sz.seq, sz.tb, sz.t, sz.fs, sz.fp
    half = seq // 2
    s, h = lax.axis_index("seq"), lax.axis_index("head")
    c, y = lax.rem(h, 2), h // 2
    z, x = s // 2, lax.rem(s, 2)
    pos = (1 - x) * z + x * (2 * half - 1 - z)

    def at_pos(p):
        q = p // half
        return (1 - q) * 2 * p + q * (2 * (2 * half - 1 - p) + 1)

    ctx.s, ctx.h, ctx.c, ctx.y, ctx.p = s, h, c, y, pos
    ctx.sib, ctx.yp = y * 2 + (1 - c), (1 - y) * 2 + c
    far = (1 - y) * 2 + (1 - c)
    ctx.right = at_pos(lax.rem(pos + 1, seq))
    ctx.left = at_pos(lax.rem(pos + seq - 1, seq))
    ctx.gsend, ctx.grecv = r["gsend"], r["grecv"]
    ctx.rsend, ctx.rrecv = r["rsend"], r["rrecv"]
    f = ctx.f = r["f"]
    lsem = r["lsem"]

    tok, cot, tok_g, cot_g = r["tok"], r["cot"], r["tok_g"], r["cot_g"]
    att, gate, mixed = r["att"], r["gate"], r["mixed"]

    loads = []

    def load(src, dst):
        copy = pltpu.make_async_copy(src, dst, lsem.at[len(loads)])
        copy.start()
        loads.append(copy)
        return copy

    mine = pl.ds(pl.multiple_of(h * LOCAL, LOCAL), LOCAL)
    own_rows = rows(h * tb, tb, tb)
    tok_in = load(tok, tok_g.at[own_rows, :])
    qkv_in = [
        load(r["w_qkvu"].at[k, :, mine], r["wqkv"].at[:, pl.ds(k * LOCAL, LOCAL)]) for k in range(3)
    ]
    gate_in = load(r["w_qkvu"].at[3], r["wgate"])
    out_in = load(r["w_out"], r["wout"])
    down_in = load(r["w_down"].at[rows(h * fs, fs, 64), :], r["wdown"].at[pl.ds(0, fs), :])
    glu_in = []
    window = y * (2 * fs) + c * (fs - fs % 128)
    tiles = fp // 128
    for k in range(2):
        for j in range(tiles):
            lane = pl.ds(pl.multiple_of(window + j * 128, 128), 128)
            glu_in.append(
                load(r["w_glu"].at[k, :, lane], f.at[pl.ds((k * tiles + j) * D, D), :])
            )
    cot_in = load(cot, cot_g.at[own_rows, :])

    barrier = pltpu.get_barrier_semaphore()
    for peer in ((s, ctx.sib), (s, ctx.yp), (ctx.right, h), (ctx.left, h)):
        pl.semaphore_signal(barrier, inc=1, device_id=peer, device_id_type=MESH)
    pl.semaphore_wait(barrier, 4)

    hb = tb // 2
    token_ag = Gather(
        ctx,
        2,
        lambda k: tok.at[pl.ds(k * hb, hb), :],
        lambda b, k: tok_g.at[rows(b * tb + k * hb, hb, hb), :],
        0,
    )
    cot_ag = Gather(
        ctx,
        2,
        lambda k: cot.at[pl.ds(k * hb, hb), :],
        lambda b, k: cot_g.at[rows(b * tb + k * hb, hb, hb), :],
        6,
    )
    ha = t_all // 2
    att_place = lambda b, k: att.at[b, pl.ds(k * ha, ha), :]
    att_ag = Gather(ctx, 2, lambda k: att_place(h, k), att_place, 12)
    low_place = lambda b, k: cot_g.at[rows(b * tb + k * hb, hb, hb), :]
    low_ag = Gather(ctx, 2, lambda k: low_place(h, k), low_place, 18)

    for k in range(2):
        token_ag.start(k)

    lane = lax.broadcasted_iota(jnp.int32, (32, HEAD_DIM), 1).astype(F32)
    step = lax.broadcasted_iota(jnp.int32, (32, HEAD_DIM), 0).astype(F32)
    frequency = jnp.exp(lane * (-9.210340371976184 / HEAD_DIM))
    fine = step * frequency
    coarse = (step * 32.0) * frequency
    cos_a, sin_a, cos_b, sin_b = jnp.cos(coarse), jnp.sin(coarse), jnp.cos(fine), jnp.sin(fine)
    for a in range(t_all // 32):
        at = pl.ds(a * 32, 32)
        ca, sa = cos_a[a : a + 1], sin_a[a : a + 1]
        r["cosine"][at, :] = ca * cos_b - sa * sin_b
        r["sine"][at, :] = sa * cos_b + ca * sin_b

    blocks = t_all // 256
    gap = lax.broadcasted_iota(jnp.int32, (256, 256), 0) - lax.broadcasted_iota(
        jnp.int32, (256, 256), 1
    )
    for e in range(2):
        slope = jnp.float32(0)
        for g in range(HEADS):
            slope = jnp.where(h * 2 + e == g, 2.0 ** (-8.0 * (g + 1) / HEADS), slope)
        for k in range(blocks):
            distance = gap + 256 * k
            value = jnp.exp(jnp.maximum(distance, 0).astype(F32) * -slope)
            r["decay"][e, k] = jnp.where(distance >= 0, value, 0.0)

    r["wdown"][pl.ds(fs, fp - fs), :] = jnp.zeros((fp - fs, D), BF)
    for one in glu_in:
        one.wait()
    part = fs % 128
    low_lanes = lax.broadcasted_iota(jnp.int32, (256, 128), 1) < 128 - part
    keep = lax.broadcasted_iota(jnp.int32, (256, 128), 1) < part if part else None
    shift = 128 - part if part else 0
    for k in range(2):
        for j in range(tiles):
            for i in range(D // 256):
                here = f[pl.ds((k * tiles + j) * D + i * 256, 256), :].astype(F32)
                value = here
                if part:
                    straight = jnp.where(keep, here, 0.0) if j == tiles - 1 else here
                    moved = pltpu.roll(here, 128 - part, 1)
                    if j < tiles - 1:
                        after = f[pl.ds((k * tiles + j + 1) * D + i * 256, 256), :].astype(F32)
                        moved = jnp.where(low_lanes, moved, pltpu.roll(after, 128 - part, 1))
                    else:
                        moved = jnp.where(low_lanes, moved, 0.0)
                    value = jnp.where(c == 1, moved, straight)
                r["wglu"][pl.ds(i * 256, 256), pl.ds(k * fp + j * 128, 128)] = value.astype(BF)

    tok_in.wait()
    for one in qkv_in:
        one.wait()
    gate_in.wait()

    def project(b):
        at = rows(b * tb, tb, tb)
        v = tok_g[at, :].astype(F32)
        n1 = (v * rms_scale(v)).astype(BF)
        r["n1"][at, :] = n1
        qkv = dot(n1, r["wqkv"][...]).astype(BF)
        r["raw"][at, :] = qkv
        co, si = r["cosine"][at, :], r["sine"][at, :]
        for e in range(2):
            for name, first in (("qpos", 0), ("kpos", LOCAL)):
                w = qkv[:, first + e * HEAD_DIM : first + (e + 1) * HEAD_DIM].astype(F32)
                act = w * sigmoid(w)
                r[name][e, at, pl.ds(0, HEAD_DIM)] = (act * co).astype(BF)
                r[name][e, at, pl.ds(HEAD_DIM, HEAD_DIM)] = (act * si).astype(BF)
        for k in range(PARTS):
            gate[k, at, :] = dot(n1, r["wgate"][:, pl.ds(k * LOCAL, LOCAL)]).astype(BF)

    project(h)
    for k in range(2):
        token_ag.wait_beside(k)
    project(ctx.sib)
    token_ag.pass_on(0)
    token_ag.pass_on(1)
    cot_ag.start(0)
    cot_ag.start(1)
    project(ctx.yp)
    token_ag.wait_relay(0)
    token_ag.wait_relay(1)
    project(far)

    value_at = 2 * LOCAL

    def attend(i):
        at = pl.ds(i * 256, 256)
        for e in range(2):
            lanes = pl.ds(value_at + e * HEAD_DIM, HEAD_DIM)
            q = r["qpos"][e, at, :]
            total = jnp.zeros((256, HEAD_DIM), F32)
            for j in range(i + 1):
                near = pl.ds(j * 256, 256)
                scores = (dot_nt(q, r["kpos"][e, near, :]) * r["decay"][e, i - j]).astype(BF)
                r["scores"][e, at, near] = scores
                total += dot(scores, r["raw"][near, lanes])
            att[h, at, pl.ds(e * HEAD_DIM, HEAD_DIM)] = total.astype(BF)

    for i in range(blocks):
        attend(i)
        if i == blocks // 2 - 1:
            att_ag.start(0)
    att_ag.start(1)

    out_in.wait()
    down_in.wait()
    cot_in.wait()
    cot_ag.pass_on(0)
    cot_ag.pass_on(1)
    for k in range(2):
        cot_ag.wait_beside(k)
        cot_ag.wait_relay(k)

    def mlp(b, carry):
        at = rows(b * 256, 256, 256)
        a = [att[k, at, :].astype(F32) for k in range(PARTS)]
        ssq = sum(jnp.sum(v * v, axis=-1, keepdims=True) for v in a)
        scale = lax.rsqrt(ssq * (1.0 / D) + EPSILON)
        hidden = tok_g[at, :].astype(F32)
        for k in range(PARTS):
            g = gate[k, at, :].astype(F32)
            m = (a[k] * scale * (g * sigmoid(g))).astype(BF)
            mixed[k, at, :] = m
            hidden += dot(m, r["wout"][pl.ds(k * LOCAL, LOCAL), :])

        @pl.when(b == h)
        def _():
            r["hidden"][...] = hidden

        n2 = (hidden * rms_scale(hidden)).astype(BF)
        r["n2"][at, :] = n2
        g = dot(n2, r["wglu"][:, pl.ds(0, fp)])
        u = dot(n2, r["wglu"][:, pl.ds(fp, fp)])
        product = (g * u).astype(BF)
        r["product"][at, :] = product
        dp = dot_nt(cot_g[at, :], r["wdown"][...])
        dg = (dp * u).astype(BF)
        du = (dp * g).astype(BF)
        r["dpair"][at, pl.ds(0, fp)] = dg
        r["dpair"][at, pl.ds(fp, fp)] = du
        r["lo_part"][at, :] = dot(product, r["wdown"][...]).astype(BF)
        back = dot_nt(dg, r["wglu"][:, pl.ds(0, fp)]) + dot_nt(du, r["wglu"][:, pl.ds(fp, fp)])
        r["dn_part"][at, :] = back.astype(BF)
        return carry

    token_ag.drain()
    for k in range(2):
        att_ag.pass_on(k)
        att_ag.wait_beside(k)
        att_ag.wait_relay(k)
        lax.fori_loop(k * blocks // 2, (k + 1) * blocks // 2, mlp, 0)

    dn_rs = Scatter(ctx, r["dn_part"], r["dn_near"], r["dn_cross"], 24)
    lo_rs = Scatter(ctx, r["lo_part"], r["lo_near"], r["lo_cross"], 27)
    one_rs = Scatter(ctx, r["lo_part"], r["one_near"], r["one_cross"], 30)
    rings = [Ring(ctx, i, r["slots%d" % i]) for i in range(3)]

    base = sz.base[0]
    for j in range(fp // 256):
        size = min(256, fs - j * 256)
        g = dot_tn(r["product"][:, pl.ds(j * 256, 256)], cot_g[...]).astype(BF)
        for k in range(D // 128):
            f[pl.ds(base + k * fs + j * 256, size), :] = g[:size, k * 128 : (k + 1) * 128]
    rings[0].reduce_send(0, first=True)
    cot_ag.drain()
    dn_rs.start()
    lo_rs.start()

    base_g = sz.base[1]
    full = sz.full_tiles

    def glu_grad(j, carry):
        g = dot_tn(r["n2"][:, rows(j * 256, 256, 256)], r["dpair"][...])
        for k in range(2):
            for i in range(full):
                at = rows(base_g + (k * full + i) * D + j * 256, 256, 16)
                first = k * fp + i * 128
                f[at, :] = g[:, first : first + 128].astype(BF)
        if part:
            a = g[:, full * 128 : full * 128 + 128]
            b = g[:, fp + full * 128 : fp + full * 128 + 128]
            at = rows(base_g + 2 * full * D + j * 256, 256, 16)
            f[at, :] = (a + pltpu.roll(b, part, 1)).astype(BF)
        return carry

    for j in range(D // 256):
        glu_grad(j, 0)
    rings[1].reduce_send(0, first=True)

    def low_block():
        dn_rs.wait()
        for i in range(tb // 128):
            at = pl.ds(i * 128, 128)
            v = r["hidden"][at, :]
            back = norm_back(v, rms_scale(v), dn_rs.result(i * 128, 128))
            d = cot_g[rows(h * tb + i * 128, 128, 128), :].astype(F32) + back
            r["dhid"][at, :] = d
            cot_g[rows(h * tb + i * 128, 128, 128), :] = d.astype(BF)
        low_ag.start(0)
        low_ag.start(1)

    def out_block():
        lo_rs.wait()
        for i in range(tb // 128):
            at = pl.ds(i * 128, 128)
            r["lo_cross"][at, :] = (r["hidden"][at, :] + lo_rs.result(i * 128, 128)).astype(BF)
        copy = pltpu.make_async_copy(r["lo_cross"], r["layer_out"], lsem.at[0])
        copy.start()
        return copy

    def low_arrive():
        for k in range(2):
            low_ag.pass_on(k)
        for k in range(2):
            low_ag.wait_beside(k)
            low_ag.wait_relay(k)

    own_out = pl.ds(pl.multiple_of(h * LOCAL, LOCAL), LOCAL)

    def mix_back(b):
        at = pl.ds(b * 256, 256)
        low = cot_g[at, :]
        a = [att[k, at, :].astype(F32) for k in range(PARTS)]
        ssq = sum(jnp.sum(v * v, axis=-1, keepdims=True) for v in a)
        scale = lax.rsqrt(ssq * (1.0 / D) + EPSILON)
        inner = jnp.zeros((256, 1), F32)
        for k in range(PARTS):
            g = gate[k, at, :].astype(F32)
            e = dot_nt(low, r["wout"][pl.ds(k * LOCAL, LOCAL), :]) * (g * sigmoid(g))
            inner += jnp.sum(e * (a[k] * scale), axis=-1, keepdims=True)
        inner = inner * (1.0 / D)
        g = gate[h, at, :].astype(F32)
        sig = sigmoid(g)
        normed = att[h, at, :].astype(F32) * scale
        dm = dot_nt(low, r["wout"][own_out, :])
        slope = sig + g * sig * (1.0 - sig)
        r["dproj"][at, pl.ds(3 * LOCAL, LOCAL)] = (dm * normed * slope).astype(BF)
        r["datt"][at, :] = (scale * (dm * (g * sig) - normed * inner)).astype(BF)

    base_r = sz.base[2]

    def out_grad():
        g = dot_tn(mixed[h], cot_g[...]).astype(BF)
        for k in range(D // 128):
            f[pl.ds(base_r + k * LOCAL, LOCAL), :] = g[:, k * 128 : (k + 1) * 128]

    def swish_slope(v):
        sig = sigmoid(v)
        return sig + v * sig * (1.0 - sig)

    def query_back(e, i):
        at = pl.ds(i * 256, 256)
        da = r["datt"][at, pl.ds(e * HEAD_DIM, HEAD_DIM)]
        total = jnp.zeros((256, 2 * HEAD_DIM), F32)
        for j in range(i + 1):
            near = pl.ds(j * 256, 256)
            v = r["raw"][near, pl.ds(value_at + e * HEAD_DIM, HEAD_DIM)]
            w = (dot_nt(da, v) * r["decay"][e, i - j]).astype(BF)
            r["weights"][at, near] = w
            total += dot(w, r["kpos"][e, near, :])
        lanes = pl.ds(e * HEAD_DIM, HEAD_DIM)
        co, si = r["cosine"][at, :], r["sine"][at, :]
        d = total[:, :HEAD_DIM] * co + total[:, HEAD_DIM:] * si
        raw = r["raw"][at, lanes].astype(F32)
        r["dproj"][at, lanes] = (d * swish_slope(raw)).astype(BF)

    def key_back(e, j):
        at = pl.ds(j * 256, 256)
        below = pl.ds(j * 256, t_all - j * 256)
        dk = dot_tn(r["weights"][below, at], r["qpos"][e, below, :])
        da = r["datt"][below, pl.ds(e * HEAD_DIM, HEAD_DIM)]
        dv = dot_tn(r["scores"][e, below, at], da)
        lanes = pl.ds(LOCAL + e * HEAD_DIM, HEAD_DIM)
        co, si = r["cosine"][at, :], r["sine"][at, :]
        d = dk[:, :HEAD_DIM] * co + dk[:, HEAD_DIM:] * si
        raw = r["raw"][at, lanes].astype(F32)
        r["dproj"][at, lanes] = (d * swish_slope(raw)).astype(BF)
        r["dproj"][at, pl.ds(value_at + e * HEAD_DIM, HEAD_DIM)] = dv.astype(BF)

    def head_query(e):
        for i in range(blocks):
            query_back(e, i)

    def head_key(e):
        for j in range(blocks):
            key_back(e, j)

    base_q = base_r + (D // 128) * LOCAL

    def qkvu_grad(j):
        g = dot_tn(r["n1"][:, pl.ds(j * 256, 256)], r["dproj"][...]).astype(BF)
        for k in range(D // 128):
            f[pl.ds(base_q + k * D + j * 256, 256), :] = g[:, k * 128 : (k + 1) * 128]

    def one_part(b):
        at = pl.ds(b * 256, 256)
        back = dot_nt(r["dproj"][at, pl.ds(0, 3 * LOCAL)], r["wqkv"][...])
        back += dot_nt(r["dproj"][at, pl.ds(3 * LOCAL, LOCAL)], r["wgate"][:, mine])
        r["lo_part"][at, :] = back.astype(BF)

    own_tok = pltpu.make_async_copy(tok, r["weights"].at[pl.ds(0, tb), :], lsem.at[5])

    def last_block():
        one_rs.wait()
        own_tok.wait()
        for i in range(tb // 128):
            at = pl.ds(i * 128, 128)
            v = r["weights"][at, :].astype(F32)
            back = norm_back(v, rms_scale(v), one_rs.result(i * 128, 128))
            r["dhid"][at, :] = r["dhid"][at, :] + back
        copy = pltpu.make_async_copy(r["dhid"], r["grad_tokens"], lsem.at[1])
        copy.start()
        return copy

    outs = []

    def publish(i):
        span = pl.ds(sz.base[i], 2 * seq * sz.chunk[i])
        copy = pltpu.make_async_copy(f.at[span, :], r["f_out"].at[span, :], lsem.at[2 + i])
        copy.start()
        outs.append(copy)

    pieces = [
        lambda: (dn_rs.middle(), lo_rs.middle()),
        low_block,
        lambda: outs.append(out_block()),
        low_arrive,
        lambda: mix_back(0),
        lambda: mix_back(1),
        lambda: mix_back(2),
        lambda: mix_back(3),
        out_grad,
        lambda: head_query(0),
        lambda: head_key(0),
        lambda: head_query(1),
        lambda: head_key(1),
        lambda: (qkvu_grad(0), qkvu_grad(1)),
        lambda: (qkvu_grad(2), qkvu_grad(3), rings[2].reduce_send(0, first=True)),
        lambda: (lo_rs.drain(), one_part(0), one_part(1)),
        lambda: (one_part(2), one_part(3), one_rs.start(), own_tok.start()),
        lambda: one_rs.middle(),
        lambda: outs.append(last_block()),
    ]
    assert blocks == 4
    if seq > 16:
        for piece in pieces:
            piece()
        for i, ring in enumerate(rings):
            ring.all_steps()
            publish(i)
    else:
        queue = list(pieces)
        total = 2 * (seq - 1)
        slot = 0
        rest = 0
        ready = len(pieces) - 4
        while slot < total or rest < total or queue:
            for _ in range(2):
                if slot < total:
                    rings[_].step(slot)
                if queue:
                    queue.pop(0)()
            if slot < total:
                slot += 1
                if slot == total:
                    publish(0)
                    publish(1)
            if len(queue) <= len(pieces) - ready - 1 + 0 and len(pieces) - len(queue) > ready - 1:
                if rest < total:
                    rings[2].step(rest)
                    rest += 1
        publish(2)

    for ag in (att_ag, low_ag):
        ag.drain()
    dn_rs.drain()
    one_rs.drain()
    for ring in rings:
        ring.drain()
    for copy in outs:
        copy.wait()


def main_call(sz, tokens, w_qkvu, w_out, w_glu, w_down, cotangent):
    any_spec = pl.BlockSpec(memory_space=pl.ANY)
    t, tb, fp, seq = sz.t, sz.tb, sz.fp, sz.seq
    scratch = dict(
        tok_g=pltpu.VMEM((t, D), BF),
        cot_g=pltpu.VMEM((t, D), BF),
        n1=pltpu.VMEM((t, D), BF),
        raw=pltpu.VMEM((t, 3 * LOCAL), BF),
        wqkv=pltpu.VMEM((D, 3 * LOCAL), BF),
        wgate=pltpu.VMEM((D, D), BF),
        wout=pltpu.VMEM((D, D), BF),
        wglu=pltpu.VMEM((D, 2 * fp), BF),
        wdown=pltpu.VMEM((fp, D), BF),
        qpos=pltpu.VMEM((2, t, 2 * HEAD_DIM), BF),
        kpos=pltpu.VMEM((2, t, 2 * HEAD_DIM), BF),
        scores=pltpu.VMEM((2, t, t), BF),
        weights=pltpu.VMEM((t, t), BF),
        decay=pltpu.VMEM((2, t // 256, 256, 256), F32),
        cosine=pltpu.VMEM((t, HEAD_DIM), F32),
        sine=pltpu.VMEM((t, HEAD_DIM), F32),
        att=pltpu.VMEM((PARTS, t, LOCAL), BF),
        gate=pltpu.VMEM((PARTS, t, LOCAL), BF),
        mixed=pltpu.VMEM((PARTS, t, LOCAL), BF),
        hidden=pltpu.VMEM((tb, D), F32),
        product=pltpu.VMEM((t, fp), BF),
        dpair=pltpu.VMEM((t, 2 * fp), BF),
        dn_part=pltpu.VMEM((t, D), BF),
        dn_near=pltpu.VMEM((2, tb, D), BF),
        dn_cross=pltpu.VMEM((tb, D), BF),
        lo_near=pltpu.VMEM((2, tb, D), BF),
        lo_cross=pltpu.VMEM((tb, D), BF),
        dhid=pltpu.VMEM((tb, D), F32),
        f=pltpu.VMEM((sz.total, 128), BF),
        slots0=pltpu.VMEM((2, seq - 1, sz.chunk[0], 128), BF),
        slots1=pltpu.VMEM((2, seq - 1, sz.chunk[1], 128), BF),
        slots2=pltpu.VMEM((2, seq - 1, sz.chunk[2], 128), BF),
        gsend=pltpu.SemaphoreType.DMA((33,)),
        grecv=pltpu.SemaphoreType.DMA((33,)),
        rsend=pltpu.SemaphoreType.DMA((3, 2, 2 * (seq - 1))),
        rrecv=pltpu.SemaphoreType.DMA((3, 2, 2 * (seq - 1))),
        lsem=pltpu.SemaphoreType.DMA((24,)),
    )
    if seq > 16:
        for i in range(3):
            del scratch["slots%d" % i]
        scratch["slots"] = pltpu.VMEM((2, seq - 1, max(sz.chunk), 128), BF)
    assert 2 * fp >= D + LOCAL and tb == 256
    names = ["tok", "w_qkvu", "w_out", "w_glu", "w_down", "cot", "layer_out", "grad_tokens", "f_out"]
    names += list(scratch)

    def kernel(*refs):
        named = dict(zip(names, refs))
        named["n2"] = named["weights"]
        for i in range(3 if seq > 16 else 0):
            named["slots%d" % i] = named["slots"].at[:, :, pl.ds(0, sz.chunk[i]), :]
        named["lo_part"] = named["tok_g"]
        named["one_near"], named["one_cross"] = named["dn_near"], named["dn_cross"]
        named["dproj"] = named["dpair"].at[:, pl.ds(0, D)]
        named["datt"] = named["dpair"].at[:, pl.ds(D, LOCAL)]
        layer_kernel(sz, list(named), *named.values())

    return pl.pallas_call(
        kernel,
        name="layer",
        out_shape=(
            jax.ShapeDtypeStruct((tb, D), BF),
            jax.ShapeDtypeStruct((tb, D), F32),
            jax.ShapeDtypeStruct((sz.total, 128), BF),
        ),
        in_specs=[any_spec] * 6,
        out_specs=(any_spec,) * 3,
        scratch_shapes=list(scratch.values()),
        compiler_params=pltpu.CompilerParams(
            collective_id=0, has_side_effects=True, vmem_limit_bytes=67043328
        ),
    )(tokens, w_qkvu, w_out, w_glu, w_down, cotangent)


def unpack(sz, flat):
    fs, full = sz.fs, sz.full_tiles
    part = fs % 128

    def columns(first, count, height):
        block = flat[first : first + count * height].reshape(count, height, 128)
        return block.transpose(1, 0, 2).reshape(height, count * 128).astype(F32)

    grad_down = columns(0, D // 128, fs)
    wide = columns(sz.base[1], sz.glu_tiles, D)
    pair = []
    for k in range(2):
        cols = [wide[:, k * full * 128 : (k + 1) * full * 128]]
        if part:
            at = 2 * full * 128 + k * part
            cols.append(wide[:, at : at + part])
        pair.append(jnp.concatenate(cols, 1))
    grad_glu = jnp.stack(pair)
    grad_out = columns(sz.base[2], D // 128, LOCAL)
    first = sz.base[2] + (D // 128) * LOCAL
    grad_qkvu = jnp.stack([columns(first + k * 2 * D, 2, D) for k in range(4)])
    return grad_qkvu, grad_out, grad_glu, grad_down


def per_device(tokens, seq_lengths, w_qkvu, w_out, w_glu, w_down, cotangent):
    assert seq_lengths.shape == (1, 1) and lax.axis_size("head") == PARTS
    sz = Sizes(lax.axis_size("seq"), tokens.shape[0], w_down.shape[0])
    layer_out, grad_tokens, flat = main_call(sz, tokens, w_qkvu, w_out, w_glu, w_down, cotangent)
    return (layer_out, grad_tokens, *unpack(sz, flat))


def solution(mesh):
    return jax.shard_map(
        per_device,
        mesh=mesh,
        in_specs=(
            P(("seq", "head"), None),
            P("seq", None),
            P(),
            P(),
            P(),
            P(),
            P(("seq", "head"), None),
        ),
        out_specs=(
            P(("seq", "head"), None),
            P(("seq", "head"), None),
            P(None, None, "head"),
            P("head", None),
            P(None, None, "head"),
            P("head", None),
        ),
        check_vma=False,
    )
```

```python
import functools

import jax
import jax.numpy as jnp
from jax import lax
from jax.experimental import pallas as pl
from jax.experimental.pallas import tpu as pltpu
from jax.sharding import PartitionSpec as P

D = 1024
HEADS = 8
HEAD_DIM = 128
EPSILON = 1e-06
PARTS = 4
LOCAL = D // PARTS
BF = jnp.bfloat16
F32 = jnp.float32
MESH = pl.DeviceIdType.MESH


def dot(a, b):
    return lax.dot_general(a, b, (((1,), (0,)), ((), ())), preferred_element_type=F32)


def dot_nt(a, b):
    return lax.dot_general(a, b, (((1,), (1,)), ((), ())), preferred_element_type=F32)


def dot_tn(a, b):
    return lax.dot_general(a, b, (((0,), (0,)), ((), ())), preferred_element_type=F32)


def sigmoid(v):
    return 1.0 / (1.0 + jnp.exp(-v))


def rms_scale(v):
    return lax.rsqrt(jnp.mean(v * v, axis=-1, keepdims=True) + EPSILON)


def norm_back(v, scale, grad):
    normed = v * scale
    return scale * (grad - normed * jnp.mean(grad * normed, axis=-1, keepdims=True))


def round_up(n, m):
    return -(-n // m) * m


def rows(start, size, align):
    return pl.ds(pl.multiple_of(start, align), size)


class Sizes:
    def __init__(self, seq, block, ff):
        self.seq = seq
        self.tb = block
        self.t = block * PARTS
        self.fs = ff // PARTS
        self.fp = round_up(self.fs, 256)
        self.full_tiles = self.fs // 128
        self.glu_tiles = 2 * self.full_tiles + (1 if self.fs % 128 else 0)
        rest = (D // 128) * LOCAL + 4 * (LOCAL // 128) * D
        chunk = lambda n: round_up(-(-n // (2 * seq)), 16)
        self.chunk = [chunk((D // 128) * self.fs), chunk(self.glu_tiles * D), chunk(rest // 2)]
        self.chunk.append(chunk(rest - 2 * seq * self.chunk[2]))
        self.base = [2 * seq * sum(self.chunk[:i]) for i in range(5)]
        self.total = self.base[4]


class Gather:
    def __init__(self, ctx, count, own, place, first):
        self.ctx, self.count, self.own, self.place, self.first = ctx, count, own, place, first

    def copy(self, src, dst, index, target):
        c = self.ctx
        return pltpu.make_async_remote_copy(
            src_ref=src,
            dst_ref=dst,
            send_sem=c.gsend.at[index],
            recv_sem=c.grecv.at[index],
            device_id=(c.s, target),
            device_id_type=MESH,
        )

    def across(self, k):
        c = self.ctx
        return self.copy(self.own(k), self.place(c.h, k), self.first + 3 * k, c.yp)

    def beside(self, k):
        c = self.ctx
        return self.copy(self.own(k), self.place(c.h, k), self.first + 3 * k + 1, c.sib)

    def relay(self, k):
        c = self.ctx
        spot = self.place(c.yp, k)
        return self.copy(spot, spot, self.first + 3 * k + 2, c.sib)

    def start(self, k):
        self.across(k).start()
        self.beside(k).start()

    def pass_on(self, k):
        self.across(k).wait_recv()
        self.relay(k).start()

    def wait_beside(self, k):
        self.beside(k).wait_recv()

    def wait_relay(self, k):
        self.relay(k).wait_recv()

    def drain(self):
        for k in range(self.count):
            self.across(k).wait_send()
            self.beside(k).wait_send()
            self.relay(k).wait_send()


class Scatter:
    def __init__(self, ctx, part, near, cross, first):
        self.ctx, self.part, self.near, self.cross, self.first = ctx, part, near, cross, first
        self.tb = ctx.sz.tb

    def block(self, index):
        return self.part.at[rows(index * self.tb, self.tb, self.tb), :]

    def copy(self, src, dst, index, target):
        c = self.ctx
        return pltpu.make_async_remote_copy(
            src_ref=src,
            dst_ref=dst,
            send_sem=c.gsend.at[index],
            recv_sem=c.grecv.at[index],
            device_id=(c.s, target),
            device_id_type=MESH,
        )

    def beside(self, k):
        c = self.ctx
        return self.copy(self.block(2 * k + 1 - c.c), self.near.at[k], self.first + k, c.sib)

    def across(self):
        c = self.ctx
        return self.copy(self.block(c.yp), self.cross, self.first + 2, c.yp)

    def start(self):
        self.beside(0).start()
        self.beside(1).start()

    def middle(self):
        c = self.ctx
        self.beside(0).wait_recv()
        self.beside(1).wait_recv()
        there = self.block(c.yp)
        there[...] = (there[...].astype(F32) + self.near[1 - c.y].astype(F32)).astype(BF)
        self.across().start()

    def result(self, lo, size):
        c = self.ctx
        here = self.part[rows(c.h * self.tb + lo, size, size), :].astype(F32)
        at = pl.ds(lo, size)
        return here + self.near[c.y, at, :].astype(F32) + self.cross[at, :].astype(F32)

    def wait(self):
        self.across().wait_recv()

    def drain(self):
        self.beside(0).wait_send()
        self.beside(1).wait_send()
        self.across().wait_send()


class Ring:
    def __init__(self, ctx, index, slots):
        self.ctx, self.index, self.slots = ctx, index, slots
        self.base, self.chunk = ctx.sz.base[index], ctx.sz.chunk[index]
        self.n = ctx.sz.seq

    def mine(self, d, k):
        k = lax.rem(k, self.n)
        return rows(self.base + (2 * k + d) * self.chunk, self.chunk, 16)

    def copy(self, d, src, dst, step):
        c = self.ctx
        return pltpu.make_async_remote_copy(
            src_ref=src,
            dst_ref=dst,
            send_sem=c.rsend.at[self.index, d, step],
            recv_sem=c.rrecv.at[self.index, d, step],
            device_id=(c.right if d == 0 else c.left, c.h),
            device_id_type=MESH,
        )

    def toward(self, d, t):
        return self.ctx.p + (self.n - t if d == 0 else t)

    def publish(self, d, k, j):
        if self.n > 16:
            return
        at = self.mine(d, k)
        c = self.ctx
        copy = pltpu.make_async_copy(c.f.at[at, :], c.f_out.at[at, :], c.psem.at[self.index, d, j])
        copy.start()
        c.outs.append(copy)

    def reduce_copy(self, d, t, first=False):
        f = self.ctx.f
        src = f.at[self.mine(d, self.toward(d, t)), :] if first else self.slots.at[d, t - 1]
        return self.copy(d, src, self.slots.at[d, t], t)

    def reduce_send(self, t, first=False):
        for d in range(2):
            self.reduce_copy(d, t, first).start()

    def reduce_take(self, t, last=False):
        f = self.ctx.f
        pieces = 4 if self.chunk % 64 == 0 else (2 if self.chunk % 32 == 0 else 1)
        size = self.chunk // pieces
        for d in range(2):
            self.reduce_copy(d, t, first=True).wait_recv()
            k = lax.rem(self.toward(d, t) + (self.n - 1 if d == 0 else 1), self.n)
            start = self.base + (2 * k + d) * self.chunk
            for i in range(pieces):
                at = rows(start + i * size, size, 16)
                inside = pl.ds(i * size, size)
                total = f[at, :].astype(F32) + self.slots[d, t, inside, :].astype(F32)
                if last:
                    f[at, :] = total.astype(BF)
                else:
                    self.slots[d, t, inside, :] = total.astype(BF)
            if last:
                self.publish(d, k, self.n - 1)

    def spread_copy(self, d, t):
        spot = self.ctx.f.at[self.mine(d, self.toward(d, t) + (1 if d == 0 else self.n - 1)), :]
        return self.copy(d, spot, spot, self.n - 1 + t)

    def spread_send(self, t):
        for d in range(2):
            self.spread_copy(d, t).start()

    def spread_take(self, t):
        for d in range(2):
            self.spread_copy(d, t).wait_recv()
            if isinstance(t, int):
                self.publish(d, self.toward(d, t), t)

    def leave(self):
        for d in range(2):
            self.reduce_copy(d, 0, first=True).wait_send()

    def step(self, t):
        last = self.n - 2
        if t <= last:
            self.reduce_take(t, last=t == last)
            if t == 0:
                self.leave()
            if t < last:
                self.reduce_send(t + 1)
            else:
                self.spread_send(0)
        else:
            t -= self.n - 1
            self.spread_take(t)
            if t < last:
                self.spread_send(t + 1)

    def all_steps(self):
        last = self.n - 2

        def turn(t, carry):
            self.reduce_take(t)
            self.reduce_send(t + 1)
            return carry

        self.leave()
        lax.fori_loop(0, last, turn, 0)
        self.reduce_take(last, last=True)
        self.spread_send(0)

        def pass_on(t, carry):
            self.spread_take(t)
            self.spread_send(t + 1)
            return carry

        lax.fori_loop(0, last, pass_on, 0)
        self.spread_take(last)

    def drain(self):
        if self.n > 16:

            def one(t, carry):
                for d in range(2):
                    self.reduce_copy(d, t + 1, first=True).wait_send()
                    self.spread_copy(d, t).wait_send()
                return carry

            lax.fori_loop(0, self.n - 2, one, 0)
        else:
            for t in range(1, self.n - 1):
                for d in range(2):
                    self.reduce_copy(d, t, first=True).wait_send()
                    self.spread_copy(d, t - 1).wait_send()
        for d in range(2):
            self.spread_copy(d, self.n - 2).wait_send()


class Ctx:
    pass


def layer_kernel(sz, names, *refs):
    r = dict(zip(names, refs))
    ctx = Ctx()
    ctx.sz = sz
    seq, tb, t_all, fs, fp = sz.seq, sz.tb, sz.t, sz.fs, sz.fp
    half = seq // 2
    s, h = lax.axis_index("seq"), lax.axis_index("head")
    c, y = lax.rem(h, 2), h // 2
    z, x = s // 2, lax.rem(s, 2)
    pos = (1 - x) * z + x * (2 * half - 1 - z)

    def at_pos(p):
        q = p // half
        return (1 - q) * 2 * p + q * (2 * (2 * half - 1 - p) + 1)

    ctx.s, ctx.h, ctx.c, ctx.y, ctx.p = s, h, c, y, pos
    ctx.sib, ctx.yp = y * 2 + (1 - c), (1 - y) * 2 + c
    far = (1 - y) * 2 + (1 - c)
    ctx.right = at_pos(lax.rem(pos + 1, seq))
    ctx.left = at_pos(lax.rem(pos + seq - 1, seq))
    ctx.gsend, ctx.grecv = r["gsend"], r["grecv"]
    ctx.rsend, ctx.rrecv = r["rsend"], r["rrecv"]
    f = ctx.f = r["f"]
    ctx.f_out, ctx.psem, ctx.outs = r["f_out"], r["psem"], []
    lsem = r["lsem"]

    tok, cot, tok_g, cot_g = r["tok"], r["cot"], r["tok_g"], r["cot_g"]
    att, gate, mixed = r["att"], r["gate"], r["mixed"]

    loads = []

    def load(src, dst):
        copy = pltpu.make_async_copy(src, dst, lsem.at[len(loads)])
        copy.start()
        loads.append(copy)
        return copy

    mine = pl.ds(pl.multiple_of(h * LOCAL, LOCAL), LOCAL)
    own_rows = rows(h * tb, tb, tb)
    tok_in = load(tok, tok_g.at[own_rows, :])
    qkv_in = [
        load(r["w_qkvu"].at[k, :, mine], r["wqkv"].at[:, pl.ds(k * LOCAL, LOCAL)]) for k in range(3)
    ]
    gate_in = load(r["w_qkvu"].at[3], r["wgate"])
    out_in = load(r["w_out"], r["wout"])
    down_in = load(r["w_down"].at[rows(h * fs, fs, 64), :], r["wdown"].at[pl.ds(0, fs), :])
    glu_in = []
    window = y * (2 * fs) + c * (fs - fs % 128)
    tiles = fp // 128
    for k in range(2):
        for j in range(tiles):
            lane = pl.ds(pl.multiple_of(window + j * 128, 128), 128)
            glu_in.append(
                load(r["w_glu"].at[k, :, lane], f.at[pl.ds((k * tiles + j) * D, D), :])
            )
    cot_in = load(cot, cot_g.at[own_rows, :])

    barrier = pltpu.get_barrier_semaphore()
    for peer in ((s, ctx.sib), (s, ctx.yp), (ctx.right, h), (ctx.left, h)):
        pl.semaphore_signal(barrier, inc=1, device_id=peer, device_id_type=MESH)
    pl.semaphore_wait(barrier, 4)

    hb = tb // 2
    token_ag = Gather(
        ctx,
        2,
        lambda k: tok.at[pl.ds(k * hb, hb), :],
        lambda b, k: tok_g.at[rows(b * tb + k * hb, hb, hb), :],
        0,
    )
    cot_ag = Gather(
        ctx,
        2,
        lambda k: cot.at[pl.ds(k * hb, hb), :],
        lambda b, k: cot_g.at[rows(b * tb + k * hb, hb, hb), :],
        6,
    )
    blocks = t_all // 256
    att_place = lambda b, k: att.at[b, pl.ds(k * 256, 256), :]
    att_ag = Gather(ctx, blocks, lambda k: att_place(h, k), att_place, 33)
    low_place = lambda b, k: cot_g.at[rows(b * tb + k * hb, hb, hb), :]
    low_ag = Gather(ctx, 2, lambda k: low_place(h, k), low_place, 18)

    for k in range(2):
        token_ag.start(k)

    lane = lax.broadcasted_iota(jnp.int32, (32, HEAD_DIM), 1).astype(F32)
    step = lax.broadcasted_iota(jnp.int32, (32, HEAD_DIM), 0).astype(F32)
    frequency = jnp.exp(lane * (-9.210340371976184 / HEAD_DIM))
    fine = step * frequency
    coarse = (step * 32.0) * frequency
    cos_a, sin_a, cos_b, sin_b = jnp.cos(coarse), jnp.sin(coarse), jnp.cos(fine), jnp.sin(fine)
    for a in range(t_all // 32):
        at = pl.ds(a * 32, 32)
        ca, sa = cos_a[a : a + 1], sin_a[a : a + 1]
        r["cosine"][at, :] = ca * cos_b - sa * sin_b
        r["sine"][at, :] = sa * cos_b + ca * sin_b

    gap = lax.broadcasted_iota(jnp.int32, (256, 256), 0) - lax.broadcasted_iota(
        jnp.int32, (256, 256), 1
    )
    for e in range(2):
        slope = jnp.float32(0)
        for g in range(HEADS):
            slope = jnp.where(h * 2 + e == g, 2.0 ** (-8.0 * (g + 1) / HEADS), slope)
        for k in range(blocks):
            distance = gap + 256 * k
            value = jnp.exp(jnp.maximum(distance, 0).astype(F32) * -slope)
            r["decay"][e, k] = jnp.where(distance >= 0, value, 0.0)

    r["wdown"][pl.ds(fs, fp - fs), :] = jnp.zeros((fp - fs, D), BF)
    for one in glu_in:
        one.wait()
    part = fs % 128
    low_lanes = lax.broadcasted_iota(jnp.int32, (256, 128), 1) < 128 - part
    keep = lax.broadcasted_iota(jnp.int32, (256, 128), 1) < part if part else None

    def window_rows(n, carry):
        k, i = n // (D // 256), lax.rem(n, D // 256)
        first = k * tiles * D + i * 256
        tile = [f[rows(first + j * D, 256, 256), :].astype(F32) for j in range(tiles)]
        for j in range(tiles):
            value = tile[j]
            if part:
                straight = jnp.where(keep, value, 0.0) if j == tiles - 1 else value
                after = pltpu.roll(tile[j + 1], 128 - part, 1) if j < tiles - 1 else 0.0
                moved = jnp.where(low_lanes, pltpu.roll(value, 128 - part, 1), after)
                value = jnp.where(c == 1, moved, straight)
            lanes = pl.ds(pl.multiple_of(k * fp + j * 128, 128), 128)
            r["wglu"][rows(i * 256, 256, 256), lanes] = value.astype(BF)
        return carry

    lax.fori_loop(0, 2 * (D // 256), window_rows, 0)

    tok_in.wait()
    for one in qkv_in:
        one.wait()
    gate_in.wait()

    def project(b):
        at = rows(b * tb, tb, tb)
        v = tok_g[at, :].astype(F32)
        n1 = (v * rms_scale(v)).astype(BF)
        r["n1"][at, :] = n1
        qkv = dot(n1, r["wqkv"][...]).astype(BF)
        r["raw"][at, :] = qkv
        co, si = r["cosine"][at, :], r["sine"][at, :]
        for e in range(2):
            for name, first in (("qpos", 0), ("kpos", LOCAL)):
                w = qkv[:, first + e * HEAD_DIM : first + (e + 1) * HEAD_DIM].astype(F32)
                act = w * sigmoid(w)
                r[name][e, at, pl.ds(0, HEAD_DIM)] = (act * co).astype(BF)
                r[name][e, at, pl.ds(HEAD_DIM, HEAD_DIM)] = (act * si).astype(BF)
        for k in range(PARTS):
            gate[k, at, :] = dot(n1, r["wgate"][:, pl.ds(k * LOCAL, LOCAL)]).astype(BF)

    def project_turn(k, carry):
        @pl.when(k == 1)
        def _():
            for i in range(2):
                token_ag.wait_beside(i)

        @pl.when(k == 2)
        def _():
            for i in range(2):
                token_ag.pass_on(i)
            for i in range(2):
                cot_ag.start(i)

        @pl.when(k == 3)
        def _():
            for i in range(2):
                token_ag.wait_relay(i)

        yy = y + (k // 2) * (1 - 2 * y)
        cc = c + lax.rem(k, 2) * (1 - 2 * c)
        project(yy * 2 + cc)
        return carry

    lax.fori_loop(0, PARTS, project_turn, 0)

    value_at = 2 * LOCAL

    def attend(i):
        at = pl.ds(i * 256, 256)

        def one_head(e, carry):
            lanes = rows(value_at + e * HEAD_DIM, HEAD_DIM, HEAD_DIM)
            q = r["qpos"][e, at, :]
            total = jnp.zeros((256, HEAD_DIM), F32)
            for j in range(i + 1):
                near = pl.ds(j * 256, 256)
                scores = (dot_nt(q, r["kpos"][e, near, :]) * r["decay"][e, i - j]).astype(BF)
                r["scores"][e, at, near] = scores
                total += dot(scores, r["raw"][near, lanes])
            att[h, at, rows(e * HEAD_DIM, HEAD_DIM, HEAD_DIM)] = total.astype(BF)
            return carry

        lax.fori_loop(0, 2, one_head, 0)

    for i in range(blocks):
        attend(i)
        att_ag.start(i)

    out_in.wait()
    down_in.wait()
    cot_in.wait()
    cot_ag.pass_on(0)
    cot_ag.pass_on(1)
    for k in range(2):
        cot_ag.wait_beside(k)
        cot_ag.wait_relay(k)

    def mlp(b, carry):
        for k in range(blocks):

            @pl.when(b == k)
            def _():
                att_ag.pass_on(k)
                att_ag.wait_beside(k)
                att_ag.wait_relay(k)

        at = rows(b * 256, 256, 256)
        a = [att[k, at, :].astype(F32) for k in range(PARTS)]
        ssq = sum(jnp.sum(v * v, axis=-1, keepdims=True) for v in a)
        scale = lax.rsqrt(ssq * (1.0 / D) + EPSILON)
        hidden = tok_g[at, :].astype(F32)
        for k in range(PARTS):
            g = gate[k, at, :].astype(F32)
            m = (a[k] * scale * (g * sigmoid(g))).astype(BF)
            mixed[k, at, :] = m
            hidden += dot(m, r["wout"][pl.ds(k * LOCAL, LOCAL), :])

        @pl.when(b == h)
        def _():
            r["hidden"][...] = hidden

        n2 = (hidden * rms_scale(hidden)).astype(BF)
        r["n2"][at, :] = n2
        g = dot(n2, r["wglu"][:, pl.ds(0, fp)])
        u = dot(n2, r["wglu"][:, pl.ds(fp, fp)])
        product = (g * u).astype(BF)
        r["product"][at, :] = product
        dp = dot_nt(cot_g[at, :], r["wdown"][...])
        dg = (dp * u).astype(BF)
        du = (dp * g).astype(BF)
        r["dpair"][at, pl.ds(0, fp)] = dg
        r["dpair"][at, pl.ds(fp, fp)] = du
        return carry

    def partials(b, carry):
        at = rows(b * 256, 256, 256)
        r["lo_part"][at, :] = dot(r["product"][at, :], r["wdown"][...]).astype(BF)
        r["dn_part"][at, :] = dot_nt(r["dpair"][at, :], r["wglu"][...]).astype(BF)
        return carry

    token_ag.drain()
    lax.fori_loop(0, blocks, mlp, 0)

    dn_rs = Scatter(ctx, r["dn_part"], r["dn_near"], r["dn_cross"], 24)
    lo_rs = Scatter(ctx, r["lo_part"], r["lo_near"], r["lo_cross"], 27)
    one_rs = Scatter(ctx, r["lo_part"], r["one_near"], r["one_cross"], 30)
    rings = [Ring(ctx, i, r["slots%d" % i]) for i in range(4)]

    base = sz.base[0]
    for j in range(fp // 256):
        size = min(256, fs - j * 256)
        g = dot_tn(r["product"][:, pl.ds(j * 256, 256)], cot_g[...]).astype(BF)
        for k in range(D // 128):
            f[pl.ds(base + k * fs + j * 256, size), :] = g[:size, k * 128 : (k + 1) * 128]
    rings[0].reduce_send(0, first=True)

    base_g = sz.base[1]
    full = sz.full_tiles

    def glu_grad(j, carry):
        g = dot_tn(r["n2"][:, rows(j * 256, 256, 256)], r["dpair"][...])
        for k in range(2):
            for i in range(full):
                at = rows(base_g + (k * full + i) * D + j * 256, 256, 16)
                first = k * fp + i * 128
                f[at, :] = g[:, first : first + 128].astype(BF)
        if part:
            a = g[:, full * 128 : full * 128 + 128]
            b = g[:, fp + full * 128 : fp + full * 128 + 128]
            at = rows(base_g + 2 * full * D + j * 256, 256, 16)
            f[at, :] = (a + pltpu.roll(b, part, 1)).astype(BF)
        return carry

    lax.fori_loop(0, D // 256, glu_grad, 0)
    rings[1].reduce_send(0, first=True)

    def low_block():
        dn_rs.wait()
        for i in range(tb // 128):
            at = pl.ds(i * 128, 128)
            v = r["hidden"][at, :]
            back = norm_back(v, rms_scale(v), dn_rs.result(i * 128, 128))
            d = cot_g[rows(h * tb + i * 128, 128, 128), :].astype(F32) + back
            r["dhid"][at, :] = d
            cot_g[rows(h * tb + i * 128, 128, 128), :] = d.astype(BF)
        low_ag.start(0)
        low_ag.start(1)

    def out_block():
        lo_rs.wait()
        for i in range(tb // 128):
            at = pl.ds(i * 128, 128)
            r["lo_cross"][at, :] = (r["hidden"][at, :] + lo_rs.result(i * 128, 128)).astype(BF)
        copy = pltpu.make_async_copy(r["lo_cross"], r["layer_out"], lsem.at[0])
        copy.start()
        return copy

    def low_arrive():
        for k in range(2):
            low_ag.pass_on(k)
        for k in range(2):
            low_ag.wait_beside(k)
            low_ag.wait_relay(k)

    own_out = pl.ds(pl.multiple_of(h * LOCAL, LOCAL), LOCAL)

    def mix_back(b, carry):
        at = rows(b * 256, 256, 256)
        low = cot_g[at, :]
        a = [att[k, at, :].astype(F32) for k in range(PARTS)]
        ssq = sum(jnp.sum(v * v, axis=-1, keepdims=True) for v in a)
        scale = lax.rsqrt(ssq * (1.0 / D) + EPSILON)
        inner = jnp.zeros((256, 1), F32)
        for k in range(PARTS):
            g = gate[k, at, :].astype(F32)
            e = dot_nt(low, r["wout"][pl.ds(k * LOCAL, LOCAL), :]) * (g * sigmoid(g))
            inner += jnp.sum(e * (a[k] * scale), axis=-1, keepdims=True)
        inner = inner * (1.0 / D)
        g = gate[h, at, :].astype(F32)
        sig = sigmoid(g)
        normed = att[h, at, :].astype(F32) * scale
        dm = dot_nt(low, r["wout"][own_out, :])
        slope = sig + g * sig * (1.0 - sig)
        r["dproj"][at, pl.ds(3 * LOCAL, LOCAL)] = (dm * normed * slope).astype(BF)
        r["datt"][at, :] = (scale * (dm * (g * sig) - normed * inner)).astype(BF)
        return carry

    base_r = sz.base[2]

    def out_grad():
        g = dot_tn(mixed[h], cot_g[...]).astype(BF)
        for k in range(D // 128):
            f[pl.ds(base_r + k * LOCAL, LOCAL), :] = g[:, k * 128 : (k + 1) * 128]

    def swish_slope(v):
        sig = sigmoid(v)
        return sig + v * sig * (1.0 - sig)

    def query_back(e, i):
        at = pl.ds(i * 256, 256)
        da = r["datt"][at, rows(e * HEAD_DIM, HEAD_DIM, HEAD_DIM)]
        total = jnp.zeros((256, 2 * HEAD_DIM), F32)
        for j in range(i + 1):
            near = pl.ds(j * 256, 256)
            v = r["raw"][near, rows(value_at + e * HEAD_DIM, HEAD_DIM, HEAD_DIM)]
            w = (dot_nt(da, v) * r["decay"][e, i - j]).astype(BF)
            r["weights"][at, near] = w
            total += dot(w, r["kpos"][e, near, :])
        lanes = rows(e * HEAD_DIM, HEAD_DIM, HEAD_DIM)
        co, si = r["cosine"][at, :], r["sine"][at, :]
        d = total[:, :HEAD_DIM] * co + total[:, HEAD_DIM:] * si
        raw = r["raw"][at, lanes].astype(F32)
        r["dproj"][at, lanes] = (d * swish_slope(raw)).astype(BF)

    def key_back(e, j):
        at = pl.ds(j * 256, 256)
        below = pl.ds(j * 256, t_all - j * 256)
        dk = dot_tn(r["weights"][below, at], r["qpos"][e, below, :])
        da = r["datt"][below, rows(e * HEAD_DIM, HEAD_DIM, HEAD_DIM)]
        dv = dot_tn(r["scores"][e, below, at], da)
        lanes = rows(LOCAL + e * HEAD_DIM, HEAD_DIM, HEAD_DIM)
        co, si = r["cosine"][at, :], r["sine"][at, :]
        d = dk[:, :HEAD_DIM] * co + dk[:, HEAD_DIM:] * si
        raw = r["raw"][at, lanes].astype(F32)
        r["dproj"][at, lanes] = (d * swish_slope(raw)).astype(BF)
        r["dproj"][at, rows(value_at + e * HEAD_DIM, HEAD_DIM, HEAD_DIM)] = dv.astype(BF)

    def head_back(e, carry):
        for i in range(blocks):
            query_back(e, i)
        for j in range(blocks):
            key_back(e, j)
        return carry

    base_q = base_r + (D // 128) * LOCAL

    def qkvu_grad(j, carry):
        g = dot_tn(r["n1"][:, rows(j * 256, 256, 256)], r["dproj"][...]).astype(BF)
        for k in range(D // 128):
            f[rows(base_q + k * D + j * 256, 256, 16), :] = g[:, k * 128 : (k + 1) * 128]
        return carry

    def one_part(b, carry):
        at = rows(b * 256, 256, 256)
        back = dot_nt(r["dproj"][at, pl.ds(0, 3 * LOCAL)], r["wqkv"][...])
        back += dot_nt(r["dproj"][at, pl.ds(3 * LOCAL, LOCAL)], r["wgate"][:, mine])
        r["lo_part"][at, :] = back.astype(BF)
        return carry

    own_tok = pltpu.make_async_copy(tok, r["weights"].at[pl.ds(0, tb), :], lsem.at[5])

    def last_block():
        one_rs.wait()
        own_tok.wait()
        for i in range(tb // 128):
            at = pl.ds(i * 128, 128)
            v = r["weights"][at, :].astype(F32)
            back = norm_back(v, rms_scale(v), one_rs.result(i * 128, 128))
            r["dhid"][at, :] = r["dhid"][at, :] + back
        copy = pltpu.make_async_copy(r["dhid"], r["grad_tokens"], lsem.at[1])
        copy.start()
        return copy

    def loop(lo, hi, body):
        lax.fori_loop(lo, hi, body, 0)

    def first_sums():
        loop(blocks // 2, blocks, partials)
        cot_ag.drain()
        dn_rs.start()
        lo_rs.start()

    def rest_sends():
        for ring in rings[2:]:
            ring.reduce_send(0, first=True)

    def input_sums():
        loop(0, blocks, one_part)
        one_rs.start()
        own_tok.start()

    outs = ctx.outs
    plan = {
        0: ((lambda: loop(0, blocks // 2, partials),), (first_sums,)),
        1: ((), (dn_rs.middle,)),
        3: ((), (low_block,)),
        6: ((low_arrive, lo_rs.middle), (lambda: loop(0, blocks, mix_back),)),
        7: (
            (out_grad, lambda: loop(0, 2, head_back)),
            (lambda: loop(0, D // 256, qkvu_grad), rest_sends),
        ),
        9: ((), (lambda: outs.append(out_block()), lo_rs.drain)),
        10: ((), (input_sums,)),
        11: ((), (one_rs.middle,)),
        13: ((), (lambda: outs.append(last_block()),)),
    }
    assert blocks == 4
    total = 2 * (seq - 1)
    if seq > 16:
        for slot in sorted(plan):
            for piece in plan[slot][0] + plan[slot][1]:
                piece()
        for ring in rings:
            ring.all_steps()
        copy = pltpu.make_async_copy(f, r["f_out"], lsem.at[2])
        copy.start()
        outs.append(copy)
    else:
        done = [0]

        def rest_step():
            if done[0] < total:
                for ring in rings[2:]:
                    ring.step(done[0])
                done[0] += 1

        for slot in range(max(total, max(plan) + 1)):
            for i in range(2):
                if slot > 7:
                    rest_step()
                if slot < total:
                    rings[i].step(slot)
                for piece in plan.get(slot, ((), ()))[i]:
                    piece()
        while done[0] < total:
            rest_step()

    for ag in (att_ag, low_ag):
        ag.drain()
    dn_rs.drain()
    one_rs.drain()
    for ring in rings:
        ring.drain()
    for copy in outs:
        copy.wait()


def main_call(sz, tokens, w_qkvu, w_out, w_glu, w_down, cotangent):
    any_spec = pl.BlockSpec(memory_space=pl.ANY)
    t, tb, fp, seq = sz.t, sz.tb, sz.fp, sz.seq
    scratch = dict(
        tok_g=pltpu.VMEM((t, D), BF),
        cot_g=pltpu.VMEM((t, D), BF),
        n1=pltpu.VMEM((t, D), BF),
        raw=pltpu.VMEM((t, 3 * LOCAL), BF),
        wqkv=pltpu.VMEM((D, 3 * LOCAL), BF),
        wgate=pltpu.VMEM((D, D), BF),
        wout=pltpu.VMEM((D, D), BF),
        wglu=pltpu.VMEM((D, 2 * fp), BF),
        wdown=pltpu.VMEM((fp, D), BF),
        qpos=pltpu.VMEM((2, t, 2 * HEAD_DIM), BF),
        kpos=pltpu.VMEM((2, t, 2 * HEAD_DIM), BF),
        scores=pltpu.VMEM((2, t, t), BF),
        weights=pltpu.VMEM((t, t), BF),
        decay=pltpu.VMEM((2, t // 256, 256, 256), F32),
        cosine=pltpu.VMEM((t, HEAD_DIM), F32),
        sine=pltpu.VMEM((t, HEAD_DIM), F32),
        att=pltpu.VMEM((PARTS, t, LOCAL), BF),
        gate=pltpu.VMEM((PARTS, t, LOCAL), BF),
        mixed=pltpu.VMEM((PARTS, t, LOCAL), BF),
        hidden=pltpu.VMEM((tb, D), F32),
        product=pltpu.VMEM((t, fp), BF),
        dpair=pltpu.VMEM((t, 2 * fp), BF),
        dn_part=pltpu.VMEM((t, D), BF),
        dn_near=pltpu.VMEM((2, tb, D), BF),
        dn_cross=pltpu.VMEM((tb, D), BF),
        lo_near=pltpu.VMEM((2, tb, D), BF),
        lo_cross=pltpu.VMEM((tb, D), BF),
        dhid=pltpu.VMEM((tb, D), F32),
        f=pltpu.VMEM((sz.total, 128), BF),
        slots0=pltpu.VMEM((2, seq - 1, sz.chunk[0], 128), BF),
        slots1=pltpu.VMEM((2, seq - 1, sz.chunk[1], 128), BF),
        slots2=pltpu.VMEM((2, seq - 1, sz.chunk[2], 128), BF),
        slots3=pltpu.VMEM((2, seq - 1, sz.chunk[3], 128), BF),
        gsend=pltpu.SemaphoreType.DMA((48,)),
        grecv=pltpu.SemaphoreType.DMA((48,)),
        rsend=pltpu.SemaphoreType.DMA((4, 2, 2 * (seq - 1))),
        rrecv=pltpu.SemaphoreType.DMA((4, 2, 2 * (seq - 1))),
        psem=pltpu.SemaphoreType.DMA((4, 2, min(seq, 16))),
        lsem=pltpu.SemaphoreType.DMA((24,)),
    )
    if seq > 16:
        for i in range(4):
            del scratch["slots%d" % i]
        scratch["slots"] = pltpu.VMEM((2, seq - 1, max(sz.chunk), 128), BF)
    assert 2 * fp >= D + LOCAL and tb == 256
    names = ["tok", "w_qkvu", "w_out", "w_glu", "w_down", "cot", "layer_out", "grad_tokens", "f_out"]
    names += list(scratch)

    def kernel(*refs):
        named = dict(zip(names, refs))
        named["n2"] = named["weights"]
        for i in range(4 if seq > 16 else 0):
            named["slots%d" % i] = named["slots"].at[:, :, pl.ds(0, sz.chunk[i]), :]
        named["lo_part"] = named["tok_g"]
        named["one_near"], named["one_cross"] = named["dn_near"], named["dn_cross"]
        named["dproj"] = named["dpair"].at[:, pl.ds(0, D)]
        named["datt"] = named["dpair"].at[:, pl.ds(D, LOCAL)]
        layer_kernel(sz, list(named), *named.values())

    return pl.pallas_call(
        kernel,
        name="layer",
        out_shape=(
            jax.ShapeDtypeStruct((tb, D), BF),
            jax.ShapeDtypeStruct((tb, D), F32),
            jax.ShapeDtypeStruct((sz.total, 128), BF),
        ),
        in_specs=[any_spec] * 6,
        out_specs=(any_spec,) * 3,
        scratch_shapes=list(scratch.values()),
        compiler_params=pltpu.CompilerParams(
            collective_id=0, has_side_effects=True, vmem_limit_bytes=67043328
        ),
    )(tokens, w_qkvu, w_out, w_glu, w_down, cotangent)


def unpack_kernel(sz, flat, lo_in, gt_in, lo_out, gt_out, qkvu, out, glu, down, *scratch):
    buf, lo_b, gt_b, qkvu_b, out_b, glu_b, down_b, sem = scratch
    fs, full = sz.fs, sz.full_tiles
    part = fs % 128
    count = [0]

    def start(src, dst):
        copy = pltpu.make_async_copy(src, dst, sem.at[count[0]])
        copy.start()
        count[0] += 1
        return copy

    def fetch(first, size):
        return start(flat.at[pl.ds(first, size), :], buf.at[pl.ds(first, size), :])

    def tile(first, size):
        return buf[pl.ds(first, size), :].astype(F32)

    base_g, base_o = sz.base[1], sz.base[2]
    base_q = base_o + (D // 128) * LOCAL
    half = full * D
    down_in = [fetch(k * 4 * fs, 4 * fs) for k in range(2)]
    glu_in = [fetch(base_g, half), fetch(base_g + 2 * half, D) if part else None]
    glu_in.append(fetch(base_g + half, half))
    out_in = fetch(base_o, (D // 128) * LOCAL)
    qkvu_in = [fetch(base_q + k * 2 * D, 2 * D) for k in range(4)]
    lo_copy, gt_copy = start(lo_in, lo_b), start(gt_in, gt_b)
    outs = []
    for k in range(2):
        down_in[k].wait()
        for i in range(4 * k, 4 * k + 4):
            down_b[:, pl.ds(i * 128, 128)] = tile(i * fs, fs)
        lanes = pl.ds(k * 512, 512)
        outs.append(start(down_b.at[:, lanes], down.at[:, lanes]))
    if part:
        glu_in[1].wait()
    for k in range(2):
        glu_in[2 * k].wait()
        for i in range(full):
            glu_b[k, :, pl.ds(i * 128, 128)] = tile(base_g + (k * full + i) * D, D)
        if part:
            both = tile(base_g + 2 * half, D)
            both = pltpu.roll(both, 128 - part, 1) if k else both
            glu_b[k, :, pl.ds(full * 128, part)] = both[:, :part]
        outs.append(start(glu_b.at[k], glu.at[k]))
    out_in.wait()
    for i in range(D // 128):
        out_b[:, pl.ds(i * 128, 128)] = tile(base_o + i * LOCAL, LOCAL)
    outs.append(start(out_b, out))
    for k in range(4):
        qkvu_in[k].wait()
        for i in range(2):
            qkvu_b[k, :, pl.ds(i * 128, 128)] = tile(base_q + (2 * k + i) * D, D)
        outs.append(start(qkvu_b.at[k], qkvu.at[k]))
    lo_copy.wait()
    outs.append(start(lo_b, lo_out))
    gt_copy.wait()
    outs.append(start(gt_b, gt_out))
    for copy in outs:
        copy.wait()


def unpack(sz, flat, layer_out, grad_tokens):
    any_spec = pl.BlockSpec(memory_space=pl.ANY)
    outs = (
        jax.ShapeDtypeStruct((sz.tb, D), BF),
        jax.ShapeDtypeStruct((sz.tb, D), F32),
        jax.ShapeDtypeStruct((4, D, LOCAL), F32),
        jax.ShapeDtypeStruct((LOCAL, D), F32),
        jax.ShapeDtypeStruct((2, D, sz.fs), F32),
        jax.ShapeDtypeStruct((sz.fs, D), F32),
    )
    return pl.pallas_call(
        functools.partial(unpack_kernel, sz),
        name="unpack",
        out_shape=outs,
        in_specs=[any_spec] * 3,
        out_specs=(any_spec,) * 6,
        scratch_shapes=[pltpu.VMEM((sz.total, 128), BF)]
        + [pltpu.VMEM(v.shape, v.dtype) for v in outs]
        + [pltpu.SemaphoreType.DMA((32,))],
        compiler_params=pltpu.CompilerParams(vmem_limit_bytes=48 << 20),
    )(flat, layer_out, grad_tokens)


def per_device(tokens, seq_lengths, w_qkvu, w_out, w_glu, w_down, cotangent):
    assert seq_lengths.shape == (1, 1) and lax.axis_size("head") == PARTS
    sz = Sizes(lax.axis_size("seq"), tokens.shape[0], w_down.shape[0])
    layer_out, grad_tokens, flat = main_call(sz, tokens, w_qkvu, w_out, w_glu, w_down, cotangent)
    return tuple(unpack(sz, flat, layer_out, grad_tokens))


def solution(mesh):
    return jax.shard_map(
        per_device,
        mesh=mesh,
        in_specs=(
            P(("seq", "head"), None),
            P("seq", None),
            P(),
            P(),
            P(),
            P(),
            P(("seq", "head"), None),
        ),
        out_specs=(
            P(("seq", "head"), None),
            P(("seq", "head"), None),
            P(None, None, "head"),
            P("head", None),
            P(None, None, "head"),
            P("head", None),
        ),
        check_vma=False,
    )
```

```python
import functools

import jax
import jax.numpy as jnp
from jax import lax
from jax.experimental import pallas as pl
from jax.experimental.pallas import tpu as pltpu
from jax.sharding import PartitionSpec as P

D = 1024
HEADS = 8
HEAD_DIM = 128
EPSILON = 1e-06
PARTS = 4
LOCAL = D // PARTS
BF = jnp.bfloat16
F32 = jnp.float32
MESH = pl.DeviceIdType.MESH


def dot(a, b):
    return lax.dot_general(a, b, (((1,), (0,)), ((), ())), preferred_element_type=F32)


def dot_nt(a, b):
    return lax.dot_general(a, b, (((1,), (1,)), ((), ())), preferred_element_type=F32)


def dot_tn(a, b):
    return lax.dot_general(a, b, (((0,), (0,)), ((), ())), preferred_element_type=F32)


def sigmoid(v):
    return 1.0 / (1.0 + jnp.exp(-v))


def rms_scale(v):
    return lax.rsqrt(jnp.mean(v * v, axis=-1, keepdims=True) + EPSILON)


def norm_back(v, scale, grad):
    normed = v * scale
    return scale * (grad - normed * jnp.mean(grad * normed, axis=-1, keepdims=True))


def round_up(n, m):
    return -(-n // m) * m


def rows(start, size, align):
    return pl.ds(pl.multiple_of(start, align), size)


class Sizes:
    def __init__(self, seq, block, ff):
        self.seq = seq
        self.tb = block
        self.t = block * PARTS
        self.fs = ff // PARTS
        self.fp = round_up(self.fs, 256)
        rest = (D // 128) * LOCAL + 4 * (LOCAL // 128) * D
        chunk = lambda n: round_up(-(-n // (2 * seq)), 16)
        self.chunk = [chunk((D // 128) * self.fs), chunk(2 * (D // 128) * self.fs), chunk(rest // 2)]
        self.chunk.append(chunk(rest - 2 * seq * self.chunk[2]))
        self.base = [2 * seq * sum(self.chunk[:i]) for i in range(5)]
        self.total = self.base[4]


class Gather:
    def __init__(self, ctx, count, own, place, first):
        self.ctx, self.count, self.own, self.place, self.first = ctx, count, own, place, first

    def copy(self, src, dst, index, target):
        c = self.ctx
        return pltpu.make_async_remote_copy(
            src_ref=src,
            dst_ref=dst,
            send_sem=c.gsend.at[index],
            recv_sem=c.grecv.at[index],
            device_id=(c.s, target),
            device_id_type=MESH,
        )

    def across(self, k):
        c = self.ctx
        return self.copy(self.own(k), self.place(c.h, k), self.first + 3 * k, c.yp)

    def beside(self, k):
        c = self.ctx
        return self.copy(self.own(k), self.place(c.h, k), self.first + 3 * k + 1, c.sib)

    def relay(self, k):
        c = self.ctx
        spot = self.place(c.yp, k)
        return self.copy(spot, spot, self.first + 3 * k + 2, c.sib)

    def start(self, k):
        self.across(k).start()
        self.beside(k).start()

    def pass_on(self, k):
        self.across(k).wait_recv()
        self.relay(k).start()

    def wait_beside(self, k):
        self.beside(k).wait_recv()

    def wait_relay(self, k):
        self.relay(k).wait_recv()

    def drain(self):
        for k in range(self.count):
            self.across(k).wait_send()
            self.beside(k).wait_send()
            self.relay(k).wait_send()


class Scatter:
    def __init__(self, ctx, part, near, cross, first):
        self.ctx, self.part, self.near, self.cross, self.first = ctx, part, near, cross, first
        self.tb = ctx.sz.tb

    def block(self, index):
        return self.part.at[rows(index * self.tb, self.tb, self.tb), :]

    def copy(self, src, dst, index, target):
        c = self.ctx
        return pltpu.make_async_remote_copy(
            src_ref=src,
            dst_ref=dst,
            send_sem=c.gsend.at[index],
            recv_sem=c.grecv.at[index],
            device_id=(c.s, target),
            device_id_type=MESH,
        )

    def beside(self, k):
        c = self.ctx
        return self.copy(self.block(2 * k + 1 - c.c), self.near.at[k], self.first + k, c.sib)

    def across(self):
        c = self.ctx
        return self.copy(self.block(c.yp), self.cross, self.first + 2, c.yp)

    def start(self):
        self.beside(0).start()
        self.beside(1).start()

    def middle(self):
        c = self.ctx
        self.beside(0).wait_recv()
        self.beside(1).wait_recv()
        there = self.block(c.yp)
        there[...] = (there[...].astype(F32) + self.near[1 - c.y].astype(F32)).astype(BF)
        self.across().start()

    def result(self, lo, size):
        c = self.ctx
        here = self.part[rows(c.h * self.tb + lo, size, size), :].astype(F32)
        at = pl.ds(lo, size)
        return here + self.near[c.y, at, :].astype(F32) + self.cross[at, :].astype(F32)

    def wait(self):
        self.across().wait_recv()

    def drain(self):
        self.beside(0).wait_send()
        self.beside(1).wait_send()
        self.across().wait_send()


class Ring:
    def __init__(self, ctx, index, slots):
        self.ctx, self.index, self.slots = ctx, index, slots
        self.base, self.chunk = ctx.sz.base[index], ctx.sz.chunk[index]
        self.n = ctx.sz.seq

    def mine(self, d, k):
        k = lax.rem(k, self.n)
        return rows(self.base + (2 * k + d) * self.chunk, self.chunk, 16)

    def copy(self, d, src, dst, step):
        c = self.ctx
        return pltpu.make_async_remote_copy(
            src_ref=src,
            dst_ref=dst,
            send_sem=c.rsend.at[self.index, d, step],
            recv_sem=c.rrecv.at[self.index, d, step],
            device_id=(c.right if d == 0 else c.left, c.h),
            device_id_type=MESH,
        )

    def toward(self, d, t):
        return self.ctx.p + (self.n - t if d == 0 else t)

    def publish(self, d, k, j):
        if self.n > 16:
            return
        at = self.mine(d, k)
        c = self.ctx
        copy = pltpu.make_async_copy(c.f.at[at, :], c.f_out.at[at, :], c.psem.at[self.index, d, j])
        copy.start()
        c.outs.append(copy)

    def reduce_copy(self, d, t, first=False):
        f = self.ctx.f
        src = f.at[self.mine(d, self.toward(d, t)), :] if first else self.slots.at[d, t - 1]
        return self.copy(d, src, self.slots.at[d, t], t)

    def reduce_send(self, t, first=False):
        for d in range(2):
            self.reduce_copy(d, t, first).start()

    def reduce_take(self, t, last=False):
        f = self.ctx.f
        pieces = 4 if self.chunk % 64 == 0 else (2 if self.chunk % 32 == 0 else 1)
        size = self.chunk // pieces
        for d in range(2):
            self.reduce_copy(d, t, first=True).wait_recv()
            k = lax.rem(self.toward(d, t) + (self.n - 1 if d == 0 else 1), self.n)
            start = self.base + (2 * k + d) * self.chunk
            for i in range(pieces):
                at = rows(start + i * size, size, 16)
                inside = pl.ds(i * size, size)
                total = f[at, :].astype(F32) + self.slots[d, t, inside, :].astype(F32)
                if last:
                    f[at, :] = total.astype(BF)
                else:
                    self.slots[d, t, inside, :] = total.astype(BF)
            if last:
                self.publish(d, k, self.n - 1)

    def spread_copy(self, d, t):
        spot = self.ctx.f.at[self.mine(d, self.toward(d, t) + (1 if d == 0 else self.n - 1)), :]
        return self.copy(d, spot, spot, self.n - 1 + t)

    def spread_send(self, t):
        for d in range(2):
            self.spread_copy(d, t).start()

    def spread_take(self, t):
        for d in range(2):
            self.spread_copy(d, t).wait_recv()
            if isinstance(t, int):
                self.publish(d, self.toward(d, t), t)

    def leave(self):
        for d in range(2):
            self.reduce_copy(d, 0, first=True).wait_send()

    def step(self, t):
        last = self.n - 2
        if t <= last:
            self.reduce_take(t, last=t == last)
            if t == 0:
                self.leave()
            if t < last:
                self.reduce_send(t + 1)
            else:
                self.spread_send(0)
        else:
            t -= self.n - 1
            self.spread_take(t)
            if t < last:
                self.spread_send(t + 1)

    def all_steps(self):
        last = self.n - 2

        def turn(t, carry):
            self.reduce_take(t)
            self.reduce_send(t + 1)
            return carry

        self.leave()
        lax.fori_loop(0, last, turn, 0)
        self.reduce_take(last, last=True)
        self.spread_send(0)

        def pass_on(t, carry):
            self.spread_take(t)
            self.spread_send(t + 1)
            return carry

        lax.fori_loop(0, last, pass_on, 0)
        self.spread_take(last)

    def drain(self):
        if self.n > 16:

            def one(t, carry):
                for d in range(2):
                    self.reduce_copy(d, t + 1, first=True).wait_send()
                    self.spread_copy(d, t).wait_send()
                return carry

            lax.fori_loop(0, self.n - 2, one, 0)
        else:
            for t in range(1, self.n - 1):
                for d in range(2):
                    self.reduce_copy(d, t, first=True).wait_send()
                    self.spread_copy(d, t - 1).wait_send()
        for d in range(2):
            self.spread_copy(d, self.n - 2).wait_send()


class Ctx:
    pass


def layer_kernel(sz, names, *refs):
    r = dict(zip(names, refs))
    ctx = Ctx()
    ctx.sz = sz
    seq, tb, t_all, fs, fp = sz.seq, sz.tb, sz.t, sz.fs, sz.fp
    half = seq // 2
    s, h = lax.axis_index("seq"), lax.axis_index("head")
    c, y = lax.rem(h, 2), h // 2
    z, x = s // 2, lax.rem(s, 2)
    pos = (1 - x) * z + x * (2 * half - 1 - z)

    def at_pos(p):
        q = p // half
        return (1 - q) * 2 * p + q * (2 * (2 * half - 1 - p) + 1)

    ctx.s, ctx.h, ctx.c, ctx.y, ctx.p = s, h, c, y, pos
    ctx.sib, ctx.yp = y * 2 + (1 - c), (1 - y) * 2 + c
    far = (1 - y) * 2 + (1 - c)
    ctx.right = at_pos(lax.rem(pos + 1, seq))
    ctx.left = at_pos(lax.rem(pos + seq - 1, seq))
    ctx.gsend, ctx.grecv = r["gsend"], r["grecv"]
    ctx.rsend, ctx.rrecv = r["rsend"], r["rrecv"]
    f = ctx.f = r["f"]
    ctx.f_out, ctx.psem, ctx.outs = r["f_out"], r["psem"], []
    lsem = r["lsem"]

    tok, cot, tok_g, cot_g = r["tok"], r["cot"], r["tok_g"], r["cot_g"]
    att, gate, mixed = r["att"], r["gate"], r["mixed"]

    loads = []

    def load(src, dst):
        copy = pltpu.make_async_copy(src, dst, lsem.at[len(loads)])
        copy.start()
        loads.append(copy)
        return copy

    mine = pl.ds(pl.multiple_of(h * LOCAL, LOCAL), LOCAL)
    own_rows = rows(h * tb, tb, tb)
    tok_in = load(tok, tok_g.at[own_rows, :])
    qkv_in = [
        load(r["w_qkvu"].at[k, :, mine], r["wqkv"].at[:, pl.ds(k * LOCAL, LOCAL)]) for k in range(3)
    ]
    gate_in = load(r["w_qkvu"].at[3], r["wgate"])
    out_in = load(r["w_out"], r["wout"])
    down_in = load(r["w_down"].at[rows(h * fs, fs, 64), :], r["wdown"].at[pl.ds(0, fs), :])
    glu_in = []
    window = y * (2 * fs) + c * (fs - fs % 128)
    tiles = fp // 128
    for k in range(2):
        for j in range(tiles):
            lane = pl.ds(pl.multiple_of(window + j * 128, 128), 128)
            glu_in.append(
                load(r["w_glu"].at[k, :, lane], f.at[pl.ds((k * tiles + j) * D, D), :])
            )
    cot_in = load(cot, cot_g.at[own_rows, :])

    barrier = pltpu.get_barrier_semaphore()
    for peer in ((s, ctx.sib), (s, ctx.yp), (ctx.right, h), (ctx.left, h)):
        pl.semaphore_signal(barrier, inc=1, device_id=peer, device_id_type=MESH)
    pl.semaphore_wait(barrier, 4)

    hb = tb // 2
    token_ag = Gather(
        ctx,
        2,
        lambda k: tok.at[pl.ds(k * hb, hb), :],
        lambda b, k: tok_g.at[rows(b * tb + k * hb, hb, hb), :],
        0,
    )
    cot_ag = Gather(
        ctx,
        2,
        lambda k: cot.at[pl.ds(k * hb, hb), :],
        lambda b, k: cot_g.at[rows(b * tb + k * hb, hb, hb), :],
        6,
    )
    blocks = t_all // 256
    att_place = lambda b, k: att.at[b, pl.ds(k * 256, 256), :]
    att_ag = Gather(ctx, blocks, lambda k: att_place(h, k), att_place, 33)
    low_place = lambda b, k: cot_g.at[rows(b * tb + k * hb, hb, hb), :]
    low_ag = Gather(ctx, 2, lambda k: low_place(h, k), low_place, 18)

    for k in range(2):
        token_ag.start(k)

    lane = lax.broadcasted_iota(jnp.int32, (32, HEAD_DIM), 1).astype(F32)
    step = lax.broadcasted_iota(jnp.int32, (32, HEAD_DIM), 0).astype(F32)
    frequency = jnp.exp(lane * (-9.210340371976184 / HEAD_DIM))
    fine = step * frequency
    coarse = (step * 32.0) * frequency
    cos_a, sin_a, cos_b, sin_b = jnp.cos(coarse), jnp.sin(coarse), jnp.cos(fine), jnp.sin(fine)
    for a in range(t_all // 32):
        at = pl.ds(a * 32, 32)
        ca, sa = cos_a[a : a + 1], sin_a[a : a + 1]
        r["cosine"][at, :] = ca * cos_b - sa * sin_b
        r["sine"][at, :] = sa * cos_b + ca * sin_b

    gap = lax.broadcasted_iota(jnp.int32, (256, 256), 0) - lax.broadcasted_iota(
        jnp.int32, (256, 256), 1
    )
    for e in range(2):
        slope = jnp.float32(0)
        for g in range(HEADS):
            slope = jnp.where(h * 2 + e == g, 2.0 ** (-8.0 * (g + 1) / HEADS), slope)
        for k in range(blocks):
            distance = gap + 256 * k
            value = jnp.exp(jnp.maximum(distance, 0).astype(F32) * -slope)
            r["decay"][e, k] = jnp.where(distance >= 0, value, 0.0)

    r["wdown"][pl.ds(fs, fp - fs), :] = jnp.zeros((fp - fs, D), BF)
    for one in glu_in:
        one.wait()
    part = fs % 128
    low_lanes = lax.broadcasted_iota(jnp.int32, (256, 128), 1) < 128 - part
    keep = lax.broadcasted_iota(jnp.int32, (256, 128), 1) < part if part else None

    def window_rows(n, carry):
        k, i = n // (D // 256), lax.rem(n, D // 256)
        first = k * tiles * D + i * 256
        tile = [f[rows(first + j * D, 256, 256), :].astype(F32) for j in range(tiles)]
        for j in range(tiles):
            value = tile[j]
            if part:
                straight = jnp.where(keep, value, 0.0) if j == tiles - 1 else value
                after = pltpu.roll(tile[j + 1], 128 - part, 1) if j < tiles - 1 else 0.0
                moved = jnp.where(low_lanes, pltpu.roll(value, 128 - part, 1), after)
                value = jnp.where(c == 1, moved, straight)
            lanes = pl.ds(pl.multiple_of(k * fp + j * 128, 128), 128)
            r["wglu"][rows(i * 256, 256, 256), lanes] = value.astype(BF)
        return carry

    lax.fori_loop(0, 2 * (D // 256), window_rows, 0)

    tok_in.wait()
    for one in qkv_in:
        one.wait()
    gate_in.wait()

    def project(b):
        at = rows(b * tb, tb, tb)
        v = tok_g[at, :].astype(F32)
        n1 = (v * rms_scale(v)).astype(BF)
        r["n1"][at, :] = n1
        qkv = dot(n1, r["wqkv"][...]).astype(BF)
        r["raw"][at, :] = qkv
        co, si = r["cosine"][at, :], r["sine"][at, :]
        for e in range(2):
            for name, first in (("qpos", 0), ("kpos", LOCAL)):
                w = qkv[:, first + e * HEAD_DIM : first + (e + 1) * HEAD_DIM].astype(F32)
                act = w * sigmoid(w)
                r[name][e, at, pl.ds(0, HEAD_DIM)] = (act * co).astype(BF)
                r[name][e, at, pl.ds(HEAD_DIM, HEAD_DIM)] = (act * si).astype(BF)
        for k in range(PARTS):
            gate[k, at, :] = dot(n1, r["wgate"][:, pl.ds(k * LOCAL, LOCAL)]).astype(BF)

    def project_turn(k, carry):
        @pl.when(k == 1)
        def _():
            for i in range(2):
                token_ag.wait_beside(i)

        @pl.when(k == 2)
        def _():
            for i in range(2):
                token_ag.pass_on(i)
            for i in range(2):
                cot_ag.start(i)

        @pl.when(k == 3)
        def _():
            for i in range(2):
                token_ag.wait_relay(i)

        yy = y + (k // 2) * (1 - 2 * y)
        cc = c + lax.rem(k, 2) * (1 - 2 * c)
        project(yy * 2 + cc)
        return carry

    lax.fori_loop(0, PARTS, project_turn, 0)

    value_at = 2 * LOCAL

    def attend(i):
        at = pl.ds(i * 256, 256)

        def one_head(e, carry):
            lanes = rows(value_at + e * HEAD_DIM, HEAD_DIM, HEAD_DIM)
            q = r["qpos"][e, at, :]
            total = jnp.zeros((256, HEAD_DIM), F32)
            for j in range(i + 1):
                near = pl.ds(j * 256, 256)
                scores = (dot_nt(q, r["kpos"][e, near, :]) * r["decay"][e, i - j]).astype(BF)
                r["scores"][e, at, near] = scores
                total += dot(scores, r["raw"][near, lanes])
            att[h, at, rows(e * HEAD_DIM, HEAD_DIM, HEAD_DIM)] = total.astype(BF)
            return carry

        lax.fori_loop(0, 2, one_head, 0)

    for i in range(blocks):
        attend(i)
        att_ag.start(i)

    out_in.wait()
    down_in.wait()
    cot_in.wait()
    cot_ag.pass_on(0)
    cot_ag.pass_on(1)
    for k in range(2):
        cot_ag.wait_beside(k)
        cot_ag.wait_relay(k)

    def mlp(b, carry):
        for k in range(blocks):

            @pl.when(b == k)
            def _():
                att_ag.pass_on(k)
                att_ag.wait_beside(k)
                att_ag.wait_relay(k)

        at = rows(b * 256, 256, 256)
        a = [att[k, at, :].astype(F32) for k in range(PARTS)]
        ssq = sum(jnp.sum(v * v, axis=-1, keepdims=True) for v in a)
        scale = lax.rsqrt(ssq * (1.0 / D) + EPSILON)
        hidden = tok_g[at, :].astype(F32)
        for k in range(PARTS):
            g = gate[k, at, :].astype(F32)
            m = (a[k] * scale * (g * sigmoid(g))).astype(BF)
            mixed[k, at, :] = m
            hidden += dot(m, r["wout"][pl.ds(k * LOCAL, LOCAL), :])

        @pl.when(b == h)
        def _():
            r["hidden"][...] = hidden

        n2 = (hidden * rms_scale(hidden)).astype(BF)
        r["n2"][at, :] = n2
        g = dot(n2, r["wglu"][:, pl.ds(0, fp)])
        u = dot(n2, r["wglu"][:, pl.ds(fp, fp)])
        product = (g * u).astype(BF)
        r["product"][at, :] = product
        dp = dot_nt(cot_g[at, :], r["wdown"][...])
        dg = (dp * u).astype(BF)
        du = (dp * g).astype(BF)
        r["dpair"][at, pl.ds(0, fp)] = dg
        r["dpair"][at, pl.ds(fp, fp)] = du
        return carry

    def partials(b, carry):
        at = rows(b * 256, 256, 256)
        r["lo_part"][at, :] = dot(r["product"][at, :], r["wdown"][...]).astype(BF)
        r["dn_part"][at, :] = dot_nt(r["dpair"][at, :], r["wglu"][...]).astype(BF)
        return carry

    token_ag.drain()
    lax.fori_loop(0, blocks, mlp, 0)

    dn_rs = Scatter(ctx, r["dn_part"], r["dn_near"], r["dn_cross"], 24)
    lo_rs = Scatter(ctx, r["lo_part"], r["lo_near"], r["lo_cross"], 27)
    one_rs = Scatter(ctx, r["lo_part"], r["one_near"], r["one_cross"], 30)
    rings = [Ring(ctx, i, r["slots%d" % i]) for i in range(4)]

    base = sz.base[0]
    for j in range(fp // 256):
        size = min(256, fs - j * 256)
        g = dot_tn(r["product"][:, pl.ds(j * 256, 256)], cot_g[...]).astype(BF)
        for k in range(D // 128):
            f[pl.ds(base + k * fs + j * 256, size), :] = g[:size, k * 128 : (k + 1) * 128]
    rings[0].reduce_send(0, first=True)

    base_g = sz.base[1]

    def glu_grad(k, carry):
        first = base_g + k * (D // 128) * fs
        for j in range(fp // 256):
            size = min(256, fs - j * 256)
            lanes = rows(k * fp + j * 256, 256, 256)
            g = dot_tn(r["dpair"][:, lanes], r["n2"][...]).astype(BF)
            for i in range(D // 128):
                at = rows(first + i * fs + j * 256, size, 16)
                f[at, :] = g[:size, i * 128 : (i + 1) * 128]
        return carry

    lax.fori_loop(0, 2, glu_grad, 0)
    rings[1].reduce_send(0, first=True)

    def low_block():
        dn_rs.wait()
        for i in range(tb // 128):
            at = pl.ds(i * 128, 128)
            v = r["hidden"][at, :]
            back = norm_back(v, rms_scale(v), dn_rs.result(i * 128, 128))
            d = cot_g[rows(h * tb + i * 128, 128, 128), :].astype(F32) + back
            r["dhid"][at, :] = d
            cot_g[rows(h * tb + i * 128, 128, 128), :] = d.astype(BF)
        low_ag.start(0)
        low_ag.start(1)

    def out_block():
        lo_rs.wait()
        for i in range(tb // 128):
            at = pl.ds(i * 128, 128)
            r["lo_cross"][at, :] = (r["hidden"][at, :] + lo_rs.result(i * 128, 128)).astype(BF)
        copy = pltpu.make_async_copy(r["lo_cross"], r["layer_out"], lsem.at[0])
        copy.start()
        return copy

    def low_arrive():
        for k in range(2):
            low_ag.pass_on(k)
        for k in range(2):
            low_ag.wait_beside(k)
            low_ag.wait_relay(k)

    own_out = pl.ds(pl.multiple_of(h * LOCAL, LOCAL), LOCAL)

    def mix_back(b, carry):
        at = rows(b * 256, 256, 256)
        low = cot_g[at, :]
        a = [att[k, at, :].astype(F32) for k in range(PARTS)]
        ssq = sum(jnp.sum(v * v, axis=-1, keepdims=True) for v in a)
        scale = lax.rsqrt(ssq * (1.0 / D) + EPSILON)
        inner = jnp.zeros((256, 1), F32)
        for k in range(PARTS):
            g = gate[k, at, :].astype(F32)
            e = dot_nt(low, r["wout"][pl.ds(k * LOCAL, LOCAL), :]) * (g * sigmoid(g))
            inner += jnp.sum(e * (a[k] * scale), axis=-1, keepdims=True)
        inner = inner * (1.0 / D)
        g = gate[h, at, :].astype(F32)
        sig = sigmoid(g)
        normed = att[h, at, :].astype(F32) * scale
        dm = dot_nt(low, r["wout"][own_out, :])
        slope = sig + g * sig * (1.0 - sig)
        r["dproj"][at, pl.ds(3 * LOCAL, LOCAL)] = (dm * normed * slope).astype(BF)
        r["datt"][at, :] = (scale * (dm * (g * sig) - normed * inner)).astype(BF)
        return carry

    base_r = sz.base[2]

    def out_grad():
        g = dot_tn(mixed[h], cot_g[...]).astype(BF)
        for k in range(D // 128):
            f[pl.ds(base_r + k * LOCAL, LOCAL), :] = g[:, k * 128 : (k + 1) * 128]

    def swish_slope(v):
        sig = sigmoid(v)
        return sig + v * sig * (1.0 - sig)

    def query_back(e, i):
        at = pl.ds(i * 256, 256)
        da = r["datt"][at, rows(e * HEAD_DIM, HEAD_DIM, HEAD_DIM)]
        total = jnp.zeros((256, 2 * HEAD_DIM), F32)
        for j in range(i + 1):
            near = pl.ds(j * 256, 256)
            v = r["raw"][near, rows(value_at + e * HEAD_DIM, HEAD_DIM, HEAD_DIM)]
            w = (dot_nt(da, v) * r["decay"][e, i - j]).astype(BF)
            r["weights"][at, near] = w
            total += dot(w, r["kpos"][e, near, :])
        lanes = rows(e * HEAD_DIM, HEAD_DIM, HEAD_DIM)
        co, si = r["cosine"][at, :], r["sine"][at, :]
        d = total[:, :HEAD_DIM] * co + total[:, HEAD_DIM:] * si
        raw = r["raw"][at, lanes].astype(F32)
        r["dproj"][at, lanes] = (d * swish_slope(raw)).astype(BF)

    def key_back(e, j):
        at = pl.ds(j * 256, 256)
        below = pl.ds(j * 256, t_all - j * 256)
        dk = dot_tn(r["weights"][below, at], r["qpos"][e, below, :])
        da = r["datt"][below, rows(e * HEAD_DIM, HEAD_DIM, HEAD_DIM)]
        dv = dot_tn(r["scores"][e, below, at], da)
        lanes = rows(LOCAL + e * HEAD_DIM, HEAD_DIM, HEAD_DIM)
        co, si = r["cosine"][at, :], r["sine"][at, :]
        d = dk[:, :HEAD_DIM] * co + dk[:, HEAD_DIM:] * si
        raw = r["raw"][at, lanes].astype(F32)
        r["dproj"][at, lanes] = (d * swish_slope(raw)).astype(BF)
        r["dproj"][at, rows(value_at + e * HEAD_DIM, HEAD_DIM, HEAD_DIM)] = dv.astype(BF)

    def head_back(e, carry):
        for i in range(blocks):
            query_back(e, i)
        for j in range(blocks):
            key_back(e, j)
        return carry

    base_q = base_r + (D // 128) * LOCAL

    def qkvu_grad(j, carry):
        g = dot_tn(r["n1"][:, rows(j * 256, 256, 256)], r["dproj"][...]).astype(BF)
        for k in range(D // 128):
            f[rows(base_q + k * D + j * 256, 256, 16), :] = g[:, k * 128 : (k + 1) * 128]
        return carry

    def one_part(b, carry):
        at = rows(b * 256, 256, 256)
        back = dot_nt(r["dproj"][at, pl.ds(0, 3 * LOCAL)], r["wqkv"][...])
        back += dot_nt(r["dproj"][at, pl.ds(3 * LOCAL, LOCAL)], r["wgate"][:, mine])
        r["lo_part"][at, :] = back.astype(BF)
        return carry

    own_tok = pltpu.make_async_copy(tok, r["weights"].at[pl.ds(0, tb), :], lsem.at[5])

    def last_block():
        one_rs.wait()
        own_tok.wait()
        for i in range(tb // 128):
            at = pl.ds(i * 128, 128)
            v = r["weights"][at, :].astype(F32)
            back = norm_back(v, rms_scale(v), one_rs.result(i * 128, 128))
            r["dhid"][at, :] = r["dhid"][at, :] + back
        copy = pltpu.make_async_copy(r["dhid"], r["grad_tokens"], lsem.at[1])
        copy.start()
        return copy

    def loop(lo, hi, body):
        lax.fori_loop(lo, hi, body, 0)

    def first_sums():
        loop(blocks // 2, blocks, partials)
        cot_ag.drain()
        dn_rs.start()
        lo_rs.start()

    def rest_sends():
        for ring in rings[2:]:
            ring.reduce_send(0, first=True)

    def input_sums():
        loop(0, blocks, one_part)
        one_rs.start()
        own_tok.start()

    outs = ctx.outs
    plan = {
        0: ((lambda: loop(0, blocks // 2, partials),), (first_sums,)),
        1: ((), (dn_rs.middle,)),
        3: ((), (low_block,)),
        6: ((low_arrive, lo_rs.middle), (lambda: loop(0, blocks, mix_back),)),
        7: (
            (out_grad, lambda: loop(0, 2, head_back)),
            (lambda: loop(0, D // 256, qkvu_grad), rest_sends),
        ),
        9: ((), (lambda: outs.append(out_block()), lo_rs.drain)),
        10: ((), (input_sums,)),
        11: ((), (one_rs.middle,)),
        13: ((), (lambda: outs.append(last_block()),)),
    }
    assert blocks == 4
    total = 2 * (seq - 1)
    if seq > 16:
        for slot in sorted(plan):
            for piece in plan[slot][0] + plan[slot][1]:
                piece()
        for ring in rings:
            ring.all_steps()
        copy = pltpu.make_async_copy(f, r["f_out"], lsem.at[2])
        copy.start()
        outs.append(copy)
    else:
        done = [0]

        def rest_step():
            if done[0] < total:
                for ring in rings[2:]:
                    ring.step(done[0])
                done[0] += 1

        for slot in range(max(total, max(plan) + 1)):
            for i in range(2):
                if slot > 7:
                    rest_step()
                if slot < total:
                    rings[i].step(slot)
                for piece in plan.get(slot, ((), ()))[i]:
                    piece()
        while done[0] < total:
            rest_step()

    for ag in (att_ag, low_ag):
        ag.drain()
    dn_rs.drain()
    one_rs.drain()
    for ring in rings:
        ring.drain()
    for copy in outs:
        copy.wait()


def main_call(sz, tokens, w_qkvu, w_out, w_glu, w_down, cotangent):
    any_spec = pl.BlockSpec(memory_space=pl.ANY)
    t, tb, fp, seq = sz.t, sz.tb, sz.fp, sz.seq
    scratch = dict(
        tok_g=pltpu.VMEM((t, D), BF),
        cot_g=pltpu.VMEM((t, D), BF),
        n1=pltpu.VMEM((t, D), BF),
        raw=pltpu.VMEM((t, 3 * LOCAL), BF),
        wqkv=pltpu.VMEM((D, 3 * LOCAL), BF),
        wgate=pltpu.VMEM((D, D), BF),
        wout=pltpu.VMEM((D, D), BF),
        wglu=pltpu.VMEM((D, 2 * fp), BF),
        wdown=pltpu.VMEM((fp, D), BF),
        qpos=pltpu.VMEM((2, t, 2 * HEAD_DIM), BF),
        kpos=pltpu.VMEM((2, t, 2 * HEAD_DIM), BF),
        scores=pltpu.VMEM((2, t, t), BF),
        weights=pltpu.VMEM((t, t), BF),
        decay=pltpu.VMEM((2, t // 256, 256, 256), F32),
        cosine=pltpu.VMEM((t, HEAD_DIM), F32),
        sine=pltpu.VMEM((t, HEAD_DIM), F32),
        att=pltpu.VMEM((PARTS, t, LOCAL), BF),
        gate=pltpu.VMEM((PARTS, t, LOCAL), BF),
        mixed=pltpu.VMEM((PARTS, t, LOCAL), BF),
        hidden=pltpu.VMEM((tb, D), F32),
        product=pltpu.VMEM((t, fp), BF),
        dpair=pltpu.VMEM((t, 2 * fp), BF),
        dn_part=pltpu.VMEM((t, D), BF),
        dn_near=pltpu.VMEM((2, tb, D), BF),
        dn_cross=pltpu.VMEM((tb, D), BF),
        lo_near=pltpu.VMEM((2, tb, D), BF),
        lo_cross=pltpu.VMEM((tb, D), BF),
        dhid=pltpu.VMEM((tb, D), F32),
        f=pltpu.VMEM((sz.total, 128), BF),
        slots0=pltpu.VMEM((2, seq - 1, sz.chunk[0], 128), BF),
        slots1=pltpu.VMEM((2, seq - 1, sz.chunk[1], 128), BF),
        slots2=pltpu.VMEM((2, seq - 1, sz.chunk[2], 128), BF),
        slots3=pltpu.VMEM((2, seq - 1, sz.chunk[3], 128), BF),
        gsend=pltpu.SemaphoreType.DMA((48,)),
        grecv=pltpu.SemaphoreType.DMA((48,)),
        rsend=pltpu.SemaphoreType.DMA((4, 2, 2 * (seq - 1))),
        rrecv=pltpu.SemaphoreType.DMA((4, 2, 2 * (seq - 1))),
        psem=pltpu.SemaphoreType.DMA((4, 2, min(seq, 16))),
        lsem=pltpu.SemaphoreType.DMA((24,)),
    )
    if seq > 16:
        for i in range(4):
            del scratch["slots%d" % i]
        scratch["slots"] = pltpu.VMEM((2, seq - 1, max(sz.chunk), 128), BF)
    assert 2 * fp >= D + LOCAL and tb == 256
    names = ["tok", "w_qkvu", "w_out", "w_glu", "w_down", "cot", "layer_out", "grad_tokens", "f_out"]
    names += list(scratch)

    def kernel(*refs):
        named = dict(zip(names, refs))
        named["n2"] = named["weights"]
        for i in range(4 if seq > 16 else 0):
            named["slots%d" % i] = named["slots"].at[:, :, pl.ds(0, sz.chunk[i]), :]
        named["lo_part"] = named["tok_g"]
        named["one_near"], named["one_cross"] = named["dn_near"], named["dn_cross"]
        named["dproj"] = named["dpair"].at[:, pl.ds(0, D)]
        named["datt"] = named["dpair"].at[:, pl.ds(D, LOCAL)]
        layer_kernel(sz, list(named), *named.values())

    return pl.pallas_call(
        kernel,
        name="layer",
        out_shape=(
            jax.ShapeDtypeStruct((tb, D), BF),
            jax.ShapeDtypeStruct((tb, D), F32),
            jax.ShapeDtypeStruct((sz.total, 128), BF),
        ),
        in_specs=[any_spec] * 6,
        out_specs=(any_spec,) * 3,
        scratch_shapes=list(scratch.values()),
        compiler_params=pltpu.CompilerParams(
            collective_id=0, has_side_effects=True, vmem_limit_bytes=67043328
        ),
    )(tokens, w_qkvu, w_out, w_glu, w_down, cotangent)


def unpack_kernel(sz, flat, lo_in, gt_in, lo_out, gt_out, qkvu, out, glu, down, *scratch):
    buf, lo_b, gt_b, qkvu_b, out_b, glu_b, down_b, sem = scratch
    fs = sz.fs
    count = [0]

    def start(src, dst):
        copy = pltpu.make_async_copy(src, dst, sem.at[count[0]])
        copy.start()
        count[0] += 1
        return copy

    def fetch(first, size):
        return start(flat.at[pl.ds(first, size), :], buf.at[pl.ds(first, size), :])

    def tile(first, size):
        return buf[pl.ds(first, size), :].astype(F32)

    base_g, base_o = sz.base[1], sz.base[2]
    base_q = base_o + (D // 128) * LOCAL
    half = (D // 128) * fs
    down_in = [fetch(k * 4 * fs, 4 * fs) for k in range(2)]
    glu_in = [fetch(base_g + k * half, half) for k in range(2)]
    out_in = fetch(base_o, (D // 128) * LOCAL)
    qkvu_in = [fetch(base_q + k * 2 * D, 2 * D) for k in range(4)]
    lo_copy, gt_copy = start(lo_in, lo_b), start(gt_in, gt_b)
    outs = []
    for k in range(2):
        down_in[k].wait()
        for i in range(4 * k, 4 * k + 4):
            down_b[:, pl.ds(i * 128, 128)] = tile(i * fs, fs)
        lanes = pl.ds(k * 512, 512)
        outs.append(start(down_b.at[:, lanes], down.at[:, lanes]))
    for k in range(2):
        glu_in[k].wait()
        for i in range(D // 128):
            glu_b[k, :, pl.ds(i * 128, 128)] = tile(base_g + k * half + i * fs, fs)
        outs.append(start(glu_b.at[k], glu.at[k]))
    out_in.wait()
    for i in range(D // 128):
        out_b[:, pl.ds(i * 128, 128)] = tile(base_o + i * LOCAL, LOCAL)
    outs.append(start(out_b, out))
    for k in range(4):
        qkvu_in[k].wait()
        for i in range(2):
            qkvu_b[k, :, pl.ds(i * 128, 128)] = tile(base_q + (2 * k + i) * D, D)
        outs.append(start(qkvu_b.at[k], qkvu.at[k]))
    lo_copy.wait()
    outs.append(start(lo_b, lo_out))
    gt_copy.wait()
    outs.append(start(gt_b, gt_out))
    for copy in outs:
        copy.wait()


def unpack(sz, flat, layer_out, grad_tokens):
    any_spec = pl.BlockSpec(memory_space=pl.ANY)
    outs = (
        jax.ShapeDtypeStruct((sz.tb, D), BF),
        jax.ShapeDtypeStruct((sz.tb, D), F32),
        jax.ShapeDtypeStruct((4, D, LOCAL), F32),
        jax.ShapeDtypeStruct((LOCAL, D), F32),
        jax.ShapeDtypeStruct((2, sz.fs, D), F32),
        jax.ShapeDtypeStruct((sz.fs, D), F32),
    )
    return pl.pallas_call(
        functools.partial(unpack_kernel, sz),
        name="unpack",
        out_shape=outs,
        in_specs=[any_spec] * 3,
        out_specs=(any_spec,) * 6,
        scratch_shapes=[pltpu.VMEM((sz.total, 128), BF)]
        + [pltpu.VMEM(v.shape, v.dtype) for v in outs]
        + [pltpu.SemaphoreType.DMA((32,))],
        compiler_params=pltpu.CompilerParams(vmem_limit_bytes=67043328),
    )(flat, layer_out, grad_tokens)


def per_device(tokens, seq_lengths, w_qkvu, w_out, w_glu, w_down, cotangent):
    assert seq_lengths.shape == (1, 1) and lax.axis_size("head") == PARTS
    sz = Sizes(lax.axis_size("seq"), tokens.shape[0], w_down.shape[0])
    layer_out, grad_tokens, flat = main_call(sz, tokens, w_qkvu, w_out, w_glu, w_down, cotangent)
    outs = list(unpack(sz, flat, layer_out, grad_tokens))
    outs[4] = outs[4].transpose(0, 2, 1)
    return tuple(outs)


def solution(mesh):
    return jax.shard_map(
        per_device,
        mesh=mesh,
        in_specs=(
            P(("seq", "head"), None),
            P("seq", None),
            P(),
            P(),
            P(),
            P(),
            P(("seq", "head"), None),
        ),
        out_specs=(
            P(("seq", "head"), None),
            P(("seq", "head"), None),
            P(None, None, "head"),
            P("head", None),
            P(None, None, "head"),
            P("head", None),
        ),
        check_vma=False,
    )
```

```python
import functools

import jax
import jax.numpy as jnp
from jax import lax
from jax.experimental import pallas as pl
from jax.experimental.pallas import tpu as pltpu
from jax.sharding import PartitionSpec as P

D = 1024
HEADS = 8
HEAD_DIM = 128
EPSILON = 1e-06
PARTS = 4
LOCAL = D // PARTS
BF = jnp.bfloat16
F32 = jnp.float32
MESH = pl.DeviceIdType.MESH


def dot(a, b):
    return lax.dot_general(a, b, (((1,), (0,)), ((), ())), preferred_element_type=F32)


def dot_nt(a, b):
    return lax.dot_general(a, b, (((1,), (1,)), ((), ())), preferred_element_type=F32)


def dot_tn(a, b):
    return lax.dot_general(a, b, (((0,), (0,)), ((), ())), preferred_element_type=F32)


def sigmoid(v):
    return 1.0 / (1.0 + jnp.exp(-v))


def rms_scale(v):
    return lax.rsqrt(jnp.mean(v * v, axis=-1, keepdims=True) + EPSILON)


def norm_back(v, scale, grad):
    normed = v * scale
    return scale * (grad - normed * jnp.mean(grad * normed, axis=-1, keepdims=True))


def round_up(n, m):
    return -(-n // m) * m


def rows(start, size, align):
    return pl.ds(pl.multiple_of(start, align), size)


class Sizes:
    def __init__(self, seq, block, ff):
        self.seq = seq
        self.tb = block
        self.t = block * PARTS
        self.fs = ff // PARTS
        self.fp = round_up(self.fs, 256)
        rest = (D // 128) * LOCAL + 4 * (LOCAL // 128) * D
        chunk = lambda n: round_up(-(-n // (2 * seq)), 16)
        self.chunk = [chunk((D // 128) * self.fs)] * 3 + [chunk(rest // 2)]
        self.chunk.append(chunk(rest - 2 * seq * self.chunk[3]))
        self.base = [2 * seq * sum(self.chunk[:i]) for i in range(6)]
        self.total = self.base[5]


class Gather:
    def __init__(self, ctx, count, own, place, first):
        self.ctx, self.count, self.own, self.place, self.first = ctx, count, own, place, first

    def copy(self, src, dst, index, target):
        c = self.ctx
        return pltpu.make_async_remote_copy(
            src_ref=src,
            dst_ref=dst,
            send_sem=c.gsend.at[index],
            recv_sem=c.grecv.at[index],
            device_id=(c.s, target),
            device_id_type=MESH,
        )

    def across(self, k):
        c = self.ctx
        return self.copy(self.own(k), self.place(c.h, k), self.first + 3 * k, c.yp)

    def beside(self, k):
        c = self.ctx
        return self.copy(self.own(k), self.place(c.h, k), self.first + 3 * k + 1, c.sib)

    def relay(self, k):
        c = self.ctx
        spot = self.place(c.yp, k)
        return self.copy(spot, spot, self.first + 3 * k + 2, c.sib)

    def start(self, k):
        self.across(k).start()
        self.beside(k).start()

    def pass_on(self, k):
        self.across(k).wait_recv()
        self.relay(k).start()

    def wait_beside(self, k):
        self.beside(k).wait_recv()

    def wait_relay(self, k):
        self.relay(k).wait_recv()

    def drain(self):
        for k in range(self.count):
            self.across(k).wait_send()
            self.beside(k).wait_send()
            self.relay(k).wait_send()


class Scatter:
    def __init__(self, ctx, part, near, cross, first):
        self.ctx, self.part, self.near, self.cross, self.first = ctx, part, near, cross, first
        self.tb = ctx.sz.tb

    def block(self, index):
        return self.part.at[rows(index * self.tb, self.tb, self.tb), :]

    def copy(self, src, dst, index, target):
        c = self.ctx
        return pltpu.make_async_remote_copy(
            src_ref=src,
            dst_ref=dst,
            send_sem=c.gsend.at[index],
            recv_sem=c.grecv.at[index],
            device_id=(c.s, target),
            device_id_type=MESH,
        )

    def beside(self, k):
        c = self.ctx
        return self.copy(self.block(2 * k + 1 - c.c), self.near.at[k], self.first + k, c.sib)

    def across(self):
        c = self.ctx
        return self.copy(self.block(c.yp), self.cross, self.first + 2, c.yp)

    def start(self):
        self.beside(0).start()
        self.beside(1).start()

    def middle(self):
        c = self.ctx
        self.beside(0).wait_recv()
        self.beside(1).wait_recv()
        there = self.block(c.yp)
        there[...] = (there[...].astype(F32) + self.near[1 - c.y].astype(F32)).astype(BF)
        self.across().start()

    def result(self, lo, size):
        c = self.ctx
        here = self.part[rows(c.h * self.tb + lo, size, size), :].astype(F32)
        at = pl.ds(lo, size)
        return here + self.near[c.y, at, :].astype(F32) + self.cross[at, :].astype(F32)

    def wait(self):
        self.across().wait_recv()

    def drain(self):
        self.beside(0).wait_send()
        self.beside(1).wait_send()
        self.across().wait_send()


class Ring:
    def __init__(self, ctx, index, slots):
        self.ctx, self.index, self.slots = ctx, index, slots
        self.base, self.chunk = ctx.sz.base[index], ctx.sz.chunk[index]
        self.n = ctx.sz.seq

    def mine(self, d, k):
        k = lax.rem(k, self.n)
        return rows(self.base + (2 * k + d) * self.chunk, self.chunk, 16)

    def copy(self, d, src, dst, step):
        c = self.ctx
        return pltpu.make_async_remote_copy(
            src_ref=src,
            dst_ref=dst,
            send_sem=c.rsend.at[self.index, d, lax.rem(step, 2)],
            recv_sem=c.rrecv.at[self.index, d, lax.rem(step, 2)],
            device_id=(c.right if d == 0 else c.left, c.h),
            device_id_type=MESH,
        )

    def toward(self, d, t):
        return self.ctx.p + (self.n - t if d == 0 else t)

    def publish(self, d, k):
        if self.n > 16:
            return
        at = self.mine(d, k)
        c = self.ctx
        pltpu.make_async_copy(c.f.at[at, :], c.f_out.at[at, :], c.psem.at[0]).start()

    def reduce_copy(self, d, t, first=False):
        f = self.ctx.f
        src = f.at[self.mine(d, self.toward(d, t)), :] if first else self.slots.at[d, t - 1]
        return self.copy(d, src, self.slots.at[d, t], t)

    def reduce_send(self, t, first=False):
        for d in range(2):
            self.reduce_copy(d, t, first).start()

    def reduce_take(self, t, last=False):
        f = self.ctx.f
        pieces = 4 if self.chunk % 64 == 0 else (2 if self.chunk % 32 == 0 else 1)
        size = self.chunk // pieces
        for d in range(2):
            self.reduce_copy(d, t, first=True).wait_recv()
            k = lax.rem(self.toward(d, t) + (self.n - 1 if d == 0 else 1), self.n)
            start = self.base + (2 * k + d) * self.chunk
            for i in range(pieces):
                at = rows(start + i * size, size, 16)
                inside = pl.ds(i * size, size)
                total = f[at, :].astype(F32) + self.slots[d, t, inside, :].astype(F32)
                if last:
                    f[at, :] = total.astype(BF)
                else:
                    self.slots[d, t, inside, :] = total.astype(BF)
            if last:
                self.publish(d, k)

    def spread_copy(self, d, t):
        spot = self.ctx.f.at[self.mine(d, self.toward(d, t) + (1 if d == 0 else self.n - 1)), :]
        return self.copy(d, spot, spot, self.n - 1 + t)

    def spread_send(self, t):
        for d in range(2):
            self.spread_copy(d, t).start()

    def spread_take(self, t):
        for d in range(2):
            self.spread_copy(d, t).wait_recv()
            if isinstance(t, int):
                self.publish(d, self.toward(d, t))

    def left(self, step):
        for d in range(2):
            if isinstance(step, int) and step >= self.n - 1:
                self.spread_copy(d, step - self.n + 1).wait_send()
            else:
                self.reduce_copy(d, step, first=True).wait_send()

    def step(self, t):
        last = self.n - 2
        if t <= last:
            self.reduce_take(t, last=t == last)
        else:
            self.spread_take(t - self.n + 1)
        if t > 0:
            self.left(t - 1)
        if t < last:
            self.reduce_send(t + 1)
        elif t < 2 * last + 1:
            self.spread_send(t - last)

    def all_steps(self):
        last = self.n - 2
        self.step(0)

        def turn(t, carry):
            self.reduce_take(t)
            self.left(t - 1)
            self.reduce_send(t + 1)
            return carry

        lax.fori_loop(1, last, turn, 0)
        self.step(last)

        def pass_on(t, carry):
            self.spread_take(t)
            self.left(last + t)
            self.spread_send(t + 1)
            return carry

        lax.fori_loop(0, last, pass_on, 0)
        self.step(2 * last + 1)

    def drain(self):
        self.left(2 * self.n - 3)


class Ctx:
    pass


def layer_kernel(sz, names, *refs):
    r = dict(zip(names, refs))
    ctx = Ctx()
    ctx.sz = sz
    seq, tb, t_all, fs, fp = sz.seq, sz.tb, sz.t, sz.fs, sz.fp
    half = seq // 2
    s, h = lax.axis_index("seq"), lax.axis_index("head")
    c, y = lax.rem(h, 2), h // 2
    z, x = s // 2, lax.rem(s, 2)
    pos = (1 - x) * z + x * (2 * half - 1 - z)

    def at_pos(p):
        q = p // half
        return (1 - q) * 2 * p + q * (2 * (2 * half - 1 - p) + 1)

    ctx.s, ctx.h, ctx.c, ctx.y, ctx.p = s, h, c, y, pos
    ctx.sib, ctx.yp = y * 2 + (1 - c), (1 - y) * 2 + c
    far = (1 - y) * 2 + (1 - c)
    ctx.right = at_pos(lax.rem(pos + 1, seq))
    ctx.left = at_pos(lax.rem(pos + seq - 1, seq))
    ctx.gsend, ctx.grecv = r["gsend"], r["grecv"]
    ctx.rsend, ctx.rrecv = r["rsend"], r["rrecv"]
    f = ctx.f = r["f"]
    ctx.f_out, ctx.psem, ctx.outs = r["f_out"], r["psem"], []
    lsem = r["lsem"]

    tok, cot, tok_g, cot_g = r["tok"], r["cot"], r["tok_g"], r["cot_g"]
    att, gate, mixed = r["att"], r["gate"], r["mixed"]

    loads = []

    def load(src, dst):
        copy = pltpu.make_async_copy(src, dst, lsem.at[len(loads)])
        copy.start()
        loads.append(copy)
        return copy

    barrier = pltpu.get_barrier_semaphore()
    for peer in ((s, ctx.sib), (s, ctx.yp), (ctx.right, h), (ctx.left, h)):
        pl.semaphore_signal(barrier, inc=1, device_id=peer, device_id_type=MESH)

    mine = pl.ds(pl.multiple_of(h * LOCAL, LOCAL), LOCAL)
    own_rows = rows(h * tb, tb, tb)
    tok_in = load(tok, tok_g.at[own_rows, :])
    qkv_in = [
        load(r["w_qkvu"].at[k, :, mine], r["wqkv"].at[:, pl.ds(k * LOCAL, LOCAL)]) for k in range(3)
    ]
    gate_in = load(r["w_qkvu"].at[3], r["wgate"])
    out_in = load(r["w_out"], r["wout"])
    down_in = load(r["w_down"].at[rows(h * fs, fs, 64), :], r["wdown"].at[pl.ds(0, fs), :])
    window = y * (2 * fs) + c * (fs - fs % 128)
    tiles = fp // 128
    for k in range(2):
        for j in range(tiles):
            lane = pl.ds(pl.multiple_of(window + j * 128, 128), 128)
            staged = f.at[pl.ds((k * tiles + j) * D, D), :]
            pltpu.make_async_copy(r["w_glu"].at[k, :, lane], staged, lsem.at[8]).start()
    cot_in = load(cot, cot_g.at[own_rows, :])

    pl.semaphore_wait(barrier, 4)

    hb = tb // 2
    token_ag = Gather(
        ctx,
        2,
        lambda k: tok.at[pl.ds(k * hb, hb), :],
        lambda b, k: tok_g.at[rows(b * tb + k * hb, hb, hb), :],
        0,
    )
    cot_ag = Gather(
        ctx,
        2,
        lambda k: cot.at[pl.ds(k * hb, hb), :],
        lambda b, k: cot_g.at[rows(b * tb + k * hb, hb, hb), :],
        6,
    )
    blocks = t_all // 256
    att_place = lambda b, k: att.at[b, pl.ds(k * 256, 256), :]
    att_ag = Gather(ctx, blocks, lambda k: att_place(h, k), att_place, 18)
    low_place = lambda b, k: cot_g.at[rows(b * tb + k * hb, hb, hb), :]
    low_ag = Gather(ctx, 2, lambda k: low_place(h, k), low_place, 0)

    for ag in (token_ag, cot_ag):
        for k in range(2):
            ag.start(k)

    lane = lax.broadcasted_iota(jnp.int32, (32, HEAD_DIM), 1).astype(F32)
    step = lax.broadcasted_iota(jnp.int32, (32, HEAD_DIM), 0).astype(F32)
    frequency = jnp.exp(lane * (-9.210340371976184 / HEAD_DIM))
    fine = step * frequency
    coarse = (step * 32.0) * frequency
    cos_a, sin_a, cos_b, sin_b = jnp.cos(coarse), jnp.sin(coarse), jnp.cos(fine), jnp.sin(fine)
    for a in range(t_all // 32):
        at = pl.ds(a * 32, 32)
        ca, sa = cos_a[a : a + 1], sin_a[a : a + 1]
        r["cosine"][at, :] = ca * cos_b - sa * sin_b
        r["sine"][at, :] = sa * cos_b + ca * sin_b

    gap = lax.broadcasted_iota(jnp.int32, (256, 256), 0) - lax.broadcasted_iota(
        jnp.int32, (256, 256), 1
    )
    for e in range(2):
        slope = jnp.float32(0)
        for g in range(HEADS):
            slope = jnp.where(h * 2 + e == g, 2.0 ** (-8.0 * (g + 1) / HEADS), slope)
        for k in range(blocks):
            distance = gap + 256 * k
            value = jnp.exp(jnp.maximum(distance, 0).astype(F32) * -slope)
            r["decay"][e, k] = jnp.where(distance >= 0, value, 0.0)

    r["wdown"][pl.ds(fs, fp - fs), :] = jnp.zeros((fp - fs, D), BF)
    staged = f.at[pl.ds(0, 2 * tiles * D), :]
    pltpu.make_async_copy(staged, staged, lsem.at[8]).wait()
    part = fs % 128
    low_lanes = lax.broadcasted_iota(jnp.int32, (256, 128), 1) < 128 - part
    keep = lax.broadcasted_iota(jnp.int32, (256, 128), 1) < part if part else None

    def window_rows(n, carry):
        k, i = n // (D // 256), lax.rem(n, D // 256)
        first = k * tiles * D + i * 256
        tile = [f[rows(first + j * D, 256, 256), :].astype(F32) for j in range(tiles)]
        for j in range(tiles):
            value = tile[j]
            if part:
                straight = jnp.where(keep, value, 0.0) if j == tiles - 1 else value
                after = pltpu.roll(tile[j + 1], 128 - part, 1) if j < tiles - 1 else 0.0
                moved = jnp.where(low_lanes, pltpu.roll(value, 128 - part, 1), after)
                value = jnp.where(c == 1, moved, straight)
            lanes = pl.ds(pl.multiple_of(k * fp + j * 128, 128), 128)
            r["wglu"][rows(i * 256, 256, 256), lanes] = value.astype(BF)
        return carry

    lax.fori_loop(0, 2 * (D // 256), window_rows, 0)

    tok_in.wait()
    for one in qkv_in:
        one.wait()
    gate_in.wait()

    def project(b):
        at = rows(b * tb, tb, tb)
        v = tok_g[at, :].astype(F32)
        n1 = (v * rms_scale(v)).astype(BF)
        r["n1"][at, :] = n1
        qkv = dot(n1, r["wqkv"][...]).astype(BF)
        r["raw"][at, :] = qkv
        co, si = r["cosine"][at, :], r["sine"][at, :]
        for e in range(2):
            for name, first in (("qpos", 0), ("kpos", LOCAL)):
                w = qkv[:, first + e * HEAD_DIM : first + (e + 1) * HEAD_DIM].astype(F32)
                act = w * sigmoid(w)
                r[name][e, at, pl.ds(0, HEAD_DIM)] = (act * co).astype(BF)
                r[name][e, at, pl.ds(HEAD_DIM, HEAD_DIM)] = (act * si).astype(BF)
        for k in range(PARTS):
            gate[k, at, :] = dot(n1, r["wgate"][:, pl.ds(k * LOCAL, LOCAL)]).astype(BF)

    def project_turn(k, carry):
        @pl.when(k == 1)
        def _():
            for i in range(2):
                token_ag.wait_beside(i)

        @pl.when(k == 2)
        def _():
            for i in range(2):
                token_ag.pass_on(i)

        @pl.when(k == 3)
        def _():
            for i in range(2):
                token_ag.wait_relay(i)

        yy = y + (k // 2) * (1 - 2 * y)
        cc = c + lax.rem(k, 2) * (1 - 2 * c)
        project(yy * 2 + cc)
        return carry

    lax.fori_loop(0, PARTS, project_turn, 0)

    value_at = 2 * LOCAL

    def attend(i):
        at = pl.ds(i * 256, 256)

        def one_head(e, carry):
            lanes = rows(value_at + e * HEAD_DIM, HEAD_DIM, HEAD_DIM)
            q = r["qpos"][e, at, :]
            total = jnp.zeros((256, HEAD_DIM), F32)
            for j in range(i + 1):
                near = pl.ds(j * 256, 256)
                scores = (dot_nt(q, r["kpos"][e, near, :]) * r["decay"][e, i - j]).astype(BF)
                r["scores"][e, at, near] = scores
                total += dot(scores, r["raw"][near, lanes])
            att[h, at, rows(e * HEAD_DIM, HEAD_DIM, HEAD_DIM)] = total.astype(BF)
            return carry

        lax.fori_loop(0, 2, one_head, 0)

    for i in range(blocks):
        attend(i)
        att_ag.start(i)

    out_in.wait()
    down_in.wait()
    cot_in.wait()
    cot_ag.pass_on(0)
    cot_ag.pass_on(1)
    for k in range(2):
        cot_ag.wait_beside(k)
        cot_ag.wait_relay(k)

    def mlp(b, carry):
        for k in range(blocks):

            @pl.when(b == k)
            def _():
                if k + 1 < blocks:
                    att_ag.pass_on(k + 1)
                att_ag.wait_beside(k)
                att_ag.wait_relay(k)

        at = rows(b * 256, 256, 256)
        a = [att[k, at, :].astype(F32) for k in range(PARTS)]
        ssq = sum(jnp.sum(v * v, axis=-1, keepdims=True) for v in a)
        scale = lax.rsqrt(ssq * (1.0 / D) + EPSILON)
        hidden = tok_g[at, :].astype(F32)
        for k in range(PARTS):
            g = gate[k, at, :].astype(F32)
            m = (a[k] * scale * (g * sigmoid(g))).astype(BF)
            mixed[k, at, :] = m
            hidden += dot(m, r["wout"][pl.ds(k * LOCAL, LOCAL), :])

        @pl.when(b == h)
        def _():
            r["hidden"][...] = hidden

        n2 = (hidden * rms_scale(hidden)).astype(BF)
        r["n2"][at, :] = n2
        g = dot(n2, r["wglu"][:, pl.ds(0, fp)])
        u = dot(n2, r["wglu"][:, pl.ds(fp, fp)])
        product = (g * u).astype(BF)
        r["product"][at, :] = product
        dp = dot_nt(cot_g[at, :], r["wdown"][...])
        dg = (dp * u).astype(BF)
        du = (dp * g).astype(BF)
        r["dpair"][at, pl.ds(0, fp)] = dg
        r["dpair"][at, pl.ds(fp, fp)] = du
        return carry

    def partials(b, carry):
        at = rows(b * 256, 256, 256)
        r["lo_part"][at, :] = dot(r["product"][at, :], r["wdown"][...]).astype(BF)
        r["dn_part"][at, :] = dot_nt(r["dpair"][at, :], r["wglu"][...]).astype(BF)
        return carry

    token_ag.drain()
    att_ag.pass_on(0)
    lax.fori_loop(0, blocks, mlp, 0)

    dn_rs = Scatter(ctx, r["dn_part"], r["dn_near"], r["dn_cross"], 12)
    lo_rs = Scatter(ctx, r["lo_part"], r["lo_near"], r["lo_cross"], 15)
    one_rs = Scatter(ctx, r["lo_part"], r["one_near"], r["one_cross"], 12)
    rings = [Ring(ctx, i, r["slots%d" % i]) for i in range(5)]

    base = sz.base[0]
    for j in range(fp // 256):
        size = min(256, fs - j * 256)
        g = dot_tn(r["product"][:, pl.ds(j * 256, 256)], cot_g[...]).astype(BF)
        for k in range(D // 128):
            f[pl.ds(base + k * fs + j * 256, size), :] = g[:size, k * 128 : (k + 1) * 128]
    rings[0].reduce_send(0, first=True)

    def glu_grad(k):
        first = sz.base[1 + k]
        for j in range(fp // 256):
            size = min(256, fs - j * 256)
            lanes = rows(k * fp + j * 256, 256, 256)
            g = dot_tn(r["dpair"][:, lanes], r["n2"][...]).astype(BF)
            for i in range(D // 128):
                at = rows(first + i * fs + j * 256, size, 16)
                f[at, :] = g[:size, i * 128 : (i + 1) * 128]
        rings[1 + k].reduce_send(0, first=True)

    for k in range(2):
        glu_grad(k)

    def low_block():
        dn_rs.wait()
        for i in range(tb // 128):
            at = pl.ds(i * 128, 128)
            v = r["hidden"][at, :]
            back = norm_back(v, rms_scale(v), dn_rs.result(i * 128, 128))
            d = cot_g[rows(h * tb + i * 128, 128, 128), :].astype(F32) + back
            r["dhid"][at, :] = d
            cot_g[rows(h * tb + i * 128, 128, 128), :] = d.astype(BF)
        low_ag.start(0)
        low_ag.start(1)

    def out_block():
        lo_rs.wait()
        for i in range(tb // 128):
            at = pl.ds(i * 128, 128)
            r["lo_cross"][at, :] = (r["hidden"][at, :] + lo_rs.result(i * 128, 128)).astype(BF)
        copy = pltpu.make_async_copy(r["lo_cross"], r["layer_out"], lsem.at[0])
        copy.start()
        return copy

    def low_arrive():
        for k in range(2):
            low_ag.pass_on(k)
        for k in range(2):
            low_ag.wait_beside(k)
            low_ag.wait_relay(k)

    own_out = pl.ds(pl.multiple_of(h * LOCAL, LOCAL), LOCAL)

    def mix_back(b, carry):
        at = rows(b * 256, 256, 256)
        low = cot_g[at, :]
        a = [att[k, at, :].astype(F32) for k in range(PARTS)]
        ssq = sum(jnp.sum(v * v, axis=-1, keepdims=True) for v in a)
        scale = lax.rsqrt(ssq * (1.0 / D) + EPSILON)
        inner = jnp.zeros((256, 1), F32)
        for k in range(PARTS):
            g = gate[k, at, :].astype(F32)
            e = dot_nt(low, r["wout"][pl.ds(k * LOCAL, LOCAL), :]) * (g * sigmoid(g))
            inner += jnp.sum(e * (a[k] * scale), axis=-1, keepdims=True)
        inner = inner * (1.0 / D)
        g = gate[h, at, :].astype(F32)
        sig = sigmoid(g)
        normed = att[h, at, :].astype(F32) * scale
        dm = dot_nt(low, r["wout"][own_out, :])
        slope = sig + g * sig * (1.0 - sig)
        r["dproj"][at, pl.ds(3 * LOCAL, LOCAL)] = (dm * normed * slope).astype(BF)
        r["datt"][at, :] = (scale * (dm * (g * sig) - normed * inner)).astype(BF)
        return carry

    base_r = sz.base[3]

    def out_grad():
        g = dot_tn(mixed[h], cot_g[...]).astype(BF)
        for k in range(D // 128):
            f[pl.ds(base_r + k * LOCAL, LOCAL), :] = g[:, k * 128 : (k + 1) * 128]

    def swish_slope(v):
        sig = sigmoid(v)
        return sig + v * sig * (1.0 - sig)

    def query_back(e, i):
        at = pl.ds(i * 256, 256)
        da = r["datt"][at, rows(e * HEAD_DIM, HEAD_DIM, HEAD_DIM)]
        total = jnp.zeros((256, 2 * HEAD_DIM), F32)
        for j in range(i + 1):
            near = pl.ds(j * 256, 256)
            v = r["raw"][near, rows(value_at + e * HEAD_DIM, HEAD_DIM, HEAD_DIM)]
            w = (dot_nt(da, v) * r["decay"][e, i - j]).astype(BF)
            r["weights"][at, near] = w
            total += dot(w, r["kpos"][e, near, :])
        lanes = rows(e * HEAD_DIM, HEAD_DIM, HEAD_DIM)
        co, si = r["cosine"][at, :], r["sine"][at, :]
        d = total[:, :HEAD_DIM] * co + total[:, HEAD_DIM:] * si
        raw = r["raw"][at, lanes].astype(F32)
        r["dproj"][at, lanes] = (d * swish_slope(raw)).astype(BF)

    def key_back(e, j):
        at = pl.ds(j * 256, 256)
        below = pl.ds(j * 256, t_all - j * 256)
        dk = dot_tn(r["weights"][below, at], r["qpos"][e, below, :])
        da = r["datt"][below, rows(e * HEAD_DIM, HEAD_DIM, HEAD_DIM)]
        dv = dot_tn(r["scores"][e, below, at], da)
        lanes = rows(LOCAL + e * HEAD_DIM, HEAD_DIM, HEAD_DIM)
        co, si = r["cosine"][at, :], r["sine"][at, :]
        d = dk[:, :HEAD_DIM] * co + dk[:, HEAD_DIM:] * si
        raw = r["raw"][at, lanes].astype(F32)
        r["dproj"][at, lanes] = (d * swish_slope(raw)).astype(BF)
        r["dproj"][at, rows(value_at + e * HEAD_DIM, HEAD_DIM, HEAD_DIM)] = dv.astype(BF)

    def head_back(e, carry):
        for i in range(blocks):
            query_back(e, i)
        for j in range(blocks):
            key_back(e, j)
        return carry

    base_q = base_r + (D // 128) * LOCAL

    def qkvu_grad(j, carry):
        g = dot_tn(r["n1"][:, rows(j * 256, 256, 256)], r["dproj"][...]).astype(BF)
        for k in range(D // 128):
            f[rows(base_q + k * D + j * 256, 256, 16), :] = g[:, k * 128 : (k + 1) * 128]
        return carry

    def one_part(b, carry):
        at = rows(b * 256, 256, 256)
        back = dot_nt(r["dproj"][at, pl.ds(0, 3 * LOCAL)], r["wqkv"][...])
        back += dot_nt(r["dproj"][at, pl.ds(3 * LOCAL, LOCAL)], r["wgate"][:, mine])
        r["lo_part"][at, :] = back.astype(BF)
        return carry

    own_tok = pltpu.make_async_copy(tok, r["weights"].at[pl.ds(0, tb), :], lsem.at[5])

    def last_block():
        one_rs.wait()
        own_tok.wait()
        for i in range(tb // 128):
            at = pl.ds(i * 128, 128)
            v = r["weights"][at, :].astype(F32)
            back = norm_back(v, rms_scale(v), one_rs.result(i * 128, 128))
            r["dhid"][at, :] = r["dhid"][at, :] + back
        copy = pltpu.make_async_copy(r["dhid"], r["grad_tokens"], lsem.at[1])
        copy.start()
        return copy

    def loop(lo, hi, body):
        lax.fori_loop(lo, hi, body, 0)

    def first_sums():
        loop(blocks // 2, blocks, partials)
        cot_ag.drain()
        dn_rs.start()
        lo_rs.start()

    def rest_sends():
        for ring in rings[3:]:
            ring.reduce_send(0, first=True)

    def input_sums():
        loop(0, blocks, one_part)
        dn_rs.drain()
        one_rs.start()
        own_tok.start()

    outs = ctx.outs
    plan = {
        0: ((lambda: loop(0, blocks // 2, partials),), (first_sums,)),
        1: ((), (dn_rs.middle,)),
        3: ((), (low_block,)),
        6: ((low_arrive, lo_rs.middle), (lambda: loop(0, blocks, mix_back),)),
        7: (
            (out_grad, lambda: loop(0, 2, head_back)),
            (lambda: loop(0, D // 256, qkvu_grad), rest_sends),
        ),
        9: ((), (lambda: outs.append(out_block()), lo_rs.drain)),
        10: ((), (input_sums,)),
        11: ((), (one_rs.middle,)),
        13: ((), (lambda: outs.append(last_block()),)),
    }
    assert blocks == 4
    total = 2 * (seq - 1)
    if seq > 16:
        for slot in sorted(plan):
            for piece in plan[slot][0] + plan[slot][1]:
                piece()
        for ring in rings:
            ring.all_steps()
        pltpu.make_async_copy(f, r["f_out"], ctx.psem.at[0]).start()
    else:
        done = [0]

        def rest_step():
            if done[0] < total:
                for ring in rings[3:]:
                    ring.step(done[0])
                done[0] += 1

        for slot in range(max(total, max(plan) + 1)):
            for i in range(2):
                if slot > 7:
                    rest_step()
                if slot < total:
                    for ring in rings[:1] if i == 0 else rings[1:3]:
                        ring.step(slot)
                for piece in plan.get(slot, ((), ()))[i]:
                    piece()
        while done[0] < total:
            rest_step()

    for ag in (att_ag, low_ag):
        ag.drain()
    one_rs.drain()
    for ring in rings:
        ring.drain()
    for copy in outs:
        copy.wait()
    pltpu.make_async_copy(f, r["f_out"], ctx.psem.at[0]).wait()


def main_call(sz, tokens, w_qkvu, w_out, w_glu, w_down, cotangent):
    any_spec = pl.BlockSpec(memory_space=pl.ANY)
    t, tb, fp, seq = sz.t, sz.tb, sz.fp, sz.seq
    scratch = dict(
        tok_g=pltpu.VMEM((t, D), BF),
        cot_g=pltpu.VMEM((t, D), BF),
        n1=pltpu.VMEM((t, D), BF),
        raw=pltpu.VMEM((t, 3 * LOCAL), BF),
        wqkv=pltpu.VMEM((D, 3 * LOCAL), BF),
        wgate=pltpu.VMEM((D, D), BF),
        wout=pltpu.VMEM((D, D), BF),
        wglu=pltpu.VMEM((D, 2 * fp), BF),
        wdown=pltpu.VMEM((fp, D), BF),
        qpos=pltpu.VMEM((2, t, 2 * HEAD_DIM), BF),
        kpos=pltpu.VMEM((2, t, 2 * HEAD_DIM), BF),
        scores=pltpu.VMEM((2, t, t), BF),
        weights=pltpu.VMEM((t, t), BF),
        decay=pltpu.VMEM((2, t // 256, 256, 256), F32),
        cosine=pltpu.VMEM((t, HEAD_DIM), F32),
        sine=pltpu.VMEM((t, HEAD_DIM), F32),
        att=pltpu.VMEM((PARTS, t, LOCAL), BF),
        gate=pltpu.VMEM((PARTS, t, LOCAL), BF),
        mixed=pltpu.VMEM((PARTS, t, LOCAL), BF),
        hidden=pltpu.VMEM((tb, D), F32),
        product=pltpu.VMEM((t, fp), BF),
        dpair=pltpu.VMEM((t, 2 * fp), BF),
        dn_part=pltpu.VMEM((t, D), BF),
        dn_near=pltpu.VMEM((2, tb, D), BF),
        dn_cross=pltpu.VMEM((tb, D), BF),
        lo_near=pltpu.VMEM((2, tb, D), BF),
        lo_cross=pltpu.VMEM((tb, D), BF),
        dhid=pltpu.VMEM((tb, D), F32),
        f=pltpu.VMEM((sz.total, 128), BF),
        slots0=pltpu.VMEM((2, seq - 1, sz.chunk[0], 128), BF),
        slots1=pltpu.VMEM((2, seq - 1, sz.chunk[1], 128), BF),
        slots2=pltpu.VMEM((2, seq - 1, sz.chunk[2], 128), BF),
        slots3=pltpu.VMEM((2, seq - 1, sz.chunk[3], 128), BF),
        slots4=pltpu.VMEM((2, seq - 1, sz.chunk[4], 128), BF),
        gsend=pltpu.SemaphoreType.DMA((30,)),
        grecv=pltpu.SemaphoreType.DMA((30,)),
        rsend=pltpu.SemaphoreType.DMA((5, 2, 2)),
        rrecv=pltpu.SemaphoreType.DMA((5, 2, 2)),
        psem=pltpu.SemaphoreType.DMA((1,)),
        lsem=pltpu.SemaphoreType.DMA((9,)),
    )
    if seq > 16:
        for i in range(5):
            del scratch["slots%d" % i]
        scratch["slots"] = pltpu.VMEM((2, seq - 1, max(sz.chunk), 128), BF)
    assert 2 * fp >= D + LOCAL and tb == 256
    names = ["tok", "w_qkvu", "w_out", "w_glu", "w_down", "cot", "layer_out", "grad_tokens", "f_out"]
    names += list(scratch)

    def kernel(*refs):
        named = dict(zip(names, refs))
        named["n2"] = named["weights"]
        for i in range(5 if seq > 16 else 0):
            named["slots%d" % i] = named["slots"].at[:, :, pl.ds(0, sz.chunk[i]), :]
        named["lo_part"] = named["tok_g"]
        named["one_near"], named["one_cross"] = named["dn_near"], named["dn_cross"]
        named["dproj"] = named["dpair"].at[:, pl.ds(0, D)]
        named["datt"] = named["dpair"].at[:, pl.ds(D, LOCAL)]
        layer_kernel(sz, list(named), *named.values())

    return pl.pallas_call(
        kernel,
        name="layer",
        out_shape=(
            jax.ShapeDtypeStruct((tb, D), BF),
            jax.ShapeDtypeStruct((tb, D), F32),
            jax.ShapeDtypeStruct((sz.total, 128), BF),
        ),
        in_specs=[any_spec] * 6,
        out_specs=(any_spec,) * 3,
        scratch_shapes=list(scratch.values()),
        compiler_params=pltpu.CompilerParams(
            collective_id=0, has_side_effects=True, vmem_limit_bytes=67043328
        ),
    )(tokens, w_qkvu, w_out, w_glu, w_down, cotangent)


def unpack_kernel(sz, flat, lo_in, gt_in, lo_out, gt_out, qkvu, out, glu, down, *scratch):
    buf, lo_b, gt_b, qkvu_b, out_b, glu_b, down_b, sem = scratch
    fs = sz.fs
    count = [0]

    def start(src, dst):
        copy = pltpu.make_async_copy(src, dst, sem.at[count[0]])
        copy.start()
        count[0] += 1
        return copy

    def fetch(first, size):
        return start(flat.at[pl.ds(first, size), :], buf.at[pl.ds(first, size), :])

    def tile(first, size):
        return buf[pl.ds(first, size), :].astype(F32)

    base_o = sz.base[3]
    base_q = base_o + (D // 128) * LOCAL
    half = (D // 128) * fs
    down_in = [fetch(k * 4 * fs, 4 * fs) for k in range(2)]
    glu_in = [fetch(sz.base[1 + k], half) for k in range(2)]
    out_in = fetch(base_o, (D // 128) * LOCAL)
    qkvu_in = [fetch(base_q + k * 2 * D, 2 * D) for k in range(4)]
    lo_copy, gt_copy = start(lo_in, lo_b), start(gt_in, gt_b)
    outs = []
    for k in range(2):
        down_in[k].wait()
        for i in range(4 * k, 4 * k + 4):
            down_b[:, pl.ds(i * 128, 128)] = tile(i * fs, fs)
        lanes = pl.ds(k * 512, 512)
        outs.append(start(down_b.at[:, lanes], down.at[:, lanes]))
    for k in range(2):
        glu_in[k].wait()
        for i in range(D // 128):
            glu_b[k, :, pl.ds(i * 128, 128)] = tile(sz.base[1 + k] + i * fs, fs)
        outs.append(start(glu_b.at[k], glu.at[k]))
    out_in.wait()
    for i in range(D // 128):
        out_b[:, pl.ds(i * 128, 128)] = tile(base_o + i * LOCAL, LOCAL)
    outs.append(start(out_b, out))
    for k in range(4):
        qkvu_in[k].wait()
        for i in range(2):
            qkvu_b[k, :, pl.ds(i * 128, 128)] = tile(base_q + (2 * k + i) * D, D)
        outs.append(start(qkvu_b.at[k], qkvu.at[k]))
    lo_copy.wait()
    outs.append(start(lo_b, lo_out))
    gt_copy.wait()
    outs.append(start(gt_b, gt_out))
    for copy in outs:
        copy.wait()


def unpack(sz, flat, layer_out, grad_tokens):
    any_spec = pl.BlockSpec(memory_space=pl.ANY)
    outs = (
        jax.ShapeDtypeStruct((sz.tb, D), BF),
        jax.ShapeDtypeStruct((sz.tb, D), F32),
        jax.ShapeDtypeStruct((4, D, LOCAL), F32),
        jax.ShapeDtypeStruct((LOCAL, D), F32),
        jax.ShapeDtypeStruct((2, sz.fs, D), F32),
        jax.ShapeDtypeStruct((sz.fs, D), F32),
    )
    return pl.pallas_call(
        functools.partial(unpack_kernel, sz),
        name="unpack",
        out_shape=outs,
        in_specs=[any_spec] * 3,
        out_specs=(any_spec,) * 6,
        scratch_shapes=[pltpu.VMEM((sz.total, 128), BF)]
        + [pltpu.VMEM(v.shape, v.dtype) for v in outs]
        + [pltpu.SemaphoreType.DMA((32,))],
        compiler_params=pltpu.CompilerParams(vmem_limit_bytes=67043328),
    )(flat, layer_out, grad_tokens)


def per_device(tokens, seq_lengths, w_qkvu, w_out, w_glu, w_down, cotangent):
    assert seq_lengths.shape == (1, 1) and lax.axis_size("head") == PARTS
    sz = Sizes(lax.axis_size("seq"), tokens.shape[0], w_down.shape[0])
    layer_out, grad_tokens, flat = main_call(sz, tokens, w_qkvu, w_out, w_glu, w_down, cotangent)
    outs = list(unpack(sz, flat, layer_out, grad_tokens))
    outs[4] = outs[4].transpose(0, 2, 1)
    return tuple(outs)


def solution(mesh):
    return jax.shard_map(
        per_device,
        mesh=mesh,
        in_specs=(
            P(("seq", "head"), None),
            P("seq", None),
            P(),
            P(),
            P(),
            P(),
            P(("seq", "head"), None),
        ),
        out_specs=(
            P(("seq", "head"), None),
            P(("seq", "head"), None),
            P(None, None, "head"),
            P("head", None),
            P(None, None, "head"),
            P("head", None),
        ),
        check_vma=False,
    )
```

```python
import functools

import jax
import jax.numpy as jnp
from jax import lax
from jax.experimental import pallas as pl
from jax.experimental.pallas import tpu as pltpu
from jax.sharding import PartitionSpec as P

D = 1024
HEADS = 8
HEAD_DIM = 128
EPSILON = 1e-06
PARTS = 4
LOCAL = D // PARTS
BF = jnp.bfloat16
F32 = jnp.float32
MESH = pl.DeviceIdType.MESH


def dot(a, b):
    return lax.dot_general(a, b, (((1,), (0,)), ((), ())), preferred_element_type=F32)


def dot_nt(a, b):
    return lax.dot_general(a, b, (((1,), (1,)), ((), ())), preferred_element_type=F32)


def dot_tn(a, b):
    return lax.dot_general(a, b, (((0,), (0,)), ((), ())), preferred_element_type=F32)


def sigmoid(v):
    return 1.0 / (1.0 + jnp.exp(-v))


def rms_scale(v):
    return lax.rsqrt(jnp.mean(v * v, axis=-1, keepdims=True) + EPSILON)


def norm_back(v, scale, grad):
    normed = v * scale
    return scale * (grad - normed * jnp.mean(grad * normed, axis=-1, keepdims=True))


def round_up(n, m):
    return -(-n // m) * m


def rows(start, size, align):
    return pl.ds(pl.multiple_of(start, align), size)


class Sizes:
    def __init__(self, seq, block, ff):
        self.seq = seq
        self.tb = block
        self.t = block * PARTS
        self.fs = ff // PARTS
        self.fp = round_up(self.fs, 256)
        rest = (D // 128) * LOCAL + 4 * (LOCAL // 128) * D
        chunk = lambda n: round_up(-(-n // (2 * seq)), 16)
        self.chunk = [chunk((D // 128) * self.fs)] * 3 + [chunk(rest // 2)]
        self.chunk.append(chunk(rest - 2 * seq * self.chunk[3]))
        self.base = [2 * seq * sum(self.chunk[:i]) for i in range(6)]
        self.total = self.base[5]


class Gather:
    def __init__(self, ctx, count, own, place, first):
        self.ctx, self.count, self.own, self.place, self.first = ctx, count, own, place, first

    def copy(self, src, dst, index, target):
        c = self.ctx
        return pltpu.make_async_remote_copy(
            src_ref=src,
            dst_ref=dst,
            send_sem=c.gsend.at[index],
            recv_sem=c.grecv.at[index],
            device_id=(c.s, target),
            device_id_type=MESH,
        )

    def across(self, k):
        c = self.ctx
        return self.copy(self.own(k), self.place(c.h, k), self.first + 3 * k, c.yp)

    def beside(self, k):
        c = self.ctx
        return self.copy(self.own(k), self.place(c.h, k), self.first + 3 * k + 1, c.sib)

    def relay(self, k):
        c = self.ctx
        spot = self.place(c.yp, k)
        return self.copy(spot, spot, self.first + 3 * k + 2, c.sib)

    def start(self, k):
        self.across(k).start()
        self.beside(k).start()

    def pass_on(self, k):
        self.across(k).wait_recv()
        self.relay(k).start()

    def wait_beside(self, k):
        self.beside(k).wait_recv()

    def wait_relay(self, k):
        self.relay(k).wait_recv()

    def drain(self):
        for k in range(self.count):
            self.across(k).wait_send()
            self.beside(k).wait_send()
            self.relay(k).wait_send()


class Scatter:
    def __init__(self, ctx, part, near, cross, first):
        self.ctx, self.part, self.near, self.cross, self.first = ctx, part, near, cross, first
        self.tb = ctx.sz.tb

    def block(self, index):
        return self.part.at[rows(index * self.tb, self.tb, self.tb), :]

    def copy(self, src, dst, index, target):
        c = self.ctx
        return pltpu.make_async_remote_copy(
            src_ref=src,
            dst_ref=dst,
            send_sem=c.gsend.at[index],
            recv_sem=c.grecv.at[index],
            device_id=(c.s, target),
            device_id_type=MESH,
        )

    def beside(self, k):
        c = self.ctx
        return self.copy(self.block(2 * k + 1 - c.c), self.near.at[k], self.first + k, c.sib)

    def across(self):
        c = self.ctx
        return self.copy(self.block(c.yp), self.cross, self.first + 2, c.yp)

    def start(self):
        self.beside(0).start()
        self.beside(1).start()

    def middle(self):
        c = self.ctx
        self.beside(0).wait_recv()
        self.beside(1).wait_recv()
        there = self.block(c.yp)
        there[...] = (there[...].astype(F32) + self.near[1 - c.y].astype(F32)).astype(BF)
        self.across().start()

    def result(self, lo, size):
        c = self.ctx
        here = self.part[rows(c.h * self.tb + lo, size, size), :].astype(F32)
        at = pl.ds(lo, size)
        return here + self.near[c.y, at, :].astype(F32) + self.cross[at, :].astype(F32)

    def wait(self):
        self.across().wait_recv()

    def drain(self):
        self.beside(0).wait_send()
        self.beside(1).wait_send()
        self.across().wait_send()


class Ring:
    def __init__(self, ctx, index, slots):
        self.ctx, self.index, self.slots = ctx, index, slots
        self.base, self.chunk = ctx.sz.base[index], ctx.sz.chunk[index]
        self.n = ctx.sz.seq

    def mine(self, d, k):
        k = lax.rem(k, self.n)
        return rows(self.base + (2 * k + d) * self.chunk, self.chunk, 16)

    def copy(self, d, src, dst, step):
        c = self.ctx
        return pltpu.make_async_remote_copy(
            src_ref=src,
            dst_ref=dst,
            send_sem=c.rsend.at[self.index, d, lax.rem(step, 2)],
            recv_sem=c.rrecv.at[self.index, d, lax.rem(step, 2)],
            device_id=(c.right if d == 0 else c.left, c.h),
            device_id_type=MESH,
        )

    def toward(self, d, t):
        return self.ctx.p + (self.n - t if d == 0 else t)

    def publish(self, d, k):
        if self.n > 16:
            return
        at = self.mine(d, k)
        c = self.ctx
        pltpu.make_async_copy(c.f.at[at, :], c.f_out.at[at, :], c.psem.at[0]).start()

    def reduce_copy(self, d, t, first=False):
        f = self.ctx.f
        src = f.at[self.mine(d, self.toward(d, t)), :] if first else self.slots.at[d, t - 1]
        return self.copy(d, src, self.slots.at[d, t], t)

    def reduce_send(self, t, first=False):
        for d in range(2):
            self.reduce_copy(d, t, first).start()

    def reduce_take(self, t, last=False):
        f = self.ctx.f
        pieces = 4 if self.chunk % 64 == 0 else (2 if self.chunk % 32 == 0 else 1)
        size = self.chunk // pieces
        for d in range(2):
            self.reduce_copy(d, t, first=True).wait_recv()
            k = lax.rem(self.toward(d, t) + (self.n - 1 if d == 0 else 1), self.n)
            start = self.base + (2 * k + d) * self.chunk
            for i in range(pieces):
                at = rows(start + i * size, size, 16)
                inside = pl.ds(i * size, size)
                total = f[at, :].astype(F32) + self.slots[d, t, inside, :].astype(F32)
                if last:
                    f[at, :] = total.astype(BF)
                else:
                    self.slots[d, t, inside, :] = total.astype(BF)
            if last:
                self.publish(d, k)

    def spread_copy(self, d, t):
        spot = self.ctx.f.at[self.mine(d, self.toward(d, t) + (1 if d == 0 else self.n - 1)), :]
        return self.copy(d, spot, spot, self.n - 1 + t)

    def spread_send(self, t):
        for d in range(2):
            self.spread_copy(d, t).start()

    def spread_take(self, t):
        for d in range(2):
            self.spread_copy(d, t).wait_recv()
            if isinstance(t, int):
                self.publish(d, self.toward(d, t))

    def left(self, step):
        for d in range(2):
            if isinstance(step, int) and step >= self.n - 1:
                self.spread_copy(d, step - self.n + 1).wait_send()
            else:
                self.reduce_copy(d, step, first=True).wait_send()

    def step(self, t):
        last = self.n - 2
        if t <= last:
            self.reduce_take(t, last=t == last)
        else:
            self.spread_take(t - self.n + 1)
        if t > 0:
            self.left(t - 1)
        if t < last:
            self.reduce_send(t + 1)
        elif t < 2 * last + 1:
            self.spread_send(t - last)

    def all_steps(self):
        last = self.n - 2
        self.step(0)

        def turn(t, carry):
            self.reduce_take(t)
            self.left(t - 1)
            self.reduce_send(t + 1)
            return carry

        lax.fori_loop(1, last, turn, 0)
        self.step(last)

        def pass_on(t, carry):
            self.spread_take(t)
            self.left(last + t)
            self.spread_send(t + 1)
            return carry

        lax.fori_loop(0, last, pass_on, 0)
        self.step(2 * last + 1)

    def drain(self):
        self.left(2 * self.n - 3)


class Ctx:
    pass


def layer_kernel(sz, names, *refs):
    r = dict(zip(names, refs))
    ctx = Ctx()
    ctx.sz = sz
    seq, tb, t_all, fs, fp = sz.seq, sz.tb, sz.t, sz.fs, sz.fp
    half = seq // 2
    s, h = lax.axis_index("seq"), lax.axis_index("head")
    c, y = lax.rem(h, 2), h // 2
    z, x = s // 2, lax.rem(s, 2)
    pos = (1 - x) * z + x * (2 * half - 1 - z)

    def at_pos(p):
        q = p // half
        return (1 - q) * 2 * p + q * (2 * (2 * half - 1 - p) + 1)

    ctx.s, ctx.h, ctx.c, ctx.y, ctx.p = s, h, c, y, pos
    ctx.sib, ctx.yp = y * 2 + (1 - c), (1 - y) * 2 + c
    far = (1 - y) * 2 + (1 - c)
    ctx.right = at_pos(lax.rem(pos + 1, seq))
    ctx.left = at_pos(lax.rem(pos + seq - 1, seq))
    ctx.gsend, ctx.grecv = r["gsend"], r["grecv"]
    ctx.rsend, ctx.rrecv = r["rsend"], r["rrecv"]
    f = ctx.f = r["f"]
    ctx.f_out, ctx.psem, ctx.outs = r["f_out"], r["psem"], []
    lsem = r["lsem"]

    tok, cot, tok_g, cot_g = r["tok"], r["cot"], r["tok_g"], r["cot_g"]
    att, gate, mixed = r["att"], r["gate"], r["mixed"]

    loads = []

    def load(src, dst):
        copy = pltpu.make_async_copy(src, dst, lsem.at[len(loads)])
        copy.start()
        loads.append(copy)
        return copy

    barrier = pltpu.get_barrier_semaphore()
    for peer in ((s, ctx.sib), (s, ctx.yp), (ctx.right, h), (ctx.left, h)):
        pl.semaphore_signal(barrier, inc=1, device_id=peer, device_id_type=MESH)

    mine = pl.ds(pl.multiple_of(h * LOCAL, LOCAL), LOCAL)
    own_rows = rows(h * tb, tb, tb)
    tok_in = load(tok, tok_g.at[own_rows, :])
    qkv_in = [
        load(r["w_qkvu"].at[k, :, mine], r["wqkv"].at[:, pl.ds(k * LOCAL, LOCAL)]) for k in range(3)
    ]
    gate_in = load(r["w_qkvu"].at[3], r["wgate"])
    out_in = load(r["w_out"], r["wout"])
    down_in = load(r["w_down"].at[rows(h * fs, fs, 64), :], r["wdown"].at[pl.ds(0, fs), :])
    window = y * (2 * fs) + c * (fs - fs % 128)
    tiles = fp // 128
    for k in range(2):
        for j in range(tiles):
            lane = pl.ds(pl.multiple_of(window + j * 128, 128), 128)
            staged = f.at[pl.ds((k * tiles + j) * D, D), :]
            pltpu.make_async_copy(r["w_glu"].at[k, :, lane], staged, lsem.at[8]).start()
    cot_in = load(cot, cot_g.at[own_rows, :])

    pl.semaphore_wait(barrier, 4)

    hb = tb // 2
    token_ag = Gather(
        ctx,
        2,
        lambda k: tok.at[pl.ds(k * hb, hb), :],
        lambda b, k: tok_g.at[rows(b * tb + k * hb, hb, hb), :],
        0,
    )
    cot_ag = Gather(
        ctx,
        2,
        lambda k: cot.at[pl.ds(k * hb, hb), :],
        lambda b, k: cot_g.at[rows(b * tb + k * hb, hb, hb), :],
        6,
    )
    blocks = t_all // 256
    att_place = lambda b, k: att.at[b, pl.ds(k * 256, 256), :]
    att_ag = Gather(ctx, blocks, lambda k: att_place(h, k), att_place, 18)
    low_place = lambda b, k: cot_g.at[rows(b * tb + k * hb, hb, hb), :]
    low_ag = Gather(ctx, 2, lambda k: low_place(h, k), low_place, 0)

    token_ag.start(0)
    token_ag.start(1)
    cot_ag.start(0)

    lane = lax.broadcasted_iota(jnp.int32, (32, HEAD_DIM), 1).astype(F32)
    step = lax.broadcasted_iota(jnp.int32, (32, HEAD_DIM), 0).astype(F32)
    frequency = jnp.exp(lane * (-9.210340371976184 / HEAD_DIM))
    fine = step * frequency
    coarse = (step * 32.0) * frequency
    cos_a, sin_a, cos_b, sin_b = jnp.cos(coarse), jnp.sin(coarse), jnp.cos(fine), jnp.sin(fine)
    for a in range(t_all // 32):
        at = pl.ds(a * 32, 32)
        ca, sa = cos_a[a : a + 1], sin_a[a : a + 1]
        r["cosine"][at, :] = ca * cos_b - sa * sin_b
        r["sine"][at, :] = sa * cos_b + ca * sin_b

    gap = lax.broadcasted_iota(jnp.int32, (256, 256), 0) - lax.broadcasted_iota(
        jnp.int32, (256, 256), 1
    )
    for e in range(2):
        slope = jnp.float32(0)
        for g in range(HEADS):
            slope = jnp.where(h * 2 + e == g, 2.0 ** (-8.0 * (g + 1) / HEADS), slope)
        for k in range(blocks):
            distance = gap + 256 * k
            value = jnp.exp(jnp.maximum(distance, 0).astype(F32) * -slope)
            r["decay"][e, k] = jnp.where(distance >= 0, value, 0.0)

    r["wdown"][pl.ds(fs, fp - fs), :] = jnp.zeros((fp - fs, D), BF)
    staged = f.at[pl.ds(0, 2 * tiles * D), :]
    pltpu.make_async_copy(staged, staged, lsem.at[8]).wait()
    part = fs % 128
    low_lanes = lax.broadcasted_iota(jnp.int32, (256, 128), 1) < 128 - part
    keep = lax.broadcasted_iota(jnp.int32, (256, 128), 1) < part if part else None

    def window_rows(n, carry):
        k, i = n // (D // 256), lax.rem(n, D // 256)
        first = k * tiles * D + i * 256
        tile = [f[rows(first + j * D, 256, 256), :].astype(F32) for j in range(tiles)]
        for j in range(tiles):
            value = tile[j]
            if part:
                straight = jnp.where(keep, value, 0.0) if j == tiles - 1 else value
                after = pltpu.roll(tile[j + 1], 128 - part, 1) if j < tiles - 1 else 0.0
                moved = jnp.where(low_lanes, pltpu.roll(value, 128 - part, 1), after)
                value = jnp.where(c == 1, moved, straight)
            lanes = pl.ds(pl.multiple_of(k * fp + j * 128, 128), 128)
            r["wglu"][rows(i * 256, 256, 256), lanes] = value.astype(BF)
        return carry

    lax.fori_loop(0, 2 * (D // 256), window_rows, 0)

    tok_in.wait()
    for one in qkv_in:
        one.wait()
    gate_in.wait()

    def project(b):
        at = rows(b * tb, tb, tb)
        v = tok_g[at, :].astype(F32)
        n1 = (v * rms_scale(v)).astype(BF)
        r["n1"][at, :] = n1
        qkv = dot(n1, r["wqkv"][...]).astype(BF)
        r["raw"][at, :] = qkv
        co, si = r["cosine"][at, :], r["sine"][at, :]
        for e in range(2):
            for name, first in (("qpos", 0), ("kpos", LOCAL)):
                w = qkv[:, first + e * HEAD_DIM : first + (e + 1) * HEAD_DIM].astype(F32)
                act = w * sigmoid(w)
                r[name][e, at, pl.ds(0, HEAD_DIM)] = (act * co).astype(BF)
                r[name][e, at, pl.ds(HEAD_DIM, HEAD_DIM)] = (act * si).astype(BF)
        for k in range(PARTS):
            gate[k, at, :] = dot(n1, r["wgate"][:, pl.ds(k * LOCAL, LOCAL)]).astype(BF)

    def member(k):
        yy = y + (k // 2) * (1 - 2 * y)
        cc = c + lax.rem(k, 2) * (1 - 2 * c)
        return yy * 2 + cc

    def project_turn(k, carry):
        @pl.when(k == 1)
        def _():
            for i in range(2):
                token_ag.wait_beside(i)

        @pl.when(k == 2)
        def _():
            for i in range(2):
                token_ag.pass_on(i)

        @pl.when(k == 3)
        def _():
            for i in range(2):
                token_ag.wait_relay(i)

        project(member(k))
        return carry

    lax.fori_loop(0, PARTS, project_turn, 0)

    value_at = 2 * LOCAL

    def attend(i):
        at = pl.ds(i * 256, 256)

        def one_head(e, carry):
            lanes = rows(value_at + e * HEAD_DIM, HEAD_DIM, HEAD_DIM)
            q = r["qpos"][e, at, :]
            total = jnp.zeros((256, HEAD_DIM), F32)
            for j in range(i + 1):
                near = pl.ds(j * 256, 256)
                scores = (dot_nt(q, r["kpos"][e, near, :]) * r["decay"][e, i - j]).astype(BF)
                r["scores"][e, at, near] = scores
                total += dot(scores, r["raw"][near, lanes])
            att[h, at, rows(e * HEAD_DIM, HEAD_DIM, HEAD_DIM)] = total.astype(BF)
            return carry

        lax.fori_loop(0, 2, one_head, 0)

    for i in range(blocks):
        attend(i)
        att_ag.start(i)
    cot_ag.start(1)

    out_in.wait()
    down_in.wait()
    cot_in.wait()
    cot_ag.pass_on(0)
    cot_ag.wait_beside(0)
    cot_ag.wait_relay(0)

    def mlp(b, carry):
        for k in range(blocks):

            @pl.when(b == k)
            def _():
                if k + 1 < blocks:
                    att_ag.pass_on(k + 1)
                att_ag.wait_beside(k)
                att_ag.wait_relay(k)

        at = rows(b * 256, 256, 256)
        a = [att[k, at, :].astype(F32) for k in range(PARTS)]
        ssq = sum(jnp.sum(v * v, axis=-1, keepdims=True) for v in a)
        scale = lax.rsqrt(ssq * (1.0 / D) + EPSILON)
        hidden = tok_g[at, :].astype(F32)
        for k in range(PARTS):
            g = gate[k, at, :].astype(F32)
            m = (a[k] * scale * (g * sigmoid(g))).astype(BF)
            mixed[k, at, :] = m
            hidden += dot(m, r["wout"][pl.ds(k * LOCAL, LOCAL), :])

        @pl.when(b == h)
        def _():
            r["hidden"][...] = hidden

        n2 = (hidden * rms_scale(hidden)).astype(BF)
        r["n2"][at, :] = n2
        g = dot(n2, r["wglu"][:, pl.ds(0, fp)])
        u = dot(n2, r["wglu"][:, pl.ds(fp, fp)])
        product = (g * u).astype(BF)
        r["product"][at, :] = product
        dp = dot_nt(cot_g[rows(b * tb, hb, hb), :], r["wdown"][...])
        for lanes, v in ((pl.ds(0, fp), u), (pl.ds(fp, fp), g)):
            r["dpair"][rows(b * tb, hb, hb), lanes] = (dp * v[:hb]).astype(BF)
            r["dpair"][rows(b * tb + hb, hb, hb), lanes] = v[hb:].astype(BF)
        return carry

    def second_half(k, carry):
        @pl.when(k == 1)
        def _():
            cot_ag.wait_beside(1)

        @pl.when(k == 2)
        def _():
            cot_ag.pass_on(1)

        @pl.when(k == 3)
        def _():
            cot_ag.wait_relay(1)

        at = rows(member(k) * tb + hb, hb, hb)
        dp = dot_nt(cot_g[at, :], r["wdown"][...])
        for lanes in (pl.ds(0, fp), pl.ds(fp, fp)):
            v = r["dpair"][at, lanes].astype(F32)
            r["dpair"][at, lanes] = (dp * v).astype(BF)
        return carry

    def partials(b, carry):
        at = rows(b * 256, 256, 256)
        r["lo_part"][at, :] = dot(r["product"][at, :], r["wdown"][...]).astype(BF)
        r["dn_part"][at, :] = dot_nt(r["dpair"][at, :], r["wglu"][...]).astype(BF)
        return carry

    token_ag.drain()
    att_ag.pass_on(0)
    lax.fori_loop(0, blocks, mlp, 0)
    lax.fori_loop(0, PARTS, second_half, 0)

    dn_rs = Scatter(ctx, r["dn_part"], r["dn_near"], r["dn_cross"], 12)
    lo_rs = Scatter(ctx, r["lo_part"], r["lo_near"], r["lo_cross"], 15)
    one_rs = Scatter(ctx, r["lo_part"], r["one_near"], r["one_cross"], 12)
    rings = [Ring(ctx, i, r["slots%d" % i]) for i in range(5)]

    base = sz.base[0]
    for j in range(fp // 256):
        size = min(256, fs - j * 256)
        g = dot_tn(r["product"][:, pl.ds(j * 256, 256)], cot_g[...]).astype(BF)
        for k in range(D // 128):
            f[pl.ds(base + k * fs + j * 256, size), :] = g[:size, k * 128 : (k + 1) * 128]
    rings[0].reduce_send(0, first=True)

    def glu_grad(k):
        first = sz.base[1 + k]
        for j in range(fp // 256):
            size = min(256, fs - j * 256)
            lanes = rows(k * fp + j * 256, 256, 256)
            g = dot_tn(r["dpair"][:, lanes], r["n2"][...]).astype(BF)
            for i in range(D // 128):
                at = rows(first + i * fs + j * 256, size, 16)
                f[at, :] = g[:size, i * 128 : (i + 1) * 128]
        rings[1 + k].reduce_send(0, first=True)

    for k in range(2):
        glu_grad(k)

    def low_block():
        dn_rs.wait()
        for i in range(tb // 128):
            at = pl.ds(i * 128, 128)
            v = r["hidden"][at, :]
            back = norm_back(v, rms_scale(v), dn_rs.result(i * 128, 128))
            d = cot_g[rows(h * tb + i * 128, 128, 128), :].astype(F32) + back
            r["dhid"][at, :] = d
            cot_g[rows(h * tb + i * 128, 128, 128), :] = d.astype(BF)
        low_ag.start(0)
        low_ag.start(1)

    def out_block():
        lo_rs.wait()
        for i in range(tb // 128):
            at = pl.ds(i * 128, 128)
            r["lo_cross"][at, :] = (r["hidden"][at, :] + lo_rs.result(i * 128, 128)).astype(BF)
        copy = pltpu.make_async_copy(r["lo_cross"], r["layer_out"], lsem.at[0])
        copy.start()
        return copy

    def low_arrive():
        for k in range(2):
            low_ag.pass_on(k)
        for k in range(2):
            low_ag.wait_beside(k)
            low_ag.wait_relay(k)

    own_out = pl.ds(pl.multiple_of(h * LOCAL, LOCAL), LOCAL)

    def mix_back(b, carry):
        at = rows(b * 256, 256, 256)
        low = cot_g[at, :]
        a = [att[k, at, :].astype(F32) for k in range(PARTS)]
        ssq = sum(jnp.sum(v * v, axis=-1, keepdims=True) for v in a)
        scale = lax.rsqrt(ssq * (1.0 / D) + EPSILON)
        inner = jnp.zeros((256, 1), F32)
        for k in range(PARTS):
            g = gate[k, at, :].astype(F32)
            e = dot_nt(low, r["wout"][pl.ds(k * LOCAL, LOCAL), :]) * (g * sigmoid(g))
            inner += jnp.sum(e * (a[k] * scale), axis=-1, keepdims=True)
        inner = inner * (1.0 / D)
        g = gate[h, at, :].astype(F32)
        sig = sigmoid(g)
        normed = att[h, at, :].astype(F32) * scale
        dm = dot_nt(low, r["wout"][own_out, :])
        slope = sig + g * sig * (1.0 - sig)
        r["dproj"][at, pl.ds(3 * LOCAL, LOCAL)] = (dm * normed * slope).astype(BF)
        r["datt"][at, :] = (scale * (dm * (g * sig) - normed * inner)).astype(BF)
        return carry

    base_r = sz.base[3]

    def out_grad():
        g = dot_tn(mixed[h], cot_g[...]).astype(BF)
        for k in range(D // 128):
            f[pl.ds(base_r + k * LOCAL, LOCAL), :] = g[:, k * 128 : (k + 1) * 128]

    def swish_slope(v):
        sig = sigmoid(v)
        return sig + v * sig * (1.0 - sig)

    def query_back(e, i):
        at = pl.ds(i * 256, 256)
        da = r["datt"][at, rows(e * HEAD_DIM, HEAD_DIM, HEAD_DIM)]
        total = jnp.zeros((256, 2 * HEAD_DIM), F32)
        for j in range(i + 1):
            near = pl.ds(j * 256, 256)
            v = r["raw"][near, rows(value_at + e * HEAD_DIM, HEAD_DIM, HEAD_DIM)]
            w = (dot_nt(da, v) * r["decay"][e, i - j]).astype(BF)
            r["weights"][at, near] = w
            total += dot(w, r["kpos"][e, near, :])
        lanes = rows(e * HEAD_DIM, HEAD_DIM, HEAD_DIM)
        co, si = r["cosine"][at, :], r["sine"][at, :]
        d = total[:, :HEAD_DIM] * co + total[:, HEAD_DIM:] * si
        raw = r["raw"][at, lanes].astype(F32)
        r["dproj"][at, lanes] = (d * swish_slope(raw)).astype(BF)

    def key_back(e, j):
        at = pl.ds(j * 256, 256)
        below = pl.ds(j * 256, t_all - j * 256)
        dk = dot_tn(r["weights"][below, at], r["qpos"][e, below, :])
        da = r["datt"][below, rows(e * HEAD_DIM, HEAD_DIM, HEAD_DIM)]
        dv = dot_tn(r["scores"][e, below, at], da)
        lanes = rows(LOCAL + e * HEAD_DIM, HEAD_DIM, HEAD_DIM)
        co, si = r["cosine"][at, :], r["sine"][at, :]
        d = dk[:, :HEAD_DIM] * co + dk[:, HEAD_DIM:] * si
        raw = r["raw"][at, lanes].astype(F32)
        r["dproj"][at, lanes] = (d * swish_slope(raw)).astype(BF)
        r["dproj"][at, rows(value_at + e * HEAD_DIM, HEAD_DIM, HEAD_DIM)] = dv.astype(BF)

    def head_back(e, carry):
        for i in range(blocks):
            query_back(e, i)
        for j in range(blocks):
            key_back(e, j)
        return carry

    base_q = base_r + (D // 128) * LOCAL

    def qkvu_grad(j, carry):
        g = dot_tn(r["n1"][:, rows(j * 256, 256, 256)], r["dproj"][...]).astype(BF)
        for k in range(D // 128):
            f[rows(base_q + k * D + j * 256, 256, 16), :] = g[:, k * 128 : (k + 1) * 128]
        return carry

    def one_part(b, carry):
        at = rows(b * 256, 256, 256)
        back = dot_nt(r["dproj"][at, pl.ds(0, 3 * LOCAL)], r["wqkv"][...])
        back += dot_nt(r["dproj"][at, pl.ds(3 * LOCAL, LOCAL)], r["wgate"][:, mine])
        r["lo_part"][at, :] = back.astype(BF)
        return carry

    own_tok = pltpu.make_async_copy(tok, r["weights"].at[pl.ds(0, tb), :], lsem.at[5])

    def last_block():
        one_rs.wait()
        own_tok.wait()
        for i in range(tb // 128):
            at = pl.ds(i * 128, 128)
            v = r["weights"][at, :].astype(F32)
            back = norm_back(v, rms_scale(v), one_rs.result(i * 128, 128))
            r["dhid"][at, :] = r["dhid"][at, :] + back
        copy = pltpu.make_async_copy(r["dhid"], r["grad_tokens"], lsem.at[1])
        copy.start()
        return copy

    def loop(lo, hi, body):
        lax.fori_loop(lo, hi, body, 0)

    def first_sums():
        loop(blocks // 2, blocks, partials)
        cot_ag.drain()
        dn_rs.start()
        lo_rs.start()

    def rest_sends():
        for ring in rings[3:]:
            ring.reduce_send(0, first=True)

    def input_sums():
        loop(0, blocks, one_part)
        dn_rs.drain()
        one_rs.start()
        own_tok.start()

    outs = ctx.outs
    plan = {
        0: ((lambda: loop(0, blocks // 2, partials),), (first_sums,)),
        1: ((), (dn_rs.middle,)),
        3: ((), (low_block,)),
        6: ((low_arrive, lo_rs.middle), (lambda: loop(0, blocks, mix_back),)),
        7: (
            (out_grad, lambda: loop(0, 2, head_back)),
            (lambda: loop(0, D // 256, qkvu_grad), rest_sends),
        ),
        9: ((), (lambda: outs.append(out_block()), lo_rs.drain)),
        10: ((), (input_sums,)),
        11: ((), (one_rs.middle,)),
        13: ((), (lambda: outs.append(last_block()),)),
    }
    assert blocks == 4
    total = 2 * (seq - 1)
    if seq > 16:
        for slot in sorted(plan):
            for piece in plan[slot][0] + plan[slot][1]:
                piece()
        for ring in rings:
            ring.all_steps()
        pltpu.make_async_copy(f, r["f_out"], ctx.psem.at[0]).start()
    else:
        done = [0]

        def rest_step():
            if done[0] < total:
                for ring in rings[3:]:
                    ring.step(done[0])
                done[0] += 1

        for slot in range(max(total, max(plan) + 1)):
            for i in range(2):
                if slot > 7:
                    rest_step()
                if slot < total:
                    for ring in rings[:1] if i == 0 else rings[1:3]:
                        ring.step(slot)
                for piece in plan.get(slot, ((), ()))[i]:
                    piece()
        while done[0] < total:
            rest_step()

    for ag in (att_ag, low_ag):
        ag.drain()
    one_rs.drain()
    for ring in rings:
        ring.drain()
    for copy in outs:
        copy.wait()
    pltpu.make_async_copy(f, r["f_out"], ctx.psem.at[0]).wait()


def main_call(sz, tokens, w_qkvu, w_out, w_glu, w_down, cotangent):
    any_spec = pl.BlockSpec(memory_space=pl.ANY)
    t, tb, fp, seq = sz.t, sz.tb, sz.fp, sz.seq
    scratch = dict(
        tok_g=pltpu.VMEM((t, D), BF),
        cot_g=pltpu.VMEM((t, D), BF),
        n1=pltpu.VMEM((t, D), BF),
        raw=pltpu.VMEM((t, 3 * LOCAL), BF),
        wqkv=pltpu.VMEM((D, 3 * LOCAL), BF),
        wgate=pltpu.VMEM((D, D), BF),
        wout=pltpu.VMEM((D, D), BF),
        wglu=pltpu.VMEM((D, 2 * fp), BF),
        wdown=pltpu.VMEM((fp, D), BF),
        qpos=pltpu.VMEM((2, t, 2 * HEAD_DIM), BF),
        kpos=pltpu.VMEM((2, t, 2 * HEAD_DIM), BF),
        scores=pltpu.VMEM((2, t, t), BF),
        weights=pltpu.VMEM((t, t), BF),
        decay=pltpu.VMEM((2, t // 256, 256, 256), F32),
        cosine=pltpu.VMEM((t, HEAD_DIM), F32),
        sine=pltpu.VMEM((t, HEAD_DIM), F32),
        att=pltpu.VMEM((PARTS, t, LOCAL), BF),
        gate=pltpu.VMEM((PARTS, t, LOCAL), BF),
        mixed=pltpu.VMEM((PARTS, t, LOCAL), BF),
        hidden=pltpu.VMEM((tb, D), F32),
        product=pltpu.VMEM((t, fp), BF),
        dpair=pltpu.VMEM((t, 2 * fp), BF),
        dn_part=pltpu.VMEM((t, D), BF),
        dn_near=pltpu.VMEM((2, tb, D), BF),
        dn_cross=pltpu.VMEM((tb, D), BF),
        lo_near=pltpu.VMEM((2, tb, D), BF),
        lo_cross=pltpu.VMEM((tb, D), BF),
        dhid=pltpu.VMEM((tb, D), F32),
        f=pltpu.VMEM((sz.total, 128), BF),
        slots0=pltpu.VMEM((2, seq - 1, sz.chunk[0], 128), BF),
        slots1=pltpu.VMEM((2, seq - 1, sz.chunk[1], 128), BF),
        slots2=pltpu.VMEM((2, seq - 1, sz.chunk[2], 128), BF),
        slots3=pltpu.VMEM((2, seq - 1, sz.chunk[3], 128), BF),
        slots4=pltpu.VMEM((2, seq - 1, sz.chunk[4], 128), BF),
        gsend=pltpu.SemaphoreType.DMA((30,)),
        grecv=pltpu.SemaphoreType.DMA((30,)),
        rsend=pltpu.SemaphoreType.DMA((5, 2, 2)),
        rrecv=pltpu.SemaphoreType.DMA((5, 2, 2)),
        psem=pltpu.SemaphoreType.DMA((1,)),
        lsem=pltpu.SemaphoreType.DMA((9,)),
    )
    if seq > 16:
        for i in range(5):
            del scratch["slots%d" % i]
        scratch["slots"] = pltpu.VMEM((2, seq - 1, max(sz.chunk), 128), BF)
    assert 2 * fp >= D + LOCAL and tb == 256
    names = ["tok", "w_qkvu", "w_out", "w_glu", "w_down", "cot", "layer_out", "grad_tokens", "f_out"]
    names += list(scratch)

    def kernel(*refs):
        named = dict(zip(names, refs))
        named["n2"] = named["weights"]
        for i in range(5 if seq > 16 else 0):
            named["slots%d" % i] = named["slots"].at[:, :, pl.ds(0, sz.chunk[i]), :]
        named["lo_part"] = named["tok_g"]
        named["one_near"], named["one_cross"] = named["dn_near"], named["dn_cross"]
        named["dproj"] = named["dpair"].at[:, pl.ds(0, D)]
        named["datt"] = named["dpair"].at[:, pl.ds(D, LOCAL)]
        layer_kernel(sz, list(named), *named.values())

    return pl.pallas_call(
        kernel,
        name="layer",
        out_shape=(
            jax.ShapeDtypeStruct((tb, D), BF),
            jax.ShapeDtypeStruct((tb, D), F32),
            jax.ShapeDtypeStruct((sz.total, 128), BF),
        ),
        in_specs=[any_spec] * 6,
        out_specs=(any_spec,) * 3,
        scratch_shapes=list(scratch.values()),
        compiler_params=pltpu.CompilerParams(
            collective_id=0, has_side_effects=True, vmem_limit_bytes=67043328
        ),
    )(tokens, w_qkvu, w_out, w_glu, w_down, cotangent)


def unpack_kernel(sz, flat, lo_in, gt_in, lo_out, gt_out, qkvu, out, glu, down, *scratch):
    buf, lo_b, gt_b, qkvu_b, out_b, glu_b, down_b, sem = scratch
    fs = sz.fs
    count = [0]

    def start(src, dst):
        copy = pltpu.make_async_copy(src, dst, sem.at[count[0]])
        copy.start()
        count[0] += 1
        return copy

    def fetch(first, size):
        return start(flat.at[pl.ds(first, size), :], buf.at[pl.ds(first, size), :])

    def tile(first, size):
        return buf[pl.ds(first, size), :].astype(F32)

    base_o = sz.base[3]
    base_q = base_o + (D // 128) * LOCAL
    half = (D // 128) * fs
    down_in = [fetch(k * 4 * fs, 4 * fs) for k in range(2)]
    glu_in = [fetch(sz.base[1 + k], half) for k in range(2)]
    out_in = fetch(base_o, (D // 128) * LOCAL)
    qkvu_in = [fetch(base_q + k * 2 * D, 2 * D) for k in range(4)]
    lo_copy, gt_copy = start(lo_in, lo_b), start(gt_in, gt_b)
    outs = []
    for k in range(2):
        down_in[k].wait()
        for i in range(4 * k, 4 * k + 4):
            down_b[:, pl.ds(i * 128, 128)] = tile(i * fs, fs)
        lanes = pl.ds(k * 512, 512)
        outs.append(start(down_b.at[:, lanes], down.at[:, lanes]))
    for k in range(2):
        glu_in[k].wait()
        for i in range(D // 128):
            glu_b[k, :, pl.ds(i * 128, 128)] = tile(sz.base[1 + k] + i * fs, fs)
        outs.append(start(glu_b.at[k], glu.at[k]))
    out_in.wait()
    for i in range(D // 128):
        out_b[:, pl.ds(i * 128, 128)] = tile(base_o + i * LOCAL, LOCAL)
    outs.append(start(out_b, out))
    for k in range(4):
        qkvu_in[k].wait()
        for i in range(2):
            qkvu_b[k, :, pl.ds(i * 128, 128)] = tile(base_q + (2 * k + i) * D, D)
        outs.append(start(qkvu_b.at[k], qkvu.at[k]))
    lo_copy.wait()
    outs.append(start(lo_b, lo_out))
    gt_copy.wait()
    outs.append(start(gt_b, gt_out))
    for copy in outs:
        copy.wait()


def unpack(sz, flat, layer_out, grad_tokens):
    any_spec = pl.BlockSpec(memory_space=pl.ANY)
    outs = (
        jax.ShapeDtypeStruct((sz.tb, D), BF),
        jax.ShapeDtypeStruct((sz.tb, D), F32),
        jax.ShapeDtypeStruct((4, D, LOCAL), F32),
        jax.ShapeDtypeStruct((LOCAL, D), F32),
        jax.ShapeDtypeStruct((2, sz.fs, D), F32),
        jax.ShapeDtypeStruct((sz.fs, D), F32),
    )
    return pl.pallas_call(
        functools.partial(unpack_kernel, sz),
        name="unpack",
        out_shape=outs,
        in_specs=[any_spec] * 3,
        out_specs=(any_spec,) * 6,
        scratch_shapes=[pltpu.VMEM((sz.total, 128), BF)]
        + [pltpu.VMEM(v.shape, v.dtype) for v in outs]
        + [pltpu.SemaphoreType.DMA((32,))],
        compiler_params=pltpu.CompilerParams(vmem_limit_bytes=67043328),
    )(flat, layer_out, grad_tokens)


def per_device(tokens, seq_lengths, w_qkvu, w_out, w_glu, w_down, cotangent):
    assert seq_lengths.shape == (1, 1) and lax.axis_size("head") == PARTS
    sz = Sizes(lax.axis_size("seq"), tokens.shape[0], w_down.shape[0])
    layer_out, grad_tokens, flat = main_call(sz, tokens, w_qkvu, w_out, w_glu, w_down, cotangent)
    outs = list(unpack(sz, flat, layer_out, grad_tokens))
    outs[4] = outs[4].transpose(0, 2, 1)
    return tuple(outs)


def solution(mesh):
    return jax.shard_map(
        per_device,
        mesh=mesh,
        in_specs=(
            P(("seq", "head"), None),
            P("seq", None),
            P(),
            P(),
            P(),
            P(),
            P(("seq", "head"), None),
        ),
        out_specs=(
            P(("seq", "head"), None),
            P(("seq", "head"), None),
            P(None, None, "head"),
            P("head", None),
            P(None, None, "head"),
            P("head", None),
        ),
        check_vma=False,
    )
```

```python
import functools

import jax
import jax.numpy as jnp
from jax import lax
from jax.experimental import pallas as pl
from jax.experimental.pallas import tpu as pltpu
from jax.sharding import PartitionSpec as P

D = 1024
HEADS = 8
HEAD_DIM = 128
EPSILON = 1e-06
PARTS = 4
LOCAL = D // PARTS
BF = jnp.bfloat16
F32 = jnp.float32
MESH = pl.DeviceIdType.MESH


def dot(a, b):
    return lax.dot_general(a, b, (((1,), (0,)), ((), ())), preferred_element_type=F32)


def dot_nt(a, b):
    return lax.dot_general(a, b, (((1,), (1,)), ((), ())), preferred_element_type=F32)


def dot_tn(a, b):
    return lax.dot_general(a, b, (((0,), (0,)), ((), ())), preferred_element_type=F32)


def sigmoid(v):
    return 1.0 / (1.0 + jnp.exp(-v))


def rms_scale(v):
    return lax.rsqrt(jnp.mean(v * v, axis=-1, keepdims=True) + EPSILON)


def norm_back(v, scale, grad):
    normed = v * scale
    return scale * (grad - normed * jnp.mean(grad * normed, axis=-1, keepdims=True))


def round_up(n, m):
    return -(-n // m) * m


def rows(start, size, align):
    return pl.ds(pl.multiple_of(start, align), size)


class Sizes:
    def __init__(self, seq, block, ff):
        self.seq = seq
        self.tb = block
        self.t = block * PARTS
        self.fs = ff // PARTS
        self.fp = round_up(self.fs, 256)
        rest = (D // 128) * LOCAL + 4 * (LOCAL // 128) * D
        chunk = lambda n: round_up(-(-n // (2 * seq)), 16)
        self.chunk = [chunk((D // 128) * self.fs)] * 3 + [chunk(rest // 2)]
        self.chunk.append(chunk(rest - 2 * seq * self.chunk[3]))
        self.base = [2 * seq * sum(self.chunk[:i]) for i in range(6)]
        self.total = self.base[5]


class Gather:
    def __init__(self, ctx, count, own, place, first):
        self.ctx, self.count, self.own, self.place, self.first = ctx, count, own, place, first

    def copy(self, src, dst, index, target):
        c = self.ctx
        return pltpu.make_async_remote_copy(
            src_ref=src,
            dst_ref=dst,
            send_sem=c.gsend.at[index],
            recv_sem=c.grecv.at[index],
            device_id=(c.s, target),
            device_id_type=MESH,
        )

    def across(self, k):
        c = self.ctx
        return self.copy(self.own(k), self.place(c.h, k), self.first + 3 * k, c.yp)

    def beside(self, k):
        c = self.ctx
        return self.copy(self.own(k), self.place(c.h, k), self.first + 3 * k + 1, c.sib)

    def relay(self, k):
        c = self.ctx
        spot = self.place(c.yp, k)
        return self.copy(spot, spot, self.first + 3 * k + 2, c.sib)

    def start(self, k):
        self.across(k).start()
        self.beside(k).start()

    def pass_on(self, k):
        self.across(k).wait_recv()
        self.relay(k).start()

    def wait_beside(self, k):
        self.beside(k).wait_recv()

    def wait_relay(self, k):
        self.relay(k).wait_recv()

    def drain(self):
        for k in range(self.count):
            self.across(k).wait_send()
            self.beside(k).wait_send()
            self.relay(k).wait_send()


class Scatter:
    def __init__(self, ctx, part, near, cross, first):
        self.ctx, self.part, self.near, self.cross, self.first = ctx, part, near, cross, first
        self.tb = ctx.sz.tb

    def block(self, index):
        return self.part.at[rows(index * self.tb, self.tb, self.tb), :]

    def copy(self, src, dst, index, target):
        c = self.ctx
        return pltpu.make_async_remote_copy(
            src_ref=src,
            dst_ref=dst,
            send_sem=c.gsend.at[index],
            recv_sem=c.grecv.at[index],
            device_id=(c.s, target),
            device_id_type=MESH,
        )

    def beside(self, k):
        c = self.ctx
        return self.copy(self.block(2 * k + 1 - c.c), self.near.at[k], self.first + k, c.sib)

    def across(self):
        c = self.ctx
        return self.copy(self.block(c.yp), self.cross, self.first + 2, c.yp)

    def start(self):
        self.beside(0).start()
        self.beside(1).start()

    def middle(self):
        c = self.ctx
        self.beside(0).wait_recv()
        self.beside(1).wait_recv()
        there = self.block(c.yp)
        there[...] = (there[...].astype(F32) + self.near[1 - c.y].astype(F32)).astype(BF)
        self.across().start()

    def result(self, lo, size):
        c = self.ctx
        here = self.part[rows(c.h * self.tb + lo, size, size), :].astype(F32)
        at = pl.ds(lo, size)
        return here + self.near[c.y, at, :].astype(F32) + self.cross[at, :].astype(F32)

    def wait(self):
        self.across().wait_recv()

    def drain(self):
        self.beside(0).wait_send()
        self.beside(1).wait_send()
        self.across().wait_send()


class Ring:
    def __init__(self, ctx, index, slots):
        self.ctx, self.index, self.slots = ctx, index, slots
        self.base, self.chunk = ctx.sz.base[index], ctx.sz.chunk[index]
        self.n = ctx.sz.seq

    def mine(self, d, k):
        k = lax.rem(k, self.n)
        return rows(self.base + (2 * k + d) * self.chunk, self.chunk, 16)

    def copy(self, d, src, dst, step):
        c = self.ctx
        return pltpu.make_async_remote_copy(
            src_ref=src,
            dst_ref=dst,
            send_sem=c.rsend.at[self.index, d, lax.rem(step, 2)],
            recv_sem=c.rrecv.at[self.index, d, lax.rem(step, 2)],
            device_id=(c.right if d == 0 else c.left, c.h),
            device_id_type=MESH,
        )

    def toward(self, d, t):
        return self.ctx.p + (self.n - t if d == 0 else t)

    def publish(self, d, k):
        if self.n > 16:
            return
        at = self.mine(d, k)
        c = self.ctx
        pltpu.make_async_copy(c.f.at[at, :], c.f_out.at[at, :], c.psem.at[0]).start()

    def reduce_copy(self, d, t, first=False):
        f = self.ctx.f
        src = f.at[self.mine(d, self.toward(d, t)), :] if first else self.slots.at[d, t - 1]
        return self.copy(d, src, self.slots.at[d, t], t)

    def reduce_send(self, t, first=False):
        for d in range(2):
            self.reduce_copy(d, t, first).start()

    def reduce_take(self, t, last=False):
        f = self.ctx.f
        pieces = 4 if self.chunk % 64 == 0 else (2 if self.chunk % 32 == 0 else 1)
        size = self.chunk // pieces
        for d in range(2):
            self.reduce_copy(d, t, first=True).wait_recv()
            k = lax.rem(self.toward(d, t) + (self.n - 1 if d == 0 else 1), self.n)
            start = self.base + (2 * k + d) * self.chunk
            for i in range(pieces):
                at = rows(start + i * size, size, 16)
                inside = pl.ds(i * size, size)
                total = f[at, :].astype(F32) + self.slots[d, t, inside, :].astype(F32)
                if last:
                    f[at, :] = total.astype(BF)
                else:
                    self.slots[d, t, inside, :] = total.astype(BF)
            if last:
                self.publish(d, k)

    def spread_copy(self, d, t):
        spot = self.ctx.f.at[self.mine(d, self.toward(d, t) + (1 if d == 0 else self.n - 1)), :]
        return self.copy(d, spot, spot, self.n - 1 + t)

    def spread_send(self, t):
        for d in range(2):
            self.spread_copy(d, t).start()

    def spread_take(self, t):
        for d in range(2):
            self.spread_copy(d, t).wait_recv()
            if isinstance(t, int):
                self.publish(d, self.toward(d, t))

    def left(self, step):
        for d in range(2):
            if isinstance(step, int) and step >= self.n - 1:
                self.spread_copy(d, step - self.n + 1).wait_send()
            else:
                self.reduce_copy(d, step, first=True).wait_send()

    def step(self, t):
        last = self.n - 2
        if t <= last:
            self.reduce_take(t, last=t == last)
        else:
            self.spread_take(t - self.n + 1)
        if t > 0:
            self.left(t - 1)
        if t < last:
            self.reduce_send(t + 1)
        elif t < 2 * last + 1:
            self.spread_send(t - last)

    def all_steps(self):
        last = self.n - 2
        self.step(0)

        def turn(t, carry):
            self.reduce_take(t)
            self.left(t - 1)
            self.reduce_send(t + 1)
            return carry

        lax.fori_loop(1, last, turn, 0)
        self.step(last)

        def pass_on(t, carry):
            self.spread_take(t)
            self.left(last + t)
            self.spread_send(t + 1)
            return carry

        lax.fori_loop(0, last, pass_on, 0)
        self.step(2 * last + 1)

    def drain(self):
        self.left(2 * self.n - 3)


class Ctx:
    pass


def layer_kernel(sz, names, *refs):
    r = dict(zip(names, refs))
    ctx = Ctx()
    ctx.sz = sz
    seq, tb, t_all, fs, fp = sz.seq, sz.tb, sz.t, sz.fs, sz.fp
    half = seq // 2
    s, h = lax.axis_index("seq"), lax.axis_index("head")
    c, y = lax.rem(h, 2), h // 2
    z, x = s // 2, lax.rem(s, 2)
    pos = (1 - x) * z + x * (2 * half - 1 - z)

    def at_pos(p):
        q = p // half
        return (1 - q) * 2 * p + q * (2 * (2 * half - 1 - p) + 1)

    ctx.s, ctx.h, ctx.c, ctx.y, ctx.p = s, h, c, y, pos
    ctx.sib, ctx.yp = y * 2 + (1 - c), (1 - y) * 2 + c
    far = (1 - y) * 2 + (1 - c)
    ctx.right = at_pos(lax.rem(pos + 1, seq))
    ctx.left = at_pos(lax.rem(pos + seq - 1, seq))
    ctx.gsend, ctx.grecv = r["gsend"], r["grecv"]
    ctx.rsend, ctx.rrecv = r["rsend"], r["rrecv"]
    f = ctx.f = r["f"]
    ctx.f_out, ctx.psem, ctx.outs = r["f_out"], r["psem"], []
    lsem = r["lsem"]

    tok, cot, tok_g, cot_g = r["tok"], r["cot"], r["tok_g"], r["cot_g"]
    att, gate, mixed = r["att"], r["gate"], r["mixed"]

    loads = []

    def load(src, dst):
        copy = pltpu.make_async_copy(src, dst, lsem.at[len(loads)])
        copy.start()
        loads.append(copy)
        return copy

    barrier = pltpu.get_barrier_semaphore()
    for peer in ((s, ctx.sib), (s, ctx.yp), (ctx.right, h), (ctx.left, h)):
        pl.semaphore_signal(barrier, inc=1, device_id=peer, device_id_type=MESH)

    mine = pl.ds(pl.multiple_of(h * LOCAL, LOCAL), LOCAL)
    own_rows = rows(h * tb, tb, tb)
    tok_in = load(tok, tok_g.at[own_rows, :])
    qkv_in = [
        load(r["w_qkvu"].at[k, :, mine], r["wqkv"].at[:, pl.ds(k * LOCAL, LOCAL)]) for k in range(3)
    ]
    gate_in = load(r["w_qkvu"].at[3], r["wgate"])
    out_in = load(r["w_out"], r["wout"])
    down_in = load(r["w_down"].at[rows(h * fs, fs, 64), :], r["wdown"].at[pl.ds(0, fs), :])
    window = y * (2 * fs) + c * (fs - fs % 128)
    tiles = fp // 128
    for k in range(2):
        for j in range(tiles):
            lane = pl.ds(pl.multiple_of(window + j * 128, 128), 128)
            staged = f.at[pl.ds((k * tiles + j) * D, D), :]
            pltpu.make_async_copy(r["w_glu"].at[k, :, lane], staged, lsem.at[8]).start()
    cot_in = load(cot, cot_g.at[own_rows, :])

    pl.semaphore_wait(barrier, 4)

    hb = tb // 2
    late = tb // 4
    early = tb - late
    token_ag = Gather(
        ctx,
        2,
        lambda k: tok.at[pl.ds(k * hb, hb), :],
        lambda b, k: tok_g.at[rows(b * tb + k * hb, hb, hb), :],
        0,
    )
    cot_ag = Gather(
        ctx,
        2,
        lambda k: cot.at[pl.ds(k * early, (tb - early) if k else early), :],
        lambda b, k: cot_g.at[rows(b * tb + k * early, (tb - early) if k else early, late), :],
        6,
    )
    blocks = t_all // 256
    att_place = lambda b, k: att.at[b, pl.ds(k * 256, 256), :]
    att_ag = Gather(ctx, blocks, lambda k: att_place(h, k), att_place, 18)
    low_place = lambda b, k: cot_g.at[rows(b * tb + k * hb, hb, hb), :]
    low_ag = Gather(ctx, 2, lambda k: low_place(h, k), low_place, 0)

    token_ag.start(0)
    token_ag.start(1)
    cot_ag.start(0)

    lane = lax.broadcasted_iota(jnp.int32, (32, HEAD_DIM), 1).astype(F32)
    step = lax.broadcasted_iota(jnp.int32, (32, HEAD_DIM), 0).astype(F32)
    frequency = jnp.exp(lane * (-9.210340371976184 / HEAD_DIM))
    fine = step * frequency
    coarse = (step * 32.0) * frequency
    cos_a, sin_a, cos_b, sin_b = jnp.cos(coarse), jnp.sin(coarse), jnp.cos(fine), jnp.sin(fine)
    for a in range(t_all // 32):
        at = pl.ds(a * 32, 32)
        ca, sa = cos_a[a : a + 1], sin_a[a : a + 1]
        r["cosine"][at, :] = ca * cos_b - sa * sin_b
        r["sine"][at, :] = sa * cos_b + ca * sin_b

    gap = lax.broadcasted_iota(jnp.int32, (256, 256), 0) - lax.broadcasted_iota(
        jnp.int32, (256, 256), 1
    )
    for e in range(2):
        slope = jnp.float32(0)
        for g in range(HEADS):
            slope = jnp.where(h * 2 + e == g, 2.0 ** (-8.0 * (g + 1) / HEADS), slope)
        for k in range(blocks):
            distance = gap + 256 * k
            value = jnp.exp(jnp.maximum(distance, 0).astype(F32) * -slope)
            r["decay"][e, k] = jnp.where(distance >= 0, value, 0.0)

    r["wdown"][pl.ds(fs, fp - fs), :] = jnp.zeros((fp - fs, D), BF)
    staged = f.at[pl.ds(0, 2 * tiles * D), :]
    pltpu.make_async_copy(staged, staged, lsem.at[8]).wait()
    part = fs % 128
    low_lanes = lax.broadcasted_iota(jnp.int32, (256, 128), 1) < 128 - part
    keep = lax.broadcasted_iota(jnp.int32, (256, 128), 1) < part if part else None

    def window_rows(n, carry):
        k, i = n // (D // 256), lax.rem(n, D // 256)
        first = k * tiles * D + i * 256
        tile = [f[rows(first + j * D, 256, 256), :].astype(F32) for j in range(tiles)]
        for j in range(tiles):
            value = tile[j]
            if part:
                straight = jnp.where(keep, value, 0.0) if j == tiles - 1 else value
                after = pltpu.roll(tile[j + 1], 128 - part, 1) if j < tiles - 1 else 0.0
                moved = jnp.where(low_lanes, pltpu.roll(value, 128 - part, 1), after)
                value = jnp.where(c == 1, moved, straight)
            lanes = pl.ds(pl.multiple_of(k * fp + j * 128, 128), 128)
            r["wglu"][rows(i * 256, 256, 256), lanes] = value.astype(BF)
        return carry

    lax.fori_loop(0, 2 * (D // 256), window_rows, 0)

    tok_in.wait()
    for one in qkv_in:
        one.wait()
    gate_in.wait()

    def project(b):
        at = rows(b * tb, tb, tb)
        v = tok_g[at, :].astype(F32)
        n1 = (v * rms_scale(v)).astype(BF)
        r["n1"][at, :] = n1
        qkv = dot(n1, r["wqkv"][...]).astype(BF)
        r["raw"][at, :] = qkv
        co, si = r["cosine"][at, :], r["sine"][at, :]
        for e in range(2):
            for name, first in (("qpos", 0), ("kpos", LOCAL)):
                w = qkv[:, first + e * HEAD_DIM : first + (e + 1) * HEAD_DIM].astype(F32)
                act = w * sigmoid(w)
                r[name][e, at, pl.ds(0, HEAD_DIM)] = (act * co).astype(BF)
                r[name][e, at, pl.ds(HEAD_DIM, HEAD_DIM)] = (act * si).astype(BF)
        for k in range(PARTS):
            gate[k, at, :] = dot(n1, r["wgate"][:, pl.ds(k * LOCAL, LOCAL)]).astype(BF)

    def member(k):
        yy = y + (k // 2) * (1 - 2 * y)
        cc = c + lax.rem(k, 2) * (1 - 2 * c)
        return yy * 2 + cc

    def project_turn(k, carry):
        @pl.when(k == 1)
        def _():
            for i in range(2):
                token_ag.wait_beside(i)

        @pl.when(k == 2)
        def _():
            for i in range(2):
                token_ag.pass_on(i)

        @pl.when(k == 3)
        def _():
            for i in range(2):
                token_ag.wait_relay(i)

        project(member(k))
        return carry

    lax.fori_loop(0, PARTS, project_turn, 0)

    value_at = 2 * LOCAL

    def attend(i):
        at = pl.ds(i * 256, 256)

        def one_head(e, carry):
            lanes = rows(value_at + e * HEAD_DIM, HEAD_DIM, HEAD_DIM)
            q = r["qpos"][e, at, :]
            total = jnp.zeros((256, HEAD_DIM), F32)
            for j in range(i + 1):
                near = pl.ds(j * 256, 256)
                scores = (dot_nt(q, r["kpos"][e, near, :]) * r["decay"][e, i - j]).astype(BF)
                r["scores"][e, at, near] = scores
                total += dot(scores, r["raw"][near, lanes])
            att[h, at, rows(e * HEAD_DIM, HEAD_DIM, HEAD_DIM)] = total.astype(BF)
            return carry

        lax.fori_loop(0, 2, one_head, 0)

    for i in range(blocks):
        attend(i)
        att_ag.start(i)
    cot_ag.start(1)

    out_in.wait()
    down_in.wait()
    cot_in.wait()
    cot_ag.pass_on(0)
    cot_ag.wait_beside(0)
    cot_ag.wait_relay(0)

    def mlp(b, carry):
        for k in range(blocks):

            @pl.when(b == k)
            def _():
                if k + 1 < blocks:
                    att_ag.pass_on(k + 1)
                att_ag.wait_beside(k)
                att_ag.wait_relay(k)

        at = rows(b * 256, 256, 256)
        a = [att[k, at, :].astype(F32) for k in range(PARTS)]
        ssq = sum(jnp.sum(v * v, axis=-1, keepdims=True) for v in a)
        scale = lax.rsqrt(ssq * (1.0 / D) + EPSILON)
        hidden = tok_g[at, :].astype(F32)
        for k in range(PARTS):
            g = gate[k, at, :].astype(F32)
            m = (a[k] * scale * (g * sigmoid(g))).astype(BF)
            mixed[k, at, :] = m
            hidden += dot(m, r["wout"][pl.ds(k * LOCAL, LOCAL), :])

        @pl.when(b == h)
        def _():
            r["hidden"][...] = hidden

        n2 = (hidden * rms_scale(hidden)).astype(BF)
        r["n2"][at, :] = n2
        g = dot(n2, r["wglu"][:, pl.ds(0, fp)])
        u = dot(n2, r["wglu"][:, pl.ds(fp, fp)])
        product = (g * u).astype(BF)
        r["product"][at, :] = product
        dp = dot_nt(cot_g[rows(b * tb, early, late), :], r["wdown"][...])
        for lanes, v in ((pl.ds(0, fp), u), (pl.ds(fp, fp), g)):
            r["dpair"][rows(b * tb, early, late), lanes] = (dp * v[:early]).astype(BF)
            r["dpair"][rows(b * tb + early, late, late), lanes] = v[early:].astype(BF)
        return carry

    def second_half(k, carry):
        @pl.when(k == 1)
        def _():
            cot_ag.wait_beside(1)

        @pl.when(k == 2)
        def _():
            cot_ag.pass_on(1)

        @pl.when(k == 3)
        def _():
            cot_ag.wait_relay(1)

        at = rows(member(k) * tb + early, late, late)
        dp = dot_nt(cot_g[at, :], r["wdown"][...])
        for lanes in (pl.ds(0, fp), pl.ds(fp, fp)):
            v = r["dpair"][at, lanes].astype(F32)
            r["dpair"][at, lanes] = (dp * v).astype(BF)
        return carry

    def partials(b, carry):
        at = rows(b * 256, 256, 256)
        r["lo_part"][at, :] = dot(r["product"][at, :], r["wdown"][...]).astype(BF)
        r["dn_part"][at, :] = dot_nt(r["dpair"][at, :], r["wglu"][...]).astype(BF)
        return carry

    token_ag.drain()
    att_ag.pass_on(0)
    lax.fori_loop(0, blocks, mlp, 0)
    lax.fori_loop(0, PARTS, second_half, 0)

    dn_rs = Scatter(ctx, r["dn_part"], r["dn_near"], r["dn_cross"], 12)
    lo_rs = Scatter(ctx, r["lo_part"], r["lo_near"], r["lo_cross"], 15)
    one_rs = Scatter(ctx, r["lo_part"], r["one_near"], r["one_cross"], 12)
    rings = [Ring(ctx, i, r["slots%d" % i]) for i in range(5)]

    base = sz.base[0]
    for j in range(fp // 256):
        size = min(256, fs - j * 256)
        g = dot_tn(r["product"][:, pl.ds(j * 256, 256)], cot_g[...]).astype(BF)
        for k in range(D // 128):
            f[pl.ds(base + k * fs + j * 256, size), :] = g[:size, k * 128 : (k + 1) * 128]
    rings[0].reduce_send(0, first=True)

    def glu_grad(k):
        first = sz.base[1 + k]
        for j in range(fp // 256):
            size = min(256, fs - j * 256)
            lanes = rows(k * fp + j * 256, 256, 256)
            g = dot_tn(r["dpair"][:, lanes], r["n2"][...]).astype(BF)
            for i in range(D // 128):
                at = rows(first + i * fs + j * 256, size, 16)
                f[at, :] = g[:size, i * 128 : (i + 1) * 128]
        rings[1 + k].reduce_send(0, first=True)

    for k in range(2):
        glu_grad(k)

    def low_block():
        dn_rs.wait()
        for i in range(tb // 128):
            at = pl.ds(i * 128, 128)
            v = r["hidden"][at, :]
            back = norm_back(v, rms_scale(v), dn_rs.result(i * 128, 128))
            d = cot_g[rows(h * tb + i * 128, 128, 128), :].astype(F32) + back
            r["dhid"][at, :] = d
            cot_g[rows(h * tb + i * 128, 128, 128), :] = d.astype(BF)
        low_ag.start(0)
        low_ag.start(1)

    def out_block():
        lo_rs.wait()
        for i in range(tb // 128):
            at = pl.ds(i * 128, 128)
            r["lo_cross"][at, :] = (r["hidden"][at, :] + lo_rs.result(i * 128, 128)).astype(BF)
        copy = pltpu.make_async_copy(r["lo_cross"], r["layer_out"], lsem.at[0])
        copy.start()
        return copy

    def low_arrive():
        for k in range(2):
            low_ag.pass_on(k)
        for k in range(2):
            low_ag.wait_beside(k)
            low_ag.wait_relay(k)

    own_out = pl.ds(pl.multiple_of(h * LOCAL, LOCAL), LOCAL)

    def mix_back(b, carry):
        at = rows(b * 256, 256, 256)
        low = cot_g[at, :]
        a = [att[k, at, :].astype(F32) for k in range(PARTS)]
        ssq = sum(jnp.sum(v * v, axis=-1, keepdims=True) for v in a)
        scale = lax.rsqrt(ssq * (1.0 / D) + EPSILON)
        inner = jnp.zeros((256, 1), F32)
        for k in range(PARTS):
            g = gate[k, at, :].astype(F32)
            e = dot_nt(low, r["wout"][pl.ds(k * LOCAL, LOCAL), :]) * (g * sigmoid(g))
            inner += jnp.sum(e * (a[k] * scale), axis=-1, keepdims=True)
        inner = inner * (1.0 / D)
        g = gate[h, at, :].astype(F32)
        sig = sigmoid(g)
        normed = att[h, at, :].astype(F32) * scale
        dm = dot_nt(low, r["wout"][own_out, :])
        slope = sig + g * sig * (1.0 - sig)
        r["dproj"][at, pl.ds(3 * LOCAL, LOCAL)] = (dm * normed * slope).astype(BF)
        r["datt"][at, :] = (scale * (dm * (g * sig) - normed * inner)).astype(BF)
        return carry

    base_r = sz.base[3]

    def out_grad():
        g = dot_tn(mixed[h], cot_g[...]).astype(BF)
        for k in range(D // 128):
            f[pl.ds(base_r + k * LOCAL, LOCAL), :] = g[:, k * 128 : (k + 1) * 128]

    def swish_slope(v):
        sig = sigmoid(v)
        return sig + v * sig * (1.0 - sig)

    def query_back(e, i):
        at = pl.ds(i * 256, 256)
        da = r["datt"][at, rows(e * HEAD_DIM, HEAD_DIM, HEAD_DIM)]
        total = jnp.zeros((256, 2 * HEAD_DIM), F32)
        for j in range(i + 1):
            near = pl.ds(j * 256, 256)
            v = r["raw"][near, rows(value_at + e * HEAD_DIM, HEAD_DIM, HEAD_DIM)]
            w = (dot_nt(da, v) * r["decay"][e, i - j]).astype(BF)
            r["weights"][at, near] = w
            total += dot(w, r["kpos"][e, near, :])
        lanes = rows(e * HEAD_DIM, HEAD_DIM, HEAD_DIM)
        co, si = r["cosine"][at, :], r["sine"][at, :]
        d = total[:, :HEAD_DIM] * co + total[:, HEAD_DIM:] * si
        raw = r["raw"][at, lanes].astype(F32)
        r["dproj"][at, lanes] = (d * swish_slope(raw)).astype(BF)

    def key_back(e, j):
        at = pl.ds(j * 256, 256)
        below = pl.ds(j * 256, t_all - j * 256)
        dk = dot_tn(r["weights"][below, at], r["qpos"][e, below, :])
        da = r["datt"][below, rows(e * HEAD_DIM, HEAD_DIM, HEAD_DIM)]
        dv = dot_tn(r["scores"][e, below, at], da)
        lanes = rows(LOCAL + e * HEAD_DIM, HEAD_DIM, HEAD_DIM)
        co, si = r["cosine"][at, :], r["sine"][at, :]
        d = dk[:, :HEAD_DIM] * co + dk[:, HEAD_DIM:] * si
        raw = r["raw"][at, lanes].astype(F32)
        r["dproj"][at, lanes] = (d * swish_slope(raw)).astype(BF)
        r["dproj"][at, rows(value_at + e * HEAD_DIM, HEAD_DIM, HEAD_DIM)] = dv.astype(BF)

    def head_back(e, carry):
        for i in range(blocks):
            query_back(e, i)
        for j in range(blocks):
            key_back(e, j)
        return carry

    base_q = base_r + (D // 128) * LOCAL

    def qkvu_grad(j, carry):
        g = dot_tn(r["n1"][:, rows(j * 256, 256, 256)], r["dproj"][...]).astype(BF)
        for k in range(D // 128):
            f[rows(base_q + k * D + j * 256, 256, 16), :] = g[:, k * 128 : (k + 1) * 128]
        return carry

    def one_part(b, carry):
        at = rows(b * 256, 256, 256)
        back = dot_nt(r["dproj"][at, pl.ds(0, 3 * LOCAL)], r["wqkv"][...])
        back += dot_nt(r["dproj"][at, pl.ds(3 * LOCAL, LOCAL)], r["wgate"][:, mine])
        r["lo_part"][at, :] = back.astype(BF)
        return carry

    own_tok = pltpu.make_async_copy(tok, r["weights"].at[pl.ds(0, tb), :], lsem.at[5])

    def last_block():
        one_rs.wait()
        own_tok.wait()
        for i in range(tb // 128):
            at = pl.ds(i * 128, 128)
            v = r["weights"][at, :].astype(F32)
            back = norm_back(v, rms_scale(v), one_rs.result(i * 128, 128))
            r["dhid"][at, :] = r["dhid"][at, :] + back
        copy = pltpu.make_async_copy(r["dhid"], r["grad_tokens"], lsem.at[1])
        copy.start()
        return copy

    def loop(lo, hi, body):
        lax.fori_loop(lo, hi, body, 0)

    def first_sums():
        loop(blocks // 2, blocks, partials)
        cot_ag.drain()
        dn_rs.start()
        lo_rs.start()

    def rest_sends():
        for ring in rings[3:]:
            ring.reduce_send(0, first=True)

    def input_sums():
        loop(0, blocks, one_part)
        dn_rs.drain()
        one_rs.start()
        own_tok.start()

    outs = ctx.outs
    plan = {
        0: ((lambda: loop(0, blocks // 2, partials),), (first_sums,)),
        1: ((), (dn_rs.middle,)),
        3: ((), (low_block,)),
        6: ((low_arrive, lo_rs.middle), (lambda: loop(0, blocks, mix_back),)),
        7: (
            (out_grad, lambda: loop(0, 2, head_back)),
            (lambda: loop(0, D // 256, qkvu_grad), rest_sends),
        ),
        9: ((), (lambda: outs.append(out_block()), lo_rs.drain)),
        10: ((), (input_sums,)),
        11: ((), (one_rs.middle,)),
        13: ((), (lambda: outs.append(last_block()),)),
    }
    assert blocks == 4
    total = 2 * (seq - 1)
    if seq > 16:
        for slot in sorted(plan):
            for piece in plan[slot][0] + plan[slot][1]:
                piece()
        for ring in rings:
            ring.all_steps()
        pltpu.make_async_copy(f, r["f_out"], ctx.psem.at[0]).start()
    else:
        done = [0]

        def rest_step():
            if done[0] < total:
                for ring in rings[3:]:
                    ring.step(done[0])
                done[0] += 1

        for slot in range(max(total, max(plan) + 1)):
            for i in range(2):
                if slot > 7:
                    rest_step()
                if slot < total:
                    for ring in rings[:1] if i == 0 else rings[1:3]:
                        ring.step(slot)
                for piece in plan.get(slot, ((), ()))[i]:
                    piece()
        while done[0] < total:
            rest_step()

    for ag in (att_ag, low_ag):
        ag.drain()
    one_rs.drain()
    for ring in rings:
        ring.drain()
    for copy in outs:
        copy.wait()
    pltpu.make_async_copy(f, r["f_out"], ctx.psem.at[0]).wait()


def main_call(sz, tokens, w_qkvu, w_out, w_glu, w_down, cotangent):
    any_spec = pl.BlockSpec(memory_space=pl.ANY)
    t, tb, fp, seq = sz.t, sz.tb, sz.fp, sz.seq
    scratch = dict(
        tok_g=pltpu.VMEM((t, D), BF),
        cot_g=pltpu.VMEM((t, D), BF),
        n1=pltpu.VMEM((t, D), BF),
        raw=pltpu.VMEM((t, 3 * LOCAL), BF),
        wqkv=pltpu.VMEM((D, 3 * LOCAL), BF),
        wgate=pltpu.VMEM((D, D), BF),
        wout=pltpu.VMEM((D, D), BF),
        wglu=pltpu.VMEM((D, 2 * fp), BF),
        wdown=pltpu.VMEM((fp, D), BF),
        qpos=pltpu.VMEM((2, t, 2 * HEAD_DIM), BF),
        kpos=pltpu.VMEM((2, t, 2 * HEAD_DIM), BF),
        scores=pltpu.VMEM((2, t, t), BF),
        weights=pltpu.VMEM((t, t), BF),
        decay=pltpu.VMEM((2, t // 256, 256, 256), F32),
        cosine=pltpu.VMEM((t, HEAD_DIM), F32),
        sine=pltpu.VMEM((t, HEAD_DIM), F32),
        att=pltpu.VMEM((PARTS, t, LOCAL), BF),
        gate=pltpu.VMEM((PARTS, t, LOCAL), BF),
        mixed=pltpu.VMEM((PARTS, t, LOCAL), BF),
        hidden=pltpu.VMEM((tb, D), F32),
        product=pltpu.VMEM((t, fp), BF),
        dpair=pltpu.VMEM((t, 2 * fp), BF),
        dn_part=pltpu.VMEM((t, D), BF),
        dn_near=pltpu.VMEM((2, tb, D), BF),
        dn_cross=pltpu.VMEM((tb, D), BF),
        lo_near=pltpu.VMEM((2, tb, D), BF),
        lo_cross=pltpu.VMEM((tb, D), BF),
        dhid=pltpu.VMEM((tb, D), F32),
        f=pltpu.VMEM((sz.total, 128), BF),
        slots0=pltpu.VMEM((2, seq - 1, sz.chunk[0], 128), BF),
        slots1=pltpu.VMEM((2, seq - 1, sz.chunk[1], 128), BF),
        slots2=pltpu.VMEM((2, seq - 1, sz.chunk[2], 128), BF),
        slots3=pltpu.VMEM((2, seq - 1, sz.chunk[3], 128), BF),
        slots4=pltpu.VMEM((2, seq - 1, sz.chunk[4], 128), BF),
        gsend=pltpu.SemaphoreType.DMA((30,)),
        grecv=pltpu.SemaphoreType.DMA((30,)),
        rsend=pltpu.SemaphoreType.DMA((5, 2, 2)),
        rrecv=pltpu.SemaphoreType.DMA((5, 2, 2)),
        psem=pltpu.SemaphoreType.DMA((1,)),
        lsem=pltpu.SemaphoreType.DMA((9,)),
    )
    if seq > 16:
        for i in range(5):
            del scratch["slots%d" % i]
        scratch["slots"] = pltpu.VMEM((2, seq - 1, max(sz.chunk), 128), BF)
    assert 2 * fp >= D + LOCAL and tb == 256
    names = ["tok", "w_qkvu", "w_out", "w_glu", "w_down", "cot", "layer_out", "grad_tokens", "f_out"]
    names += list(scratch)

    def kernel(*refs):
        named = dict(zip(names, refs))
        named["n2"] = named["weights"]
        for i in range(5 if seq > 16 else 0):
            named["slots%d" % i] = named["slots"].at[:, :, pl.ds(0, sz.chunk[i]), :]
        named["lo_part"] = named["tok_g"]
        named["one_near"], named["one_cross"] = named["dn_near"], named["dn_cross"]
        named["dproj"] = named["dpair"].at[:, pl.ds(0, D)]
        named["datt"] = named["dpair"].at[:, pl.ds(D, LOCAL)]
        layer_kernel(sz, list(named), *named.values())

    return pl.pallas_call(
        kernel,
        name="layer",
        out_shape=(
            jax.ShapeDtypeStruct((tb, D), BF),
            jax.ShapeDtypeStruct((tb, D), F32),
            jax.ShapeDtypeStruct((sz.total, 128), BF),
        ),
        in_specs=[any_spec] * 6,
        out_specs=(any_spec,) * 3,
        scratch_shapes=list(scratch.values()),
        compiler_params=pltpu.CompilerParams(
            collective_id=0, has_side_effects=True, vmem_limit_bytes=67043328
        ),
    )(tokens, w_qkvu, w_out, w_glu, w_down, cotangent)


def unpack_kernel(sz, flat, lo_in, gt_in, lo_out, gt_out, qkvu, out, glu, down, *scratch):
    buf, lo_b, gt_b, qkvu_b, out_b, glu_b, down_b, sem = scratch
    fs = sz.fs
    count = [0]

    def start(src, dst):
        copy = pltpu.make_async_copy(src, dst, sem.at[count[0]])
        copy.start()
        count[0] += 1
        return copy

    def fetch(first, size):
        return start(flat.at[pl.ds(first, size), :], buf.at[pl.ds(first, size), :])

    def tile(first, size):
        return buf[pl.ds(first, size), :].astype(F32)

    base_o = sz.base[3]
    base_q = base_o + (D // 128) * LOCAL
    half = (D // 128) * fs
    down_in = [fetch(k * 4 * fs, 4 * fs) for k in range(2)]
    glu_in = [fetch(sz.base[1 + k], half) for k in range(2)]
    out_in = fetch(base_o, (D // 128) * LOCAL)
    qkvu_in = [fetch(base_q + k * 2 * D, 2 * D) for k in range(4)]
    lo_copy, gt_copy = start(lo_in, lo_b), start(gt_in, gt_b)
    outs = []
    for k in range(2):
        down_in[k].wait()
        for i in range(4 * k, 4 * k + 4):
            down_b[:, pl.ds(i * 128, 128)] = tile(i * fs, fs)
        lanes = pl.ds(k * 512, 512)
        outs.append(start(down_b.at[:, lanes], down.at[:, lanes]))
    for k in range(2):
        glu_in[k].wait()
        for i in range(D // 128):
            glu_b[k, :, pl.ds(i * 128, 128)] = tile(sz.base[1 + k] + i * fs, fs)
        outs.append(start(glu_b.at[k], glu.at[k]))
    out_in.wait()
    for i in range(D // 128):
        out_b[:, pl.ds(i * 128, 128)] = tile(base_o + i * LOCAL, LOCAL)
    outs.append(start(out_b, out))
    for k in range(4):
        qkvu_in[k].wait()
        for i in range(2):
            qkvu_b[k, :, pl.ds(i * 128, 128)] = tile(base_q + (2 * k + i) * D, D)
        outs.append(start(qkvu_b.at[k], qkvu.at[k]))
    lo_copy.wait()
    outs.append(start(lo_b, lo_out))
    gt_copy.wait()
    outs.append(start(gt_b, gt_out))
    for copy in outs:
        copy.wait()


def unpack(sz, flat, layer_out, grad_tokens):
    any_spec = pl.BlockSpec(memory_space=pl.ANY)
    outs = (
        jax.ShapeDtypeStruct((sz.tb, D), BF),
        jax.ShapeDtypeStruct((sz.tb, D), F32),
        jax.ShapeDtypeStruct((4, D, LOCAL), F32),
        jax.ShapeDtypeStruct((LOCAL, D), F32),
        jax.ShapeDtypeStruct((2, sz.fs, D), F32),
        jax.ShapeDtypeStruct((sz.fs, D), F32),
    )
    return pl.pallas_call(
        functools.partial(unpack_kernel, sz),
        name="unpack",
        out_shape=outs,
        in_specs=[any_spec] * 3,
        out_specs=(any_spec,) * 6,
        scratch_shapes=[pltpu.VMEM((sz.total, 128), BF)]
        + [pltpu.VMEM(v.shape, v.dtype) for v in outs]
        + [pltpu.SemaphoreType.DMA((32,))],
        compiler_params=pltpu.CompilerParams(vmem_limit_bytes=67043328),
    )(flat, layer_out, grad_tokens)


def per_device(tokens, seq_lengths, w_qkvu, w_out, w_glu, w_down, cotangent):
    assert seq_lengths.shape == (1, 1) and lax.axis_size("head") == PARTS
    sz = Sizes(lax.axis_size("seq"), tokens.shape[0], w_down.shape[0])
    layer_out, grad_tokens, flat = main_call(sz, tokens, w_qkvu, w_out, w_glu, w_down, cotangent)
    outs = list(unpack(sz, flat, layer_out, grad_tokens))
    outs[4] = outs[4].transpose(0, 2, 1)
    return tuple(outs)


def solution(mesh):
    return jax.shard_map(
        per_device,
        mesh=mesh,
        in_specs=(
            P(("seq", "head"), None),
            P("seq", None),
            P(),
            P(),
            P(),
            P(),
            P(("seq", "head"), None),
        ),
        out_specs=(
            P(("seq", "head"), None),
            P(("seq", "head"), None),
            P(None, None, "head"),
            P("head", None),
            P(None, None, "head"),
            P("head", None),
        ),
        check_vma=False,
    )
```
